32 devices in a mesh: ctx: 8 (over y, x, core), tp: 4 (over z).
Axes of the slice: x: 2, y: 2, z: 4, core: 2. Of those that a mesh axis runs over, the one named last changes fastest.
Arguments:
- tokens: bfloat16 [2, 1024, 2048], P(None, 'ctx', 'tp'), may hold values from -6 to 6
- w_query: bfloat16 [2048, 2048], P('ctx', 'tp'), may hold values from -0.125 to 0.125
- w_key: bfloat16 [2048, 2048], P('ctx', 'tp'), may hold values from -0.125 to 0.125
- w_value: bfloat16 [2048, 2048], P('ctx', 'tp'), may hold values from -0.125 to 0.125
- w_output: bfloat16 [2048, 2048], P('tp', 'ctx'), may hold values from -0.125 to 0.125
- w_gate: bfloat16 [2048, 8192], P('ctx', 'tp'), may hold values from -0.125 to 0.125
- w_up: bfloat16 [2048, 8192], P('ctx', 'tp'), may hold values from -0.125 to 0.125
- w_down: bfloat16 [8192, 2048], P('tp', 'ctx'), may hold values from -0.0625 to 0.0625
- gain_query: bfloat16 [2048], P(('tp', 'ctx')), may hold values from 0.5 to 1.5
- gain_key: bfloat16 [2048], P(('tp', 'ctx')), may hold values from 0.5 to 1.5
- gain_attention: bfloat16 [2048], P(('tp', 'ctx')), may hold values from 0.5 to 1.5
- gain_feedforward: bfloat16 [2048], P(('tp', 'ctx')), may hold values from 0.5 to 1.5
- block_order: int32 [2, 8], replicated, may hold values from 0 to 7, each once within a row
- cotangent: bfloat16 [2, 1024, 2048], P(None, 'ctx', 'tp'), may hold values from -6 to 6
Outputs:
- output: float32 [2, 1024, 2048], P(None, 'ctx', 'tp')
- grad_input: float32 [2, 1024, 2048], P(None, 'ctx', 'tp')
- grad_query: float32 [2048, 2048], P('ctx', 'tp')
- grad_key: float32 [2048, 2048], P('ctx', 'tp')
- grad_value: float32 [2048, 2048], P('ctx', 'tp')
- grad_output_proj: float32 [2048, 2048], P('tp', 'ctx')
- grad_gate: float32 [2048, 8192], P('ctx', 'tp')
- grad_up: float32 [2048, 8192], P('ctx', 'tp')
- grad_down: float32 [8192, 2048], P('tp', 'ctx')
- grad_gain_query: float32 [2048], P(('tp', 'ctx'))
- grad_gain_key: float32 [2048], P(('tp', 'ctx'))
- grad_gain_attention: float32 [2048], P(('tp', 'ctx'))
- grad_gain_feedforward: float32 [2048], P(('tp', 'ctx'))
The draws below stay inside these ranges and needn't reach their ends.
Inputs may be any that keep to these rules, and one draw needn't show every extreme that they name: Each row of block_order names each of the 8 blocks of a sequence once.
All inputs are finite; a program needn't handle non-finite values.
Results may differ from the reference program's by a relative error of at most 0.023.
Values may be sent and summed in bfloat16 or wider, within the bound.
A program may use at most 192 MiB of HBM per device.

```python
import jax
import jax.numpy as jnp
from jax import lax

D = 2048
H = 16
FF = 8192
HD = 128
SEQS = 2
BLK = 128
LEN = 1024
N_CTX = 8


def steps_of(key, shape, cuts, least, largest):
    level = 1.0
    for dim, shards_of in cuts:
        steps = jax.random.uniform(jax.random.fold_in(jax.random.fold_in(key, 6), dim), (shards_of,), jnp.float32, least / len(cuts), largest / len(cuts))
        level = level * jnp.repeat(jnp.exp(steps), shape[dim] // shards_of).reshape((-1,) + (1,) * (len(shape) - 1 - dim))
    return level


def normal_values(stream_key, extent, width, reach, cuts=(), kind=jnp.bfloat16):
    level = steps_of(stream_key, extent, cuts, -0.22, 0.18) if cuts else 1.0
    drawn = jax.random.normal(stream_key, extent, jnp.float32) * width * level
    return jnp.minimum(jnp.maximum(drawn, -reach), reach).astype(kind)


def setup_inputs(seed: int = 0) -> dict:
    key_of = jax.random.split(jax.random.key(seed), 15)
    return {
        "tokens": normal_values(key_of[0], (SEQS, LEN, D), 1.0, 6.0, ((1, 8), (2, 4))),
        "w_query": normal_values(key_of[1], (D, D), D ** -0.5, 0.125, ((0, 8), (1, 4))),
        "w_key": normal_values(key_of[2], (D, D), D ** -0.5, 0.125, ((0, 8), (1, 4))),
        "w_value": normal_values(key_of[3], (D, D), D ** -0.5, 0.125, ((0, 8), (1, 4))),
        "w_output": normal_values(key_of[4], (D, D), D ** -0.5, 0.125, ((0, 4), (1, 8))),
        "w_gate": normal_values(key_of[5], (D, FF), D ** -0.5, 0.125, ((0, 8), (1, 4))),
        "w_up": normal_values(key_of[6], (D, FF), D ** -0.5, 0.125, ((0, 8), (1, 4))),
        "w_down": normal_values(key_of[7], (FF, D), FF ** -0.5, 0.0625, ((0, 4), (1, 8))),
        "gain_query": jnp.clip(1.0 + 0.1 * jax.random.normal(key_of[8], (D,), jnp.float32), 0.5, 1.5).astype(jnp.bfloat16),
        "gain_key": jnp.clip(1.0 + 0.1 * jax.random.normal(key_of[9], (D,), jnp.float32), 0.5, 1.5).astype(jnp.bfloat16),
        "gain_attention": jnp.clip(1.0 + 0.1 * jax.random.normal(key_of[10], (D,), jnp.float32), 0.5, 1.5).astype(jnp.bfloat16),
        "gain_feedforward": jnp.clip(1.0 + 0.1 * jax.random.normal(key_of[11], (D,), jnp.float32), 0.5, 1.5).astype(jnp.bfloat16),
        "block_order": jax.vmap(lambda own: jax.random.permutation(own, N_CTX))(jax.random.split(key_of[12], SEQS)).reshape((SEQS, N_CTX)).astype(jnp.int32),
        "cotangent": normal_values(key_of[13], (SEQS, LEN, D), 1.0, 6.0, ((1, 8), (2, 4))),
    }


EPS = 1e-06
THETA = 500000.0
NEGATIVE = -1e+30

def rounded(value):
    return lax.optimization_barrier(value.astype(jnp.bfloat16)).astype(jnp.float32)

def rms_forward(value, gain):
    inverse = lax.rsqrt(lax.optimization_barrier(jnp.mean(value * value, axis=-1, keepdims=True)) + EPS)
    return (value * inverse * gain, inverse)

def rms_backward(value, inverse, gain, upstream):
    scaled = gain * upstream
    d_value = inverse * scaled - value * inverse ** 3 * lax.optimization_barrier(jnp.mean(scaled * value, axis=-1, keepdims=True))
    d_gain = lax.optimization_barrier(jnp.sum(upstream * value * inverse, axis=0))
    return (d_value, d_gain)

def rotary_tables(positions):
    half_dim = HD // 2
    frequency = THETA ** (-2.0 * jnp.arange(half_dim, dtype=jnp.float32) / HD)
    angles = positions.astype(jnp.float32)[..., None] * frequency
    return (jnp.cos(angles)[..., None, :], jnp.sin(angles)[..., None, :])

def rotate(value, cosine, sine):
    half_dim = value.shape[-1] // 2
    first, second = (value[..., :half_dim], value[..., half_dim:])
    return jnp.concatenate([first * cosine - second * sine, second * cosine + first * sine], axis=-1)

def unrotate(grad, cosine, sine):
    half_dim = grad.shape[-1] // 2
    first, second = (grad[..., :half_dim], grad[..., half_dim:])
    return jnp.concatenate([first * cosine + second * sine, second * cosine - first * sine], axis=-1)

def reference(tokens, w_query, w_key, w_value, w_output, w_gate, w_up, w_down, gain_query, gain_key, gain_attention, gain_feedforward, block_order, cotangent):
    scale = HD ** (-0.5)
    q_block = 512 if LEN % 512 == 0 else LEN
    block_count = LEN // q_block
    g_query = gain_query.astype(jnp.float32)
    g_key = gain_key.astype(jnp.float32)
    g_attn = gain_attention.astype(jnp.float32)
    g_feed = gain_feedforward.astype(jnp.float32)

    def one_sequence(carry, inputs):
        seq_tokens, upstream, order_row = inputs
        slots = jnp.arange(LEN, dtype=jnp.int32)
        positions = order_row[slots // BLK] * BLK + slots % BLK
        cosine, sine = rotary_tables(positions)
        queries = jnp.dot(seq_tokens, w_query, preferred_element_type=jnp.float32)
        keys_raw = jnp.dot(seq_tokens, w_key, preferred_element_type=jnp.float32)
        values_raw = jnp.dot(seq_tokens, w_value, preferred_element_type=jnp.float32)
        q_normed, q_inverse = rms_forward(queries, g_query)
        k_normed, k_inverse = rms_forward(keys_raw, g_key)
        q_rot = rounded(rotate(q_normed.reshape(LEN, H, HD), cosine, sine))
        k_rot = rounded(rotate(k_normed.reshape(LEN, H, HD), cosine, sine))
        v_heads = rounded(values_raw.reshape(LEN, H, HD))
        q_parts = q_rot.reshape(block_count, q_block, H, HD)
        pos_parts = positions.reshape(block_count, q_block)

        def attend(args):
            q_piece, pos_piece = args
            scores = jnp.einsum('qhd,khd->hqk', q_piece, k_rot) * scale
            visible = positions[None, None, :] <= pos_piece[None, :, None]
            scores = jnp.where(visible, scores, NEGATIVE)
            top = lax.optimization_barrier(jnp.max(scores, axis=-1, keepdims=True))
            total = lax.optimization_barrier(jnp.sum(jnp.where(visible, jnp.exp(scores - top), 0.0), axis=-1, keepdims=True))
            log_total = top + jnp.log(total)
            weights = rounded(jnp.where(visible, jnp.exp(scores - log_total), 0.0))
            return (jnp.einsum('hqk,khd->qhd', weights, v_heads), log_total[..., 0])
        attended, log_totals = lax.map(attend, (q_parts, pos_parts))
        attended = attended.reshape(LEN, H, HD)
        attn_bf = attended.reshape(LEN, D).astype(jnp.bfloat16)
        attn_proj = jnp.dot(attn_bf, w_output, preferred_element_type=jnp.float32)
        a_normed, a_inverse = rms_forward(attn_proj, g_attn)
        hidden_state = seq_tokens.astype(jnp.float32) + a_normed
        hidden_bf = hidden_state.astype(jnp.bfloat16)
        gate = jnp.dot(hidden_bf, w_gate, preferred_element_type=jnp.float32)
        up_vals = jnp.dot(hidden_bf, w_up, preferred_element_type=jnp.float32)
        sigma = jax.nn.sigmoid(gate)
        activation = (gate * sigma * up_vals).astype(jnp.bfloat16)
        mixed = jnp.dot(activation, w_down, preferred_element_type=jnp.float32)
        m_normed, m_inverse = rms_forward(mixed, g_feed)
        output = hidden_state + m_normed
        upstream_f = upstream.astype(jnp.float32)
        d_mixed, d_gfeed = rms_backward(mixed, m_inverse, g_feed, upstream_f)
        d_mixed_bf = d_mixed.astype(jnp.bfloat16)
        grad_down = jnp.dot(activation.T, d_mixed_bf, preferred_element_type=jnp.float32)
        d_act = jnp.dot(d_mixed_bf, w_down.T, preferred_element_type=jnp.float32)
        d_up_bf = (d_act * gate * sigma).astype(jnp.bfloat16)
        d_gate_bf = (d_act * up_vals * sigma * (1.0 + gate * (1.0 - sigma))).astype(jnp.bfloat16)
        grad_gate = jnp.dot(hidden_bf.T, d_gate_bf, preferred_element_type=jnp.float32)
        grad_up = jnp.dot(hidden_bf.T, d_up_bf, preferred_element_type=jnp.float32)
        d_hidden = upstream_f + jnp.dot(d_gate_bf, w_gate.T, preferred_element_type=jnp.float32) + jnp.dot(d_up_bf, w_up.T, preferred_element_type=jnp.float32)
        d_attn, d_gattn = rms_backward(attn_proj, a_inverse, g_attn, d_hidden)
        d_attn_bf = d_attn.astype(jnp.bfloat16)
        grad_outproj = jnp.dot(attn_bf.T, d_attn_bf, preferred_element_type=jnp.float32)
        d_heads = jnp.dot(d_attn_bf, w_output.T, preferred_element_type=jnp.float32).reshape(LEN, H, HD)
        deltas = lax.optimization_barrier(jnp.sum(d_heads * attended, axis=-1)).T
        delta_parts = deltas.reshape(H, block_count, q_block).transpose(1, 0, 2)
        d_heads_r = rounded(d_heads)
        dout_parts = d_heads_r.reshape(block_count, q_block, H, HD)

        def backward(state, args):
            dk_acc, dv_acc = state
            q_piece, pos_piece, dout_piece, lse_piece, delta_piece = args
            scores = jnp.einsum('qhd,khd->hqk', q_piece, k_rot) * scale
            visible = positions[None, None, :] <= pos_piece[None, :, None]
            probs = jnp.where(visible, jnp.exp(scores - lse_piece[..., None]), 0.0)
            d_probs = jnp.einsum('qhd,khd->hqk', dout_piece, v_heads)
            d_scores = rounded(probs * (d_probs - delta_piece[..., None]))
            dq_piece = jnp.einsum('hqk,khd->qhd', d_scores, k_rot) * scale
            dk_acc = dk_acc + jnp.einsum('hqk,qhd->khd', d_scores, q_piece) * scale
            dv_acc = dv_acc + jnp.einsum('hqk,qhd->khd', rounded(probs), dout_piece)
            return ((dk_acc, dv_acc), dq_piece)
        zeros_heads = jnp.zeros((LEN, H, HD), jnp.float32)
        (d_krot, d_values), d_qrot = lax.scan(backward, (zeros_heads, zeros_heads), (q_parts, pos_parts, dout_parts, log_totals, delta_parts))
        d_qrot = d_qrot.reshape(LEN, H, HD)
        dq_normed = unrotate(d_qrot, cosine, sine).reshape(LEN, D)
        dk_normed = unrotate(d_krot, cosine, sine).reshape(LEN, D)
        d_queries, d_gquery = rms_backward(queries, q_inverse, g_query, dq_normed)
        d_keys, d_gkey = rms_backward(keys_raw, k_inverse, g_key, dk_normed)
        dq_bf = d_queries.astype(jnp.bfloat16)
        dk_bf = d_keys.astype(jnp.bfloat16)
        dv_bf = d_values.reshape(LEN, D).astype(jnp.bfloat16)
        grad_q = jnp.dot(seq_tokens.T, dq_bf, preferred_element_type=jnp.float32)
        grad_k = jnp.dot(seq_tokens.T, dk_bf, preferred_element_type=jnp.float32)
        grad_v = jnp.dot(seq_tokens.T, dv_bf, preferred_element_type=jnp.float32)
        d_input = d_hidden + jnp.dot(dq_bf, w_query.T, preferred_element_type=jnp.float32) + jnp.dot(dk_bf, w_key.T, preferred_element_type=jnp.float32) + jnp.dot(dv_bf, w_value.T, preferred_element_type=jnp.float32)
        fresh = (grad_q, grad_k, grad_v, grad_outproj, grad_gate, grad_up, grad_down, d_gquery, d_gkey, d_gattn, d_gfeed)
        carry = tuple((old + new for old, new in zip(carry, fresh)))
        return (carry, (output, d_input))
    init = (jnp.zeros((D, D), jnp.float32), jnp.zeros((D, D), jnp.float32), jnp.zeros((D, D), jnp.float32), jnp.zeros((D, D), jnp.float32), jnp.zeros((D, FF), jnp.float32), jnp.zeros((D, FF), jnp.float32), jnp.zeros((FF, D), jnp.float32), jnp.zeros((D,), jnp.float32), jnp.zeros((D,), jnp.float32), jnp.zeros((D,), jnp.float32), jnp.zeros((D,), jnp.float32))
    totals, (output, grad_input) = lax.scan(one_sequence, init, (tokens, cotangent, block_order))
    return (output, grad_input, totals[0], totals[1], totals[2], totals[3], totals[4], totals[5], totals[6], totals[7], totals[8], totals[9], totals[10])
```

```python
import functools

import jax
import jax.numpy as jnp
from jax import lax
from jax.experimental import pallas as pl
from jax.experimental.pallas import tpu as pltpu
from jax.sharding import PartitionSpec as P

HD = 128


EPS = 1e-06
THETA = 500000.0
NEGATIVE = -1e30


def full_width(value):
    return lax.all_gather(value, "tp", axis=2, tiled=True)


def share(value):
    return lax.psum_scatter(value, "tp", scatter_dimension=2, tiled=True)


def tp_total(values):
    return lax.psum(values, "tp")


def rotary_tables(positions):
    half_dim = HD // 2
    frequency = THETA ** (-2.0 * jnp.arange(half_dim, dtype=jnp.float32) / HD)
    angles = positions.astype(jnp.float32)[..., None] * frequency
    return (jnp.cos(angles)[..., None, :], jnp.sin(angles)[..., None, :])


def rotate(value, cosine, sine):
    half_dim = value.shape[-1] // 2
    first, second = (value[..., :half_dim], value[..., half_dim:])
    return jnp.concatenate(
        [first * cosine - second * sine, second * cosine + first * sine], axis=-1
    )


def unrotate(grad, cosine, sine):
    half_dim = grad.shape[-1] // 2
    first, second = (grad[..., :half_dim], grad[..., half_dim:])
    return jnp.concatenate(
        [first * cosine + second * sine, second * cosine - first * sine], axis=-1
    )


def key_positions(block_order, start, count, block_len):
    slots = start + jnp.arange(count, dtype=jnp.int32)
    owner = slots // block_len
    ranks = jnp.arange(block_order.shape[1], dtype=jnp.int32)
    chosen = jnp.sum(
        jnp.where(owner[None, :, None] == ranks[None, None, :], block_order[:, None, :], 0), axis=2
    )
    return chosen * block_len + slots % block_len


def span_of():
    return 512


def shards(
    tokens,
    w_query,
    w_key,
    w_value,
    w_output,
    w_gate,
    w_up,
    w_down,
    gain_query,
    gain_key,
    gain_attention,
    gain_feedforward,
    block_order,
    cotangent,
):
    gathered = (
        lax.all_gather(w_query, "ctx", axis=0, tiled=True),
        lax.all_gather(w_key, "ctx", axis=0, tiled=True),
        lax.all_gather(w_value, "ctx", axis=0, tiled=True),
        lax.all_gather(w_output, "ctx", axis=1, tiled=True),
        lax.all_gather(w_gate, "ctx", axis=0, tiled=True),
        lax.all_gather(w_up, "ctx", axis=0, tiled=True),
        lax.all_gather(w_down, "ctx", axis=1, tiled=True),
        lax.all_gather(gain_query, "ctx", axis=0, tiled=True),
        lax.all_gather(gain_key, "ctx", axis=0, tiled=True),
        lax.all_gather(gain_attention, "ctx", axis=0, tiled=True),
        lax.all_gather(gain_feedforward, "ctx", axis=0, tiled=True),
    )
    wq_full, wk_full, wv_full, wo_full, wg_full, wu_full, wd_full = gathered[:7]
    g_query = gathered[7].astype(jnp.float32)
    g_key = gathered[8].astype(jnp.float32)
    g_attn = gathered[9].astype(jnp.float32)
    g_feed = gathered[10].astype(jnp.float32)
    seq_count, block_len, local_width = tokens.shape
    row_count = seq_count * block_len
    scale = HD ** (-0.5)
    tok_full = full_width(tokens)
    tok_rows = tok_full.reshape(row_count, -1)
    width = tok_rows.shape[1]
    queries = jnp.dot(tok_rows, wq_full, preferred_element_type=jnp.float32)
    keys_raw = jnp.dot(tok_rows, wk_full, preferred_element_type=jnp.float32)
    values_raw = jnp.dot(tok_rows, wv_full, preferred_element_type=jnp.float32)
    head_width = queries.shape[1]
    head_count = head_width // HD
    q_squares, k_squares = tp_total(
        (jnp.sum(queries * queries, axis=1), jnp.sum(keys_raw * keys_raw, axis=1))
    )
    q_inverse = lax.rsqrt(q_squares / width + EPS)[:, None]
    k_inverse = lax.rsqrt(k_squares / width + EPS)[:, None]
    q_normed = queries * q_inverse * g_query
    k_normed = keys_raw * k_inverse * g_key
    ctx_rank = lax.axis_index("ctx")
    ranks = jnp.arange(block_order.shape[1], dtype=jnp.int32)
    my_block = jnp.sum(jnp.where(ranks[None, :] == ctx_rank, block_order, 0), axis=1)
    q_pos = my_block[:, None] * block_len + jnp.arange(block_len, dtype=jnp.int32)[None, :]
    cosine, sine = rotary_tables(q_pos)
    q_rot = rotate(q_normed.reshape(seq_count, block_len, head_count, HD), cosine, sine).astype(
        jnp.bfloat16
    )
    k_rot = rotate(k_normed.reshape(seq_count, block_len, head_count, HD), cosine, sine).astype(
        jnp.bfloat16
    )
    k_flat = k_rot.reshape(seq_count, block_len, head_width)
    v_flat = values_raw.astype(jnp.bfloat16).reshape(seq_count, block_len, head_width)

    def stat_block(state, key_piece, k_pos):
        run_max, run_sum = state
        scores = (
            jnp.einsum("sqhd,skhd->shqk", q_rot, key_piece, preferred_element_type=jnp.float32)
            * scale
        )
        visible = k_pos[:, None, None, :] <= q_pos[:, None, :, None]
        scores = jnp.where(visible, scores, NEGATIVE)
        new_max = jnp.maximum(run_max, jnp.max(scores, axis=-1))
        weights = jnp.where(visible, jnp.exp(scores - new_max[..., None]), 0.0)
        run_sum = run_sum * jnp.exp(run_max - new_max) + jnp.sum(weights, axis=-1)
        return (new_max, run_sum)

    init = (
        jnp.full((seq_count, head_count, block_len), NEGATIVE, jnp.float32),
        jnp.zeros((seq_count, head_count, block_len), jnp.float32),
    )
    fold_key_all = lax.all_gather(k_flat, "ctx", axis=1, tiled=True)
    count = fold_key_all.shape[1]
    span = span_of()

    def fold_one_span(step_index, inner):
        offset = step_index * span
        key_piece = lax.dynamic_slice_in_dim(fold_key_all, offset, span, 1).reshape(
            seq_count, span, head_count, HD
        )
        k_pos = key_positions(block_order, offset, span, block_len)
        return stat_block(inner, key_piece, k_pos)

    run_max, run_sum = lax.fori_loop(0, count // span, fold_one_span, init)
    key_all, val_all = (
        lax.all_gather(k_flat, "ctx", axis=1, tiled=True),
        lax.all_gather(v_flat, "ctx", axis=1, tiled=True),
    )
    log_total = run_max + jnp.log(run_sum)
    total_len = key_all.shape[1]
    total_span = span_of()

    def value_span(step_index, acc):
        offset = step_index * total_span
        key_piece = lax.dynamic_slice_in_dim(key_all, offset, total_span, 1).reshape(
            seq_count, total_span, head_count, HD
        )
        val_piece = lax.dynamic_slice_in_dim(val_all, offset, total_span, 1).reshape(
            seq_count, total_span, head_count, HD
        )
        k_pos = key_positions(block_order, offset, total_span, block_len)
        scores = (
            jnp.einsum("sqhd,skhd->shqk", q_rot, key_piece, preferred_element_type=jnp.float32)
            * scale
        )
        visible = k_pos[:, None, None, :] <= q_pos[:, None, :, None]
        weights = jnp.where(visible, jnp.exp(scores - log_total[..., None]), 0.0).astype(
            jnp.bfloat16
        )
        return acc + jnp.einsum(
            "shqk,skhd->sqhd", weights, val_piece, preferred_element_type=jnp.float32
        )

    attended = lax.fori_loop(
        0,
        total_len // total_span,
        value_span,
        jnp.zeros((seq_count, block_len, head_count, HD), jnp.float32),
    )
    attn_bf = attended.reshape(row_count, head_width).astype(jnp.bfloat16)
    attn_proj = share(
        jnp.dot(attn_bf, wo_full, preferred_element_type=jnp.float32).reshape(
            seq_count, block_len, -1
        )
    )
    (a_squares,) = tp_total((jnp.sum(attn_proj * attn_proj, axis=2),))
    a_inverse = lax.rsqrt(a_squares / width + EPS)[..., None]
    hidden_state = tokens.astype(jnp.float32) + attn_proj * a_inverse * g_attn
    hidden_rows = full_width(hidden_state.astype(jnp.bfloat16)).reshape(row_count, -1)
    gate = jnp.dot(hidden_rows, wg_full, preferred_element_type=jnp.float32)
    up_vals = jnp.dot(hidden_rows, wu_full, preferred_element_type=jnp.float32)
    sigma = jax.nn.sigmoid(gate)
    activation = (gate * sigma * up_vals).astype(jnp.bfloat16)
    mixed = share(
        jnp.dot(activation, wd_full, preferred_element_type=jnp.float32).reshape(
            seq_count, block_len, -1
        )
    )
    (m_squares,) = tp_total((jnp.sum(mixed * mixed, axis=2),))
    m_inverse = lax.rsqrt(m_squares / width + EPS)[..., None]
    output = hidden_state + mixed * m_inverse * g_feed
    upstream = cotangent.astype(jnp.float32)
    (m_dots,) = tp_total((jnp.sum(g_feed * upstream * mixed, axis=2),))
    d_mixed = m_inverse * (g_feed * upstream) - mixed * m_inverse**3 * (m_dots / width)[..., None]
    d_gfeed = jnp.sum(upstream * mixed * m_inverse, axis=(0, 1))
    d_mixed_rows = full_width(d_mixed.astype(jnp.bfloat16)).reshape(row_count, -1)
    grad_down = jnp.dot(activation.T, d_mixed_rows, preferred_element_type=jnp.float32)
    d_act = jnp.dot(d_mixed_rows, wd_full.T, preferred_element_type=jnp.float32)
    d_up_bf = (d_act * gate * sigma).astype(jnp.bfloat16)
    d_gate_bf = (d_act * up_vals * sigma * (1.0 + gate * (1.0 - sigma))).astype(jnp.bfloat16)
    grad_gate = jnp.dot(hidden_rows.T, d_gate_bf, preferred_element_type=jnp.float32)
    grad_up = jnp.dot(hidden_rows.T, d_up_bf, preferred_element_type=jnp.float32)
    back_ff = jnp.dot(d_gate_bf, wg_full.T, preferred_element_type=jnp.float32) + jnp.dot(
        d_up_bf, wu_full.T, preferred_element_type=jnp.float32
    )
    d_hidden = upstream + share(back_ff.reshape(seq_count, block_len, -1))
    (a_dots,) = tp_total((jnp.sum(g_attn * d_hidden * attn_proj, axis=2),))
    d_attn = (
        a_inverse * (g_attn * d_hidden) - attn_proj * a_inverse**3 * (a_dots / width)[..., None]
    )
    d_gattn = jnp.sum(d_hidden * attn_proj * a_inverse, axis=(0, 1))
    d_attn_rows = full_width(d_attn.astype(jnp.bfloat16)).reshape(row_count, -1)
    grad_outproj = jnp.dot(attn_bf.T, d_attn_rows, preferred_element_type=jnp.float32)
    d_heads = jnp.dot(d_attn_rows, wo_full.T, preferred_element_type=jnp.float32).reshape(
        seq_count, block_len, head_count, HD
    )
    deltas = jnp.sum(d_heads * attended, axis=3).transpose(0, 2, 1)
    d_heads_bf = d_heads.astype(jnp.bfloat16)

    def grad_block(key_piece, val_piece, k_pos):
        scores = (
            jnp.einsum("sqhd,skhd->shqk", q_rot, key_piece, preferred_element_type=jnp.float32)
            * scale
        )
        visible = k_pos[:, None, None, :] <= q_pos[:, None, :, None]
        probs = jnp.where(visible, jnp.exp(scores - log_total[..., None]), 0.0)
        d_probs = jnp.einsum(
            "sqhd,skhd->shqk", d_heads_bf, val_piece, preferred_element_type=jnp.float32
        )
        d_scores = (probs * (d_probs - deltas[..., None])).astype(jnp.bfloat16)
        return (probs, d_scores)

    def query_span(step_index, acc):
        offset = step_index * total_span
        key_piece = lax.dynamic_slice_in_dim(key_all, offset, total_span, 1).reshape(
            seq_count, total_span, head_count, HD
        )
        val_piece = lax.dynamic_slice_in_dim(val_all, offset, total_span, 1).reshape(
            seq_count, total_span, head_count, HD
        )
        k_pos = key_positions(block_order, offset, total_span, block_len)
        probs, d_scores = grad_block(key_piece, val_piece, k_pos)
        return (
            acc
            + jnp.einsum("shqk,skhd->sqhd", d_scores, key_piece, preferred_element_type=jnp.float32)
            * scale
        )

    d_qrot = lax.fori_loop(
        0,
        total_len // total_span,
        query_span,
        jnp.zeros((seq_count, block_len, head_count, HD), jnp.float32),
    )
    count = block_len * lax.axis_size("ctx")
    key_span = span_of()

    def key_one_span(step_index, buffer):
        offset = step_index * key_span
        key_piece = lax.dynamic_slice_in_dim(key_all, offset, key_span, 1).reshape(
            seq_count, key_span, head_count, HD
        )
        val_piece = lax.dynamic_slice_in_dim(val_all, offset, key_span, 1).reshape(
            seq_count, key_span, head_count, HD
        )
        k_pos = key_positions(block_order, offset, key_span, block_len)
        probs, d_scores = grad_block(key_piece, val_piece, k_pos)
        d_keyp = (
            jnp.einsum("shqk,sqhd->skhd", d_scores, q_rot, preferred_element_type=jnp.float32)
            * scale
        )
        d_valp = jnp.einsum(
            "shqk,sqhd->skhd",
            probs.astype(jnp.bfloat16),
            d_heads_bf,
            preferred_element_type=jnp.float32,
        )
        both = jnp.concatenate(
            [
                d_keyp.reshape(seq_count, key_span, head_width),
                d_valp.reshape(seq_count, key_span, head_width),
            ],
            axis=2,
        )
        return lax.dynamic_update_slice_in_dim(buffer, both.transpose(1, 0, 2), offset, 0)

    key_sums = (
        lax.psum_scatter(
            lax.fori_loop(
                0,
                count // key_span,
                key_one_span,
                jnp.zeros((count, seq_count, 2 * head_width), jnp.float32),
            ).astype(jnp.bfloat16),
            "ctx",
            scatter_dimension=0,
            tiled=True,
        )
        .astype(jnp.float32)
        .transpose(1, 0, 2)
    )
    d_krot = key_sums[..., :head_width].reshape(seq_count, block_len, head_count, HD)
    d_values = key_sums[..., head_width:].reshape(row_count, head_width)
    dq_normed = unrotate(d_qrot, cosine, sine).reshape(row_count, head_width)
    dk_normed = unrotate(d_krot, cosine, sine).reshape(row_count, head_width)
    q_dots, k_dots = tp_total(
        (
            jnp.sum(g_query * dq_normed * queries, axis=1),
            jnp.sum(g_key * dk_normed * keys_raw, axis=1),
        )
    )
    d_queries = (
        q_inverse * (g_query * dq_normed) - queries * q_inverse**3 * (q_dots / width)[:, None]
    )
    d_keys = k_inverse * (g_key * dk_normed) - keys_raw * k_inverse**3 * (k_dots / width)[:, None]
    d_gquery = jnp.sum(dq_normed * queries * q_inverse, axis=0)
    d_gkey = jnp.sum(dk_normed * keys_raw * k_inverse, axis=0)
    dq_bf = d_queries.astype(jnp.bfloat16)
    dk_bf = d_keys.astype(jnp.bfloat16)
    dv_bf = d_values.astype(jnp.bfloat16)
    grad_q = jnp.dot(tok_rows.T, dq_bf, preferred_element_type=jnp.float32)
    grad_k = jnp.dot(tok_rows.T, dk_bf, preferred_element_type=jnp.float32)
    grad_v = jnp.dot(tok_rows.T, dv_bf, preferred_element_type=jnp.float32)
    back_attn = (
        jnp.dot(dq_bf, wq_full.T, preferred_element_type=jnp.float32)
        + jnp.dot(dk_bf, wk_full.T, preferred_element_type=jnp.float32)
        + jnp.dot(dv_bf, wv_full.T, preferred_element_type=jnp.float32)
    )
    grad_input = d_hidden + share(back_attn.reshape(seq_count, block_len, -1))
    summed = (
        lax.psum_scatter(
            grad_q.astype(jnp.bfloat16), "ctx", scatter_dimension=0, tiled=True
        ).astype(jnp.float32),
        lax.psum_scatter(
            grad_k.astype(jnp.bfloat16), "ctx", scatter_dimension=0, tiled=True
        ).astype(jnp.float32),
        lax.psum_scatter(
            grad_v.astype(jnp.bfloat16), "ctx", scatter_dimension=0, tiled=True
        ).astype(jnp.float32),
        lax.psum_scatter(
            grad_outproj.astype(jnp.bfloat16), "ctx", scatter_dimension=1, tiled=True
        ).astype(jnp.float32),
        lax.psum_scatter(
            grad_gate.astype(jnp.bfloat16), "ctx", scatter_dimension=0, tiled=True
        ).astype(jnp.float32),
        lax.psum_scatter(
            grad_up.astype(jnp.bfloat16), "ctx", scatter_dimension=0, tiled=True
        ).astype(jnp.float32),
        lax.psum_scatter(
            grad_down.astype(jnp.bfloat16), "ctx", scatter_dimension=1, tiled=True
        ).astype(jnp.float32),
        lax.psum_scatter(
            d_gquery.astype(jnp.bfloat16), "ctx", scatter_dimension=0, tiled=True
        ).astype(jnp.float32),
        lax.psum_scatter(
            d_gkey.astype(jnp.bfloat16), "ctx", scatter_dimension=0, tiled=True
        ).astype(jnp.float32),
        lax.psum_scatter(
            d_gattn.astype(jnp.bfloat16), "ctx", scatter_dimension=0, tiled=True
        ).astype(jnp.float32),
        lax.psum_scatter(
            d_gfeed.astype(jnp.bfloat16), "ctx", scatter_dimension=0, tiled=True
        ).astype(jnp.float32),
    )
    return (
        output,
        grad_input,
        summed[0],
        summed[1],
        summed[2],
        summed[3],
        summed[4],
        summed[5],
        summed[6],
        summed[7],
        summed[8],
        summed[9],
        summed[10],
    )


MESH = pl.DeviceIdType.MESH
NT = (((1,), (1,)), ((), ()))
TN = (((0,), (0,)), ((), ()))
F32 = jnp.float32
BF16 = jnp.bfloat16
COLS = (0, 1, 2, 4, 5)


def layer_kernel(dims, *refs):
    (chips, tps, seqs, blk, width, head_w, ff_w) = dims
    rows = seqs * blk
    both = 2 * rows
    share_rows = rows // tps
    feats = width // tps
    heads = head_w // HD
    slab = width // (2 * chips)
    halves = (head_w, head_w, head_w, head_w, ff_w, ff_w, ff_w)
    total = 2 * chips * blk
    scale = HD ** (-0.5)
    it = iter(refs)

    def take(n):
        return [next(it) for _ in range(n)]

    (tok_in, cot_in) = take(2)
    w_in = take(7)
    (gtile, cosf, sinf, pos_row, pos_col) = take(5)
    (out_ref, gin_ref, ggain_ref) = take(3)
    rx_g = take(7)
    w = take(7)
    (tok, tok_t, hid, hid_t, dmix, dattn) = take(6)
    (lin, fac, act, act_t, dgate, dup) = take(6)
    (st_p, rx_p, st_z, rx_z, rx_f) = take(5)
    (q_raw, k_raw, qkv, qa, probs, att_f, att_st, att, att_t) = take(9)
    (dh, d_o, dk_acc, dv_acc, dqkv_st, dqkv) = take(6)
    (sq_own, sq_rx, inv_q, inv_k) = take(4)
    (cot, proj, hstate, mixed, dhid, stage) = take(6)
    (gbuf, gall, gfull, gqk, gg_row, gg_rx1, gg_mid, gg_rx2) = take(8)
    (ws, wr, gs, gr) = take(4)
    (zs, zr, ps, pr) = take(4)
    (rps, rpr, rzs, rzr) = take(4)
    (ms, mr) = take(2)
    (ss, sr) = take(2)
    (as_, ar) = take(2)
    (loc,) = take(1)

    ctx = lax.axis_index("ctx")
    z = lax.axis_index("tp")
    c = ctx // 2
    k = ctx % 2
    ok = 1 - k
    partner = c * 2 + ok

    def zp(i):
        return (z + i) % tps

    def chip(i):
        return (c + i) % chips

    def ds(start, size):
        return pl.ds(pl.multiple_of(start, size), size)

    def remote(src, dst, ssem, rsem, to_ctx, to_z):
        return pltpu.make_async_remote_copy(
            src_ref=src,
            dst_ref=dst,
            send_sem=ssem,
            recv_sem=rsem,
            device_id=(to_ctx, to_z),
            device_id_type=MESH,
        )

    peers = [(chip(i) * 2 + (k + d) % 2, z) for i in range(chips) for d in range(2) if i or d]
    peers += [(ctx, zp(i)) for i in range(1, tps)]
    peers += [(partner, zp(i)) for i in range(1, tps)]
    barrier = pltpu.get_barrier_semaphore()
    for peer in peers:
        pl.semaphore_signal(barrier, inc=1, device_id=peer, device_id_type=MESH)

    pending = []

    def go(copy):
        copy.start()
        pending.append(copy)
        return copy

    def w_copy(m, i, d):
        core = (k + d) % 2
        half = halves[m]
        if m in COLS:
            src = w_in[m].at[:, ds(core * half, half)]
            dst = w[m].at[ds(ctx * slab, slab), :]
        else:
            src = w_in[m].at[ds(core * half, half), :]
            dst = w[m].at[:, ds(ctx * slab, slab)]
        if i == 0 and d == 0:
            return pltpu.make_async_copy(src, dst, loc.at[m])
        return remote(src, dst, ws.at[m, 2 * i + d], wr.at[m, 2 * i + d], chip(i) * 2 + core, z)

    slots = [(i, d) for i in range(chips) for d in range(2)]
    w_live = {}

    def send_w(m):
        for i, d in slots:
            copy = w_copy(m, i, d)
            copy.start()
            w_live[m, i, d] = copy
            if i or d:
                pending.append(copy)

    def wait_w(m, i, d):
        copy = w_live[m, i, d]
        if i or d:
            copy.wait_recv()
        else:
            copy.wait()

    def send_g(m, chips_from=0, chips_to=chips):
        half = halves[m]
        for i in range(chips_from, chips_to):
            for d in range(2):
                to = chip(i) * 2 + (k + d) % 2
                if m in COLS:
                    src = w[m].at[ds(to * slab, slab), :]
                    dst = rx_g[m].at[i, :, ds(k * half, half)]
                else:
                    src = w[m].at[:, ds(to * slab, slab)]
                    dst = rx_g[m].at[i, ds(k * half, half), :]
                if i or d:
                    copy = remote(src, dst, gs.at[m, 2 * i + d], gr.at[m, 2 * i + d], to, z)
                    go(copy)
                    g_live.append(copy)
                else:
                    copy = pltpu.make_async_copy(src, dst, loc.at[8 + m])
                    copy.start()
                    g_own.append(copy)

    g_live = []
    g_own = []

    own_tok = pltpu.make_async_copy(tok_in, tok.at[ds(k * rows, rows), ds(z * feats, feats)], loc.at[16])
    own_tok.start()
    own_cot = pltpu.make_async_copy(cot_in.at[ds(z * share_rows, share_rows), :], cot.at[:, ds(z * feats, feats)], loc.at[17])
    own_cot.start()
    own_gain = pltpu.make_async_copy(gtile, gbuf.at[ctx], loc.at[18])
    own_gain.start()
    pl.semaphore_wait(barrier, len(peers))

    tok_z = []
    for i in range(1, tps):
        tok_z.append(go(remote(tok_in, tok.at[ds(k * rows, rows), ds(z * feats, feats)], zs.at[0, i - 1], zr.at[0, i - 1], ctx, zp(i))))
    tok_p = [go(remote(tok_in, tok.at[ds(k * rows, rows), ds(z * feats, feats)], ps.at[0, 0], pr.at[0, 0], partner, z))]
    gain1 = []
    n = 0
    for i, d in slots:
        if i or d:
            gain1.append(go(remote(gtile, gbuf.at[ctx], ms.at[0, n], mr.at[0, n], chip(i) * 2 + (k + d) % 2, z)))
            n += 1
    cot_z = []
    for i in range(1, tps):
        cot_z.append(go(remote(cot_in.at[ds(zp(i) * share_rows, share_rows), :], cot.at[:, ds(z * feats, feats)], ms.at[1, i - 1], mr.at[1, i - 1], ctx, zp(i))))
    for m in (0, 1, 2, 3):
        send_w(m)

    own_gain.wait()
    for copy in gain1:
        copy.wait_recv()
    own_gain2 = pltpu.make_async_copy(gbuf, gall.at[z], loc.at[19])
    own_gain2.start()
    gain2 = []
    for i in range(1, tps):
        gain2.append(go(remote(gbuf, gall.at[z], ms.at[2, i - 1], mr.at[2, i - 1], ctx, zp(i))))
    for r in range(2):
        pieces = [gbuf[4 * k + 2 * m, r : r + 1, :] + gbuf[4 * k + 2 * m + 1, r : r + 1, :] for m in range(head_w // 128)]
        gqk[r : r + 1, :] = jnp.concatenate(pieces, axis=1)

    own_tok.wait()
    for i in range(1, tps):
        tok_z[i - 1].wait_recv()
        part = tok.at[ds(k * rows, rows), ds(((z - i) % tps) * feats, feats)]
        tok_p.append(go(remote(part, part, ps.at[0, i], pr.at[0, i], partner, z)))
    own_gain2.wait()
    for copy in gain2:
        copy.wait_recv()
    for r in range(2):
        pieces = []
        for zz in range(tps):
            for m in range(chips):
                pieces.append(gall[zz, 2 * m, 2 + r : 3 + r, :] + gall[zz, 2 * m + 1, 2 + r : 3 + r, :])
        gfull[r : r + 1, :] = jnp.concatenate(pieces, axis=1)
    for copy in tok_p:
        copy.wait_recv()

    def row_of(value):
        folded = value[:, :128]
        for h in range(1, heads):
            folded = folded + value[:, h * 128 : (h + 1) * 128]
        return jnp.sum(jnp.transpose(folded), axis=0, keepdims=True)

    def column_of(row):
        return jnp.transpose(jnp.broadcast_to(row, (128, both)))

    def totals(idx):
        copies = []
        n = 0
        for i in range(tps):
            for d in range(2):
                if i or d:
                    to = ctx if d == 0 else partner
                    copies.append(go(remote(sq_own.at[idx], sq_rx.at[idx, n], ss.at[idx, n], sr.at[idx, n], to, zp(i))))
                    n += 1
        total = sq_own[idx]
        for j, copy in enumerate(copies):
            copy.wait_recv()
            total = total + sq_rx[idx, j]
        return total

    for m in (0, 1, 2):
        for i, d in slots:
            wait_w(m, i, d)
        value = jnp.dot(tok[...], w[m][...], preferred_element_type=F32)
        if m == 0:
            q_raw[...] = value
            sq_own[0, 0:1, :] = row_of(value * value)
        elif m == 1:
            k_raw[...] = value
            sq_own[0, 1:2, :] = row_of(value * value)
            squares = None
        else:
            qkv[2] = value.astype(BF16).reshape(2, seqs, blk, head_w)
    sq_own[0, 2:8, :] = jnp.zeros((6, both), F32)
    squares = totals(0)
    inverse = lax.rsqrt(squares / width + EPS)
    inv_q[...] = column_of(inverse[0:1, :])
    inv_k[...] = column_of(inverse[1:2, :])
    for t, (raw, inv) in enumerate(((q_raw, inv_q), (k_raw, inv_k))):
        for h in range(heads):
            lanes = slice(h * HD, (h + 1) * HD)
            normed = raw[:, lanes] * inv[...] * gqk[t : t + 1, lanes]
            turned = normed * cosf[...] + pltpu.roll(normed, HD // 2, 1) * sinf[...]
            qkv[t, :, :, :, lanes] = turned.astype(BF16).reshape(2, seqs, blk, HD)

    def to_owner(idx, value, owned, stacked):
        copies = []
        for i in range(chips):
            to = chip(i)
            s, h = to // heads, to % heads
            if stacked:
                src = value.at[:, :, s, :, ds(h * HD, HD)]
                dst = owned.at[:, ds(2 * c, 2)]
            else:
                src = value.at[:, s, :, ds(h * HD, HD)]
                dst = owned.at[ds(2 * c, 2)]
            if i:
                copies.append(go(remote(src, dst, as_.at[idx, i - 1], ar.at[idx, i - 1], to * 2 + k, z)))
            else:
                own = pltpu.make_async_copy(src, dst, loc.at[20 + idx])
                own.start()
        return own, copies

    def from_owner(idx, owned, value, stacked):
        s, h = c // heads, c % heads
        copies = []
        for i in range(chips):
            to = chip(i)
            if stacked:
                src = owned.at[:, ds(2 * to, 2)]
                dst = value.at[:, :, s, :, ds(h * HD, HD)]
            else:
                src = owned.at[ds(2 * to, 2)]
                dst = value.at[:, s, :, ds(h * HD, HD)]
            if i:
                copies.append(go(remote(src, dst, as_.at[idx, i - 1], ar.at[idx, i - 1], to * 2 + k, z)))
            else:
                own = pltpu.make_async_copy(src, dst, loc.at[20 + idx])
                own.start()
        return own, copies

    def arrive(pair):
        own, copies = pair
        own.wait()
        for copy in copies:
            copy.wait_recv()

    arrive(to_owner(0, qkv, qa, True))
    step = 2 * blk

    def attend(i, carry):
        here = ds(i * step, step)
        q = qa[0, pl.ds(2 * i, 2)].reshape(step, HD)
        s = lax.dot_general(q, qa[1].reshape(total, HD), NT, preferred_element_type=F32) * scale
        visible = pos_row[0:1, :] <= pos_col[here, 0:1]
        s = jnp.where(visible, s, NEGATIVE)
        top = jnp.max(s, axis=1, keepdims=True)
        e = jnp.where(visible, jnp.exp(s - top), 0.0)
        p = (e * (1.0 / jnp.sum(e, axis=1, keepdims=True))).astype(BF16)
        probs[here, :] = p
        o = jnp.dot(p, qa[2].reshape(total, HD), preferred_element_type=F32)
        att_f[here, :] = o
        att_st[pl.ds(2 * i, 2)] = o.astype(BF16).reshape(2, blk, HD)
        return carry

    lax.fori_loop(0, chips, attend, 0)
    back = from_owner(1, att_st, att, False)
    for m in (4, 5, 6):
        send_w(m)
    for s in range(width // 256):
        tok_t[s * 256 : (s + 1) * 256, :] = jnp.transpose(tok[:, s * 256 : (s + 1) * 256])
    arrive(back)
    for i, d in slots:
        wait_w(3, i, d)

    cw = feats
    rs_live = {}

    def rp_copy(idx, i, off):
        return remote(st_p.at[:, ds(off, cw)], rx_p.at[idx % 2, :, ds(off, cw)], rps.at[idx, i], rpr.at[idx, i], partner, z)

    def rz_copy(idx, i, j, off):
        return remote(
            st_z.at[ds(zp(j) * share_rows, share_rows), ds(off, cw)],
            rx_z.at[idx % 2, j - 1, :, ds(off, cw)],
            rzs.at[idx, i, j - 1],
            rzr.at[idx, i, j - 1],
            ctx,
            zp(j),
        )

    def reduce_rows(idx, partial, offset, before=None):
        def one(i):
            off = offset(i)
            if before is not None:
                before(i)
            st_p[:, ds(off, cw)] = partial(ok, off).astype(BF16)
            rp_copy(idx, i, off).start()
            mine = partial(k, off)
            rp_copy(idx, i, off).wait_recv()
            st_z[:, ds(off, cw)] = (mine + rx_p[idx % 2, :, ds(off, cw)].astype(F32)).astype(BF16)
            for j in range(1, tps):
                rz_copy(idx, i, j, off).start()

        def finish(i):
            off = offset(i)
            for j in range(1, tps):
                rz_copy(idx, i, j, off).wait_recv()
                rz_copy(idx, i, j, off).wait_send()
            rp_copy(idx, i, off).wait_send()

        if before is None:
            lax.fori_loop(0, tps, lambda i, x: (one(i), x)[1], 0)
        else:
            for i in range(tps):
                one(i)
        lax.fori_loop(0, tps, lambda i, x: (finish(i), x)[1], 0)
        mine = st_z[ds(z * share_rows, share_rows), :].astype(F32)
        for j in range(tps - 1):
            mine = mine + rx_z[idx % 2, j].astype(F32)
        return mine

    def straight(i):
        return i * cw

    def mean_of(value):
        return jnp.sum(value, axis=1, keepdims=True) / width

    def spread(idx, buf):
        mine = buf.at[ds(k * rows + z * share_rows, share_rows), :]
        along = [go(remote(mine, mine, zs.at[idx, i - 1], zr.at[idx, i - 1], ctx, zp(i))) for i in range(1, tps)]
        across = [go(remote(mine, mine, ps.at[idx, 0], pr.at[idx, 0], partner, z))]

        def finish():
            for i in range(1, tps):
                along[i - 1].wait_recv()
                part = buf.at[ds(k * rows + ((z - i) % tps) * share_rows, share_rows), :]
                across.append(go(remote(part, part, ps.at[idx, i], pr.at[idx, i], partner, z)))
            for copy in across:
                copy.wait_recv()

        return finish

    my_rows = ds(k * rows + z * share_rows, share_rows)
    heads_rows = [None]

    def o_partial(core, off):
        left = att[pl.ds(core, 1)].reshape(rows, head_w)
        return jnp.dot(left, w[3][:, ds(off, cw)], preferred_element_type=F32)

    value = reduce_rows(0, o_partial, straight)
    proj[...] = value
    a_inverse = lax.rsqrt(mean_of(value * value) + EPS)
    state = tok[my_rows, :].astype(F32) + value * a_inverse * gfull[0:1, :]
    hstate[...] = state
    hid[my_rows, :] = state.astype(BF16)
    finish = spread(1, hid)
    own_cot.wait()
    for copy in cot_z:
        copy.wait_recv()
    att_t[...] = jnp.transpose(att[...].reshape(both, head_w))
    finish()

    fw = 256
    for i, d in slots:
        wait_w(4, i, d)

    def gate_step(j, carry):
        here = ds(j * fw, fw)
        lin[:, here] = jnp.dot(hid[...], w[4][:, here], preferred_element_type=F32)
        return carry

    lax.fori_loop(0, ff_w // fw, gate_step, 0)
    for s in range(width // 256):
        hid_t[s * 256 : (s + 1) * 256, :] = jnp.transpose(hid[:, s * 256 : (s + 1) * 256])
    for i, d in slots:
        wait_w(5, i, d)

    def up_step(j, carry):
        here = ds(j * fw, fw)
        up = jnp.dot(hid[...], w[5][:, here], preferred_element_type=F32)
        gate = lin[:, here]
        sigma = jax.nn.sigmoid(gate)
        swish = gate * sigma
        lin[:, here] = swish
        fac[:, here] = up * sigma * (1.0 + gate * (1.0 - sigma))
        value = (swish * up).astype(BF16)
        act[:, here] = value
        act_t[here, :] = jnp.transpose(value)
        return carry

    lax.fori_loop(0, ff_w // fw, up_step, 0)

    def down_partial(core, off):
        return jnp.dot(act[ds(core * rows, rows), :], w[6][:, ds(off, cw)], preferred_element_type=F32)

    def from_chip(i):
        return ((c - i) % chips) * cw

    def down_ready(i):
        wait_w(6, i, 0)
        wait_w(6, i, 1)

    value = reduce_rows(1, down_partial, from_chip, down_ready)
    m_inverse = lax.rsqrt(mean_of(value * value) + EPS)
    scaled = value * m_inverse
    stage[...] = hstate[...] + scaled * gfull[1:2, :]
    for i in range(1, tps):
        go(remote(stage.at[:, ds(zp(i) * feats, feats)], out_ref.at[ds(z * share_rows, share_rows), :], ms.at[3, i - 1], mr.at[3, i - 1], ctx, zp(i)))
    out_z = pending[-(tps - 1) :]
    own_out = pltpu.make_async_copy(stage.at[:, ds(z * feats, feats)], out_ref.at[ds(z * share_rows, share_rows), :], loc.at[24])
    own_out.start()
    upstream = cot[...].astype(F32)
    gained = upstream * gfull[1:2, :]
    gg_row[1:2, :] = jnp.sum(upstream * scaled, axis=0, keepdims=True)
    back_mix = m_inverse * gained - scaled * (m_inverse * m_inverse) * mean_of(gained * value)
    dmix[my_rows, :] = back_mix.astype(BF16)
    spread(2, dmix)()

    def dact_step(j, carry):
        here = ds(j * fw, fw)
        d_act = lax.dot_general(dmix[...], w[6][here, :], NT, preferred_element_type=F32)
        dup[:, here] = (d_act * lin[:, here]).astype(BF16)
        dgate[:, here] = (d_act * fac[:, here]).astype(BF16)
        return carry

    lax.fori_loop(0, ff_w // fw, dact_step, 0)

    def gdown_step(j, carry):
        here = ds(j * fw, fw)
        w[6][:, here] = jnp.dot(act_t[...], dmix[:, here], preferred_element_type=F32).astype(BF16)
        return carry

    lax.fori_loop(0, width // fw, gdown_step, 0)
    send_g(6)

    def ff_partial(core, off):
        here = ds(core * rows, rows)
        return lax.dot_general(dgate[here, :], w[4][ds(off, cw), :], NT, preferred_element_type=F32) + lax.dot_general(
            dup[here, :], w[5][ds(off, cw), :], NT, preferred_element_type=F32
        )

    value = reduce_rows(2, ff_partial, straight) + cot[...].astype(F32)
    dhid[...] = value
    projected = proj[...]
    a_inverse = lax.rsqrt(mean_of(projected * projected) + EPS)
    scaled = projected * a_inverse
    gained = value * gfull[0:1, :]
    gg_row[0:1, :] = jnp.sum(value * scaled, axis=0, keepdims=True)
    gg_row[2:8, :] = jnp.zeros((6, width), F32)
    back_att = a_inverse * gained - scaled * (a_inverse * a_inverse) * mean_of(gained * projected)
    dattn[my_rows, :] = back_att.astype(BF16)
    finish = spread(3, dattn)
    gains_z = []
    for i in range(1, tps):
        gains_z.append(go(remote(gg_row.at[:, ds(zp(i) * feats, feats)], gg_rx1.at[i - 1], ms.at[4, i - 1], mr.at[4, i - 1], ctx, zp(i))))

    def ggate_step(j, carry):
        here = ds(j * fw, fw)
        w[4][:, here] = jnp.dot(hid_t[...], dgate[:, here], preferred_element_type=F32).astype(BF16)
        return carry

    lax.fori_loop(0, ff_w // fw, ggate_step, 0)
    send_g(4, 0, 2)
    finish()

    value = lax.dot_general(dattn[...], w[3][...], NT, preferred_element_type=F32)
    dh[...] = value.astype(BF16).reshape(2, seqs, blk, head_w)
    pair = to_owner(2, dh, d_o, False)
    send_g(4, 2, 3)

    def go_step(j, carry):
        here = ds(j * fw, fw)
        w[3][:, here] = jnp.dot(att_t[...], dattn[:, here], preferred_element_type=F32).astype(BF16)
        return carry

    lax.fori_loop(0, width // fw, go_step, 0)
    arrive(pair)
    dk_acc[...] = jnp.zeros((total, HD), F32)
    dv_acc[...] = jnp.zeros((total, HD), F32)

    def unattend(i, carry):
        here = ds(i * step, step)
        q = qa[0, pl.ds(2 * i, 2)].reshape(step, HD)
        d_out = d_o[pl.ds(2 * i, 2)].reshape(step, HD)
        d_p = lax.dot_general(d_out, qa[2].reshape(total, HD), NT, preferred_element_type=F32)
        delta = jnp.sum(d_out.astype(F32) * att_f[here, :], axis=1, keepdims=True)
        p = probs[here, :]
        d_s = (p.astype(F32) * (d_p - delta)).astype(BF16)
        d_q = jnp.dot(d_s, qa[1].reshape(total, HD), preferred_element_type=F32) * scale
        dqkv_st[0, pl.ds(2 * i, 2)] = d_q.astype(BF16).reshape(2, blk, HD)
        dk_acc[...] += lax.dot_general(d_s, q, TN, preferred_element_type=F32)
        dv_acc[...] += lax.dot_general(p, d_out, TN, preferred_element_type=F32)
        return carry

    lax.fori_loop(0, chips, unattend, 0)
    dqkv_st[1] = (dk_acc[...] * scale).astype(BF16).reshape(2 * chips, blk, HD)
    dqkv_st[2] = dv_acc[...].astype(BF16).reshape(2 * chips, blk, HD)
    pair = from_owner(3, dqkv_st, dqkv, True)

    def gup_step(j, carry):
        here = ds(j * fw, fw)
        w[5][:, here] = jnp.dot(hid_t[...], dup[:, here], preferred_element_type=F32).astype(BF16)
        return carry

    lax.fori_loop(0, ff_w // fw, gup_step, 0)
    send_g(4, 3, 4)
    send_g(5)
    send_g(3)
    arrive(pair)

    gg_mid[...] = jnp.zeros((8, feats), F32)
    for t, (raw, inv) in enumerate(((q_raw, inv_q), (k_raw, inv_k))):
        folded = None
        for h in range(heads):
            lanes = slice(h * HD, (h + 1) * HD)
            turned = dqkv[t, :, :, :, lanes].reshape(both, HD).astype(F32)
            back_rot = turned * cosf[...] - pltpu.roll(turned, HD // 2, 1) * sinf[...]
            plain = raw[:, lanes]
            scaled = plain * inv[...]
            gg_mid[2 + t : 3 + t, pl.ds(pl.multiple_of(k * head_w + h * HD, HD), HD)] = jnp.sum(back_rot * scaled, axis=0, keepdims=True)
            gained = back_rot * gqk[t : t + 1, lanes]
            dqkv[t, :, :, :, lanes] = gained.astype(BF16).reshape(2, seqs, blk, HD)
            term = gained * plain
            folded = term if folded is None else folded + term
        sq_own[1, t : t + 1, :] = jnp.sum(jnp.transpose(folded), axis=0, keepdims=True)
    sq_own[1, 2:8, :] = jnp.zeros((6, both), F32)
    dots = totals(1) / width
    for t, (raw, inv) in enumerate(((q_raw, inv_q), (k_raw, inv_k))):
        spread_dot = column_of(dots[t : t + 1, :])
        for h in range(heads):
            lanes = slice(h * HD, (h + 1) * HD)
            gained = dqkv[t, :, :, :, lanes].reshape(both, HD).astype(F32)
            r = inv[...]
            grad = r * gained - raw[:, lanes] * (r * r * r) * spread_dot
            dqkv[t, :, :, :, lanes] = grad.astype(BF16).reshape(2, seqs, blk, HD)

    def rf_copy(i, off):
        return remote(st_z.at[:, ds(off, cw)], rx_f.at[i], rzs.at[3, i, 0], rzr.at[3, i, 0], ctx, zp(i + 1))

    def in_partial(core, off):
        here = ds(off, cw)
        acc = None
        for t in range(3):
            left = dqkv[t, pl.ds(core, 1)].reshape(rows, head_w)
            term = lax.dot_general(left, w[t][here, :], NT, preferred_element_type=F32)
            acc = term if acc is None else acc + term
        return acc

    own_rows = ds(z * share_rows, share_rows)
    for i in range(tps):
        off = zp(i + 1) * cw
        st_p[:, ds(off, cw)] = in_partial(ok, off).astype(BF16)
        rp_copy(3, i, off).start()
        mine = in_partial(k, off)
        rp_copy(3, i, off).wait_recv()
        st_z[:, ds(off, cw)] = (mine + rx_p[1, :, ds(off, cw)].astype(F32)).astype(BF16)
        st_z[own_rows, ds(off, cw)] = (st_z[own_rows, ds(off, cw)].astype(F32) + dhid[:, ds(off, cw)]).astype(BF16)
        if i < tps - 1:
            rf_copy(i, off).start()

    for m in range(3):

        def gqkv_step(j, carry):
            here = ds(j * 512, 512)
            right = dqkv[m].reshape(both, head_w)
            w[m][here, :] = jnp.dot(tok_t[here, :], right, preferred_element_type=F32).astype(BF16)
            return carry

        lax.fori_loop(0, width // 512, gqkv_step, 0)
        send_g(m)
    middle = gg_row[:, ds(z * feats, feats)]
    for i, copy in enumerate(gains_z):
        copy.wait_recv()
        middle = middle + gg_rx1[i]
    gg_mid[...] = gg_mid[...] + middle
    gains_c = []
    n = 0
    for i, d in slots:
        if i or d:
            core = (k + d) % 2
            gains_c.append(go(remote(gg_mid.at[:, ds(chip(i) * 128, 128)], gg_rx2.at[n], ms.at[5, n], mr.at[5, n], chip(i) * 2 + core, z)))
            n += 1

    for i in range(tps - 1):
        rf_copy(i, zp(i + 1) * cw).wait_recv()
    final = st_z[:, ds(z * feats, cw)].astype(F32)
    for i in range(tps - 1):
        final = final + rx_f[i].astype(F32)
    gin_ref[...] = final
    for i in range(tps):
        rp_copy(3, i, zp(i + 1) * cw).wait_send()
        if i < tps - 1:
            rf_copy(i, zp(i + 1) * cw).wait_send()
    gain_sum = gg_mid[:, ds(c * 128, 128)]
    for i, copy in enumerate(gains_c):
        copy.wait_recv()
        gain_sum = gain_sum + gg_rx2[i]
    ggain_ref[...] = gain_sum
    own_out.wait()
    for copy in out_z:
        copy.wait_recv()
    for copy in g_own:
        copy.wait()
    for copy in g_live:
        copy.wait_recv()
    for copy in pending:
        copy.wait_send()


def fused(
    tokens,
    w_query,
    w_key,
    w_value,
    w_output,
    w_gate,
    w_up,
    w_down,
    gain_query,
    gain_key,
    gain_attention,
    gain_feedforward,
    block_order,
    cotangent,
):
    seqs, blk, feats = tokens.shape
    tps = lax.axis_size("tp")
    chips = lax.axis_size("ctx") // 2
    width = feats * tps
    rows = seqs * blk
    both = 2 * rows
    share_rows = rows // tps
    total = 2 * chips * blk
    head_w = w_query.shape[1] // 2
    ff_w = w_gate.shape[1] // 2
    heads = head_w // HD
    slab = width // (2 * chips)
    ctx = lax.axis_index("ctx")
    chip = ctx // 2
    pair = lax.dynamic_slice_in_dim(block_order, 2 * chip, 2, 1)
    inner = jnp.arange(blk, dtype=jnp.int32)
    positions = (pair.T[:, :, None] * blk + inner).reshape(both)
    frequency = THETA ** (-2.0 * jnp.arange(HD // 2, dtype=F32) / HD)
    angles = positions.astype(F32)[:, None] * frequency
    cosine, sine = jnp.cos(angles), jnp.sin(angles)
    cosf = jnp.concatenate([cosine, cosine], axis=1)
    sinf = jnp.concatenate([-sine, sine], axis=1)
    mine = lax.dynamic_slice_in_dim(block_order, chip // heads, 1, 0)
    order = (mine.reshape(-1, 1) * blk + inner).reshape(total)
    pos_row = jnp.broadcast_to(order[None, :], (8, total))
    pos_col = jnp.broadcast_to(order[:, None], (total, 128))
    gains = jnp.stack([gain_query, gain_key, gain_attention, gain_feedforward]).astype(F32)
    gains = jnp.pad(gains, ((0, 4), (0, 0)))
    blank = jnp.zeros_like(gains)
    gtile = jnp.where(ctx % 2 == 0, jnp.concatenate([gains, blank], axis=1), jnp.concatenate([blank, gains], axis=1))
    weights = (w_query, w_key, w_value, w_output, w_gate, w_up, w_down)
    dims = (chips, tps, seqs, blk, width, head_w, ff_w)
    halves = (head_w, head_w, head_w, head_w, ff_w, ff_w, ff_w)
    hbm = pl.BlockSpec(memory_space=pl.ANY)
    vmem = pl.BlockSpec(memory_space=pltpu.VMEM)

    def v(shape, dtype=BF16):
        return pltpu.VMEM(shape, dtype)

    w_shapes = [v((width, h)) if m in COLS else v((h, width)) for m, h in enumerate(halves)]
    dma = pltpu.SemaphoreType.DMA
    scratch = w_shapes + [
        v((both, width)),
        v((width, both)),
        v((both, width)),
        v((width, both)),
        v((both, width)),
        v((both, width)),
        v((both, ff_w), F32),
        v((both, ff_w), F32),
        v((both, ff_w)),
        v((ff_w, both)),
        v((both, ff_w)),
        v((both, ff_w)),
        v((rows, width)),
        v((2, rows, width)),
        v((rows, width)),
        v((2, tps - 1, share_rows, width)),
        v((tps - 1, rows, feats)),
        v((both, head_w), F32),
        v((both, head_w), F32),
        v((3, 2, seqs, blk, head_w)),
        v((3, 2 * chips, blk, HD)),
        v((total, total)),
        v((total, HD), F32),
        v((2 * chips, blk, HD)),
        v((2, seqs, blk, head_w)),
        v((head_w, both)),
        v((2, seqs, blk, head_w)),
        v((2 * chips, blk, HD)),
        v((total, HD), F32),
        v((total, HD), F32),
        v((3, 2 * chips, blk, HD)),
        v((3, 2, seqs, blk, head_w)),
        v((2, 8, both), F32),
        v((2, 2 * tps - 1, 8, both), F32),
        v((both, 128), F32),
        v((both, 128), F32),
        v((share_rows, width)),
        v((share_rows, width), F32),
        v((share_rows, width), F32),
        v((share_rows, width), F32),
        v((share_rows, width), F32),
        v((share_rows, width), F32),
        v((2 * chips, 8, 128), F32),
        v((tps, 2 * chips, 8, 128), F32),
        v((8, width), F32),
        v((8, head_w), F32),
        v((8, width), F32),
        v((tps - 1, 8, feats), F32),
        v((8, feats), F32),
        v((2 * chips - 1, 8, 128), F32),
        dma((7, 2 * chips)),
        dma((7, 2 * chips)),
        dma((7, 2 * chips)),
        dma((7, 2 * chips)),
        dma((4, tps - 1)),
        dma((4, tps - 1)),
        dma((4, tps)),
        dma((4, tps)),
        dma((4, tps)),
        dma((4, tps)),
        dma((4, tps, tps - 1)),
        dma((4, tps, tps - 1)),
        dma((6, 2 * chips)),
        dma((6, 2 * chips)),
        dma((2, 2 * tps - 1)),
        dma((2, 2 * tps - 1)),
        dma((4, chips - 1)),
        dma((4, chips - 1)),
        dma((25,)),
    ]
    results = pl.pallas_call(
        functools.partial(layer_kernel, dims),
        out_shape=[
            jax.ShapeDtypeStruct((rows, feats), F32),
            jax.ShapeDtypeStruct((rows, feats), F32),
            jax.ShapeDtypeStruct((8, 128), F32),
        ]
        + [jax.ShapeDtypeStruct((chips,) + weight.shape, BF16) for weight in weights],
        in_specs=[hbm] * 9 + [vmem] * 5,
        out_specs=[hbm, vmem, vmem] + [hbm] * 7,
        scratch_shapes=scratch,
        compiler_params=pltpu.CompilerParams(
            collective_id=0, has_side_effects=True, vmem_limit_bytes=67043328
        ),
        name="layer",
    )(tokens.reshape(rows, feats), cotangent.reshape(rows, feats), *weights, gtile, cosf, sinf, pos_row, pos_col)
    output = results[0].reshape(tokens.shape)
    grad_input = results[1].reshape(tokens.shape)
    grads = [jnp.sum(received.astype(F32), axis=0) for received in results[3:]]
    lanes = lax.dynamic_slice_in_dim(results[2], (ctx % 2) * 64, 64, 1)
    return (output, grad_input, *grads, lanes[2], lanes[3], lanes[0], lanes[1])


def fits(mesh):
    return mesh.shape["ctx"] == 8 and mesh.shape["tp"] == 4


def solution(mesh):
    placed = (
        P(None, "ctx", "tp"),
        P("ctx", "tp"),
        P("ctx", "tp"),
        P("ctx", "tp"),
        P("tp", "ctx"),
        P("ctx", "tp"),
        P("ctx", "tp"),
        P("tp", "ctx"),
        P(("tp", "ctx")),
        P(("tp", "ctx")),
        P(("tp", "ctx")),
        P(("tp", "ctx")),
        P(),
        P(None, "ctx", "tp"),
    )
    return jax.shard_map(
        fused if fits(mesh) else shards,
        mesh=mesh,
        in_specs=placed,
        out_specs=(
            P(None, "ctx", "tp"),
            P(None, "ctx", "tp"),
            P("ctx", "tp"),
            P("ctx", "tp"),
            P("ctx", "tp"),
            P("tp", "ctx"),
            P("ctx", "tp"),
            P("ctx", "tp"),
            P("tp", "ctx"),
            P(("tp", "ctx")),
            P(("tp", "ctx")),
            P(("tp", "ctx")),
            P(("tp", "ctx")),
        ),
        check_vma=False,
    )
```

```python
import functools

import jax
import jax.numpy as jnp
from jax import lax
from jax.experimental import pallas as pl
from jax.experimental.pallas import tpu as pltpu
from jax.sharding import PartitionSpec as P

HD = 128


EPS = 1e-06
THETA = 500000.0
NEGATIVE = -1e30


def full_width(value):
    return lax.all_gather(value, "tp", axis=2, tiled=True)


def share(value):
    return lax.psum_scatter(value, "tp", scatter_dimension=2, tiled=True)


def tp_total(values):
    return lax.psum(values, "tp")


def rotary_tables(positions):
    half_dim = HD // 2
    frequency = THETA ** (-2.0 * jnp.arange(half_dim, dtype=jnp.float32) / HD)
    angles = positions.astype(jnp.float32)[..., None] * frequency
    return (jnp.cos(angles)[..., None, :], jnp.sin(angles)[..., None, :])


def rotate(value, cosine, sine):
    half_dim = value.shape[-1] // 2
    first, second = (value[..., :half_dim], value[..., half_dim:])
    return jnp.concatenate(
        [first * cosine - second * sine, second * cosine + first * sine], axis=-1
    )


def unrotate(grad, cosine, sine):
    half_dim = grad.shape[-1] // 2
    first, second = (grad[..., :half_dim], grad[..., half_dim:])
    return jnp.concatenate(
        [first * cosine + second * sine, second * cosine - first * sine], axis=-1
    )


def key_positions(block_order, start, count, block_len):
    slots = start + jnp.arange(count, dtype=jnp.int32)
    owner = slots // block_len
    ranks = jnp.arange(block_order.shape[1], dtype=jnp.int32)
    chosen = jnp.sum(
        jnp.where(owner[None, :, None] == ranks[None, None, :], block_order[:, None, :], 0), axis=2
    )
    return chosen * block_len + slots % block_len


def span_of():
    return 512


def shards(
    tokens,
    w_query,
    w_key,
    w_value,
    w_output,
    w_gate,
    w_up,
    w_down,
    gain_query,
    gain_key,
    gain_attention,
    gain_feedforward,
    block_order,
    cotangent,
):
    gathered = (
        lax.all_gather(w_query, "ctx", axis=0, tiled=True),
        lax.all_gather(w_key, "ctx", axis=0, tiled=True),
        lax.all_gather(w_value, "ctx", axis=0, tiled=True),
        lax.all_gather(w_output, "ctx", axis=1, tiled=True),
        lax.all_gather(w_gate, "ctx", axis=0, tiled=True),
        lax.all_gather(w_up, "ctx", axis=0, tiled=True),
        lax.all_gather(w_down, "ctx", axis=1, tiled=True),
        lax.all_gather(gain_query, "ctx", axis=0, tiled=True),
        lax.all_gather(gain_key, "ctx", axis=0, tiled=True),
        lax.all_gather(gain_attention, "ctx", axis=0, tiled=True),
        lax.all_gather(gain_feedforward, "ctx", axis=0, tiled=True),
    )
    wq_full, wk_full, wv_full, wo_full, wg_full, wu_full, wd_full = gathered[:7]
    g_query = gathered[7].astype(jnp.float32)
    g_key = gathered[8].astype(jnp.float32)
    g_attn = gathered[9].astype(jnp.float32)
    g_feed = gathered[10].astype(jnp.float32)
    seq_count, block_len, local_width = tokens.shape
    row_count = seq_count * block_len
    scale = HD ** (-0.5)
    tok_full = full_width(tokens)
    tok_rows = tok_full.reshape(row_count, -1)
    width = tok_rows.shape[1]
    queries = jnp.dot(tok_rows, wq_full, preferred_element_type=jnp.float32)
    keys_raw = jnp.dot(tok_rows, wk_full, preferred_element_type=jnp.float32)
    values_raw = jnp.dot(tok_rows, wv_full, preferred_element_type=jnp.float32)
    head_width = queries.shape[1]
    head_count = head_width // HD
    q_squares, k_squares = tp_total(
        (jnp.sum(queries * queries, axis=1), jnp.sum(keys_raw * keys_raw, axis=1))
    )
    q_inverse = lax.rsqrt(q_squares / width + EPS)[:, None]
    k_inverse = lax.rsqrt(k_squares / width + EPS)[:, None]
    q_normed = queries * q_inverse * g_query
    k_normed = keys_raw * k_inverse * g_key
    ctx_rank = lax.axis_index("ctx")
    ranks = jnp.arange(block_order.shape[1], dtype=jnp.int32)
    my_block = jnp.sum(jnp.where(ranks[None, :] == ctx_rank, block_order, 0), axis=1)
    q_pos = my_block[:, None] * block_len + jnp.arange(block_len, dtype=jnp.int32)[None, :]
    cosine, sine = rotary_tables(q_pos)
    q_rot = rotate(q_normed.reshape(seq_count, block_len, head_count, HD), cosine, sine).astype(
        jnp.bfloat16
    )
    k_rot = rotate(k_normed.reshape(seq_count, block_len, head_count, HD), cosine, sine).astype(
        jnp.bfloat16
    )
    k_flat = k_rot.reshape(seq_count, block_len, head_width)
    v_flat = values_raw.astype(jnp.bfloat16).reshape(seq_count, block_len, head_width)

    def stat_block(state, key_piece, k_pos):
        run_max, run_sum = state
        scores = (
            jnp.einsum("sqhd,skhd->shqk", q_rot, key_piece, preferred_element_type=jnp.float32)
            * scale
        )
        visible = k_pos[:, None, None, :] <= q_pos[:, None, :, None]
        scores = jnp.where(visible, scores, NEGATIVE)
        new_max = jnp.maximum(run_max, jnp.max(scores, axis=-1))
        weights = jnp.where(visible, jnp.exp(scores - new_max[..., None]), 0.0)
        run_sum = run_sum * jnp.exp(run_max - new_max) + jnp.sum(weights, axis=-1)
        return (new_max, run_sum)

    init = (
        jnp.full((seq_count, head_count, block_len), NEGATIVE, jnp.float32),
        jnp.zeros((seq_count, head_count, block_len), jnp.float32),
    )
    fold_key_all = lax.all_gather(k_flat, "ctx", axis=1, tiled=True)
    count = fold_key_all.shape[1]
    span = span_of()

    def fold_one_span(step_index, inner):
        offset = step_index * span
        key_piece = lax.dynamic_slice_in_dim(fold_key_all, offset, span, 1).reshape(
            seq_count, span, head_count, HD
        )
        k_pos = key_positions(block_order, offset, span, block_len)
        return stat_block(inner, key_piece, k_pos)

    run_max, run_sum = lax.fori_loop(0, count // span, fold_one_span, init)
    key_all, val_all = (
        lax.all_gather(k_flat, "ctx", axis=1, tiled=True),
        lax.all_gather(v_flat, "ctx", axis=1, tiled=True),
    )
    log_total = run_max + jnp.log(run_sum)
    total_len = key_all.shape[1]
    total_span = span_of()

    def value_span(step_index, acc):
        offset = step_index * total_span
        key_piece = lax.dynamic_slice_in_dim(key_all, offset, total_span, 1).reshape(
            seq_count, total_span, head_count, HD
        )
        val_piece = lax.dynamic_slice_in_dim(val_all, offset, total_span, 1).reshape(
            seq_count, total_span, head_count, HD
        )
        k_pos = key_positions(block_order, offset, total_span, block_len)
        scores = (
            jnp.einsum("sqhd,skhd->shqk", q_rot, key_piece, preferred_element_type=jnp.float32)
            * scale
        )
        visible = k_pos[:, None, None, :] <= q_pos[:, None, :, None]
        weights = jnp.where(visible, jnp.exp(scores - log_total[..., None]), 0.0).astype(
            jnp.bfloat16
        )
        return acc + jnp.einsum(
            "shqk,skhd->sqhd", weights, val_piece, preferred_element_type=jnp.float32
        )

    attended = lax.fori_loop(
        0,
        total_len // total_span,
        value_span,
        jnp.zeros((seq_count, block_len, head_count, HD), jnp.float32),
    )
    attn_bf = attended.reshape(row_count, head_width).astype(jnp.bfloat16)
    attn_proj = share(
        jnp.dot(attn_bf, wo_full, preferred_element_type=jnp.float32).reshape(
            seq_count, block_len, -1
        )
    )
    (a_squares,) = tp_total((jnp.sum(attn_proj * attn_proj, axis=2),))
    a_inverse = lax.rsqrt(a_squares / width + EPS)[..., None]
    hidden_state = tokens.astype(jnp.float32) + attn_proj * a_inverse * g_attn
    hidden_rows = full_width(hidden_state.astype(jnp.bfloat16)).reshape(row_count, -1)
    gate = jnp.dot(hidden_rows, wg_full, preferred_element_type=jnp.float32)
    up_vals = jnp.dot(hidden_rows, wu_full, preferred_element_type=jnp.float32)
    sigma = jax.nn.sigmoid(gate)
    activation = (gate * sigma * up_vals).astype(jnp.bfloat16)
    mixed = share(
        jnp.dot(activation, wd_full, preferred_element_type=jnp.float32).reshape(
            seq_count, block_len, -1
        )
    )
    (m_squares,) = tp_total((jnp.sum(mixed * mixed, axis=2),))
    m_inverse = lax.rsqrt(m_squares / width + EPS)[..., None]
    output = hidden_state + mixed * m_inverse * g_feed
    upstream = cotangent.astype(jnp.float32)
    (m_dots,) = tp_total((jnp.sum(g_feed * upstream * mixed, axis=2),))
    d_mixed = m_inverse * (g_feed * upstream) - mixed * m_inverse**3 * (m_dots / width)[..., None]
    d_gfeed = jnp.sum(upstream * mixed * m_inverse, axis=(0, 1))
    d_mixed_rows = full_width(d_mixed.astype(jnp.bfloat16)).reshape(row_count, -1)
    grad_down = jnp.dot(activation.T, d_mixed_rows, preferred_element_type=jnp.float32)
    d_act = jnp.dot(d_mixed_rows, wd_full.T, preferred_element_type=jnp.float32)
    d_up_bf = (d_act * gate * sigma).astype(jnp.bfloat16)
    d_gate_bf = (d_act * up_vals * sigma * (1.0 + gate * (1.0 - sigma))).astype(jnp.bfloat16)
    grad_gate = jnp.dot(hidden_rows.T, d_gate_bf, preferred_element_type=jnp.float32)
    grad_up = jnp.dot(hidden_rows.T, d_up_bf, preferred_element_type=jnp.float32)
    back_ff = jnp.dot(d_gate_bf, wg_full.T, preferred_element_type=jnp.float32) + jnp.dot(
        d_up_bf, wu_full.T, preferred_element_type=jnp.float32
    )
    d_hidden = upstream + share(back_ff.reshape(seq_count, block_len, -1))
    (a_dots,) = tp_total((jnp.sum(g_attn * d_hidden * attn_proj, axis=2),))
    d_attn = (
        a_inverse * (g_attn * d_hidden) - attn_proj * a_inverse**3 * (a_dots / width)[..., None]
    )
    d_gattn = jnp.sum(d_hidden * attn_proj * a_inverse, axis=(0, 1))
    d_attn_rows = full_width(d_attn.astype(jnp.bfloat16)).reshape(row_count, -1)
    grad_outproj = jnp.dot(attn_bf.T, d_attn_rows, preferred_element_type=jnp.float32)
    d_heads = jnp.dot(d_attn_rows, wo_full.T, preferred_element_type=jnp.float32).reshape(
        seq_count, block_len, head_count, HD
    )
    deltas = jnp.sum(d_heads * attended, axis=3).transpose(0, 2, 1)
    d_heads_bf = d_heads.astype(jnp.bfloat16)

    def grad_block(key_piece, val_piece, k_pos):
        scores = (
            jnp.einsum("sqhd,skhd->shqk", q_rot, key_piece, preferred_element_type=jnp.float32)
            * scale
        )
        visible = k_pos[:, None, None, :] <= q_pos[:, None, :, None]
        probs = jnp.where(visible, jnp.exp(scores - log_total[..., None]), 0.0)
        d_probs = jnp.einsum(
            "sqhd,skhd->shqk", d_heads_bf, val_piece, preferred_element_type=jnp.float32
        )
        d_scores = (probs * (d_probs - deltas[..., None])).astype(jnp.bfloat16)
        return (probs, d_scores)

    def query_span(step_index, acc):
        offset = step_index * total_span
        key_piece = lax.dynamic_slice_in_dim(key_all, offset, total_span, 1).reshape(
            seq_count, total_span, head_count, HD
        )
        val_piece = lax.dynamic_slice_in_dim(val_all, offset, total_span, 1).reshape(
            seq_count, total_span, head_count, HD
        )
        k_pos = key_positions(block_order, offset, total_span, block_len)
        probs, d_scores = grad_block(key_piece, val_piece, k_pos)
        return (
            acc
            + jnp.einsum("shqk,skhd->sqhd", d_scores, key_piece, preferred_element_type=jnp.float32)
            * scale
        )

    d_qrot = lax.fori_loop(
        0,
        total_len // total_span,
        query_span,
        jnp.zeros((seq_count, block_len, head_count, HD), jnp.float32),
    )
    count = block_len * lax.axis_size("ctx")
    key_span = span_of()

    def key_one_span(step_index, buffer):
        offset = step_index * key_span
        key_piece = lax.dynamic_slice_in_dim(key_all, offset, key_span, 1).reshape(
            seq_count, key_span, head_count, HD
        )
        val_piece = lax.dynamic_slice_in_dim(val_all, offset, key_span, 1).reshape(
            seq_count, key_span, head_count, HD
        )
        k_pos = key_positions(block_order, offset, key_span, block_len)
        probs, d_scores = grad_block(key_piece, val_piece, k_pos)
        d_keyp = (
            jnp.einsum("shqk,sqhd->skhd", d_scores, q_rot, preferred_element_type=jnp.float32)
            * scale
        )
        d_valp = jnp.einsum(
            "shqk,sqhd->skhd",
            probs.astype(jnp.bfloat16),
            d_heads_bf,
            preferred_element_type=jnp.float32,
        )
        both = jnp.concatenate(
            [
                d_keyp.reshape(seq_count, key_span, head_width),
                d_valp.reshape(seq_count, key_span, head_width),
            ],
            axis=2,
        )
        return lax.dynamic_update_slice_in_dim(buffer, both.transpose(1, 0, 2), offset, 0)

    key_sums = (
        lax.psum_scatter(
            lax.fori_loop(
                0,
                count // key_span,
                key_one_span,
                jnp.zeros((count, seq_count, 2 * head_width), jnp.float32),
            ).astype(jnp.bfloat16),
            "ctx",
            scatter_dimension=0,
            tiled=True,
        )
        .astype(jnp.float32)
        .transpose(1, 0, 2)
    )
    d_krot = key_sums[..., :head_width].reshape(seq_count, block_len, head_count, HD)
    d_values = key_sums[..., head_width:].reshape(row_count, head_width)
    dq_normed = unrotate(d_qrot, cosine, sine).reshape(row_count, head_width)
    dk_normed = unrotate(d_krot, cosine, sine).reshape(row_count, head_width)
    q_dots, k_dots = tp_total(
        (
            jnp.sum(g_query * dq_normed * queries, axis=1),
            jnp.sum(g_key * dk_normed * keys_raw, axis=1),
        )
    )
    d_queries = (
        q_inverse * (g_query * dq_normed) - queries * q_inverse**3 * (q_dots / width)[:, None]
    )
    d_keys = k_inverse * (g_key * dk_normed) - keys_raw * k_inverse**3 * (k_dots / width)[:, None]
    d_gquery = jnp.sum(dq_normed * queries * q_inverse, axis=0)
    d_gkey = jnp.sum(dk_normed * keys_raw * k_inverse, axis=0)
    dq_bf = d_queries.astype(jnp.bfloat16)
    dk_bf = d_keys.astype(jnp.bfloat16)
    dv_bf = d_values.astype(jnp.bfloat16)
    grad_q = jnp.dot(tok_rows.T, dq_bf, preferred_element_type=jnp.float32)
    grad_k = jnp.dot(tok_rows.T, dk_bf, preferred_element_type=jnp.float32)
    grad_v = jnp.dot(tok_rows.T, dv_bf, preferred_element_type=jnp.float32)
    back_attn = (
        jnp.dot(dq_bf, wq_full.T, preferred_element_type=jnp.float32)
        + jnp.dot(dk_bf, wk_full.T, preferred_element_type=jnp.float32)
        + jnp.dot(dv_bf, wv_full.T, preferred_element_type=jnp.float32)
    )
    grad_input = d_hidden + share(back_attn.reshape(seq_count, block_len, -1))
    summed = (
        lax.psum_scatter(
            grad_q.astype(jnp.bfloat16), "ctx", scatter_dimension=0, tiled=True
        ).astype(jnp.float32),
        lax.psum_scatter(
            grad_k.astype(jnp.bfloat16), "ctx", scatter_dimension=0, tiled=True
        ).astype(jnp.float32),
        lax.psum_scatter(
            grad_v.astype(jnp.bfloat16), "ctx", scatter_dimension=0, tiled=True
        ).astype(jnp.float32),
        lax.psum_scatter(
            grad_outproj.astype(jnp.bfloat16), "ctx", scatter_dimension=1, tiled=True
        ).astype(jnp.float32),
        lax.psum_scatter(
            grad_gate.astype(jnp.bfloat16), "ctx", scatter_dimension=0, tiled=True
        ).astype(jnp.float32),
        lax.psum_scatter(
            grad_up.astype(jnp.bfloat16), "ctx", scatter_dimension=0, tiled=True
        ).astype(jnp.float32),
        lax.psum_scatter(
            grad_down.astype(jnp.bfloat16), "ctx", scatter_dimension=1, tiled=True
        ).astype(jnp.float32),
        lax.psum_scatter(
            d_gquery.astype(jnp.bfloat16), "ctx", scatter_dimension=0, tiled=True
        ).astype(jnp.float32),
        lax.psum_scatter(
            d_gkey.astype(jnp.bfloat16), "ctx", scatter_dimension=0, tiled=True
        ).astype(jnp.float32),
        lax.psum_scatter(
            d_gattn.astype(jnp.bfloat16), "ctx", scatter_dimension=0, tiled=True
        ).astype(jnp.float32),
        lax.psum_scatter(
            d_gfeed.astype(jnp.bfloat16), "ctx", scatter_dimension=0, tiled=True
        ).astype(jnp.float32),
    )
    return (
        output,
        grad_input,
        summed[0],
        summed[1],
        summed[2],
        summed[3],
        summed[4],
        summed[5],
        summed[6],
        summed[7],
        summed[8],
        summed[9],
        summed[10],
    )


MESH = pl.DeviceIdType.MESH
NT = (((1,), (1,)), ((), ()))
TN = (((0,), (0,)), ((), ()))
F32 = jnp.float32
BF16 = jnp.bfloat16
COLS = (0, 1, 2, 4, 5)


def layer_kernel(dims, *refs):
    (chips, tps, seqs, blk, width, head_w, ff_w) = dims
    rows = seqs * blk
    both = 2 * rows
    share_rows = rows // tps
    feats = width // tps
    heads = head_w // HD
    slab = width // (2 * chips)
    halves = (head_w, head_w, head_w, head_w, ff_w, ff_w, ff_w)
    total = 2 * chips * blk
    scale = HD ** (-0.5)
    it = iter(refs)

    def take(n):
        return [next(it) for _ in range(n)]

    (tok_in, cot_in) = take(2)
    w_in = take(7)
    (gtile, cosf, sinf, pos_row, pos_col) = take(5)
    (out_ref, gin_ref, ggain_ref) = take(3)
    rx_g = take(7)
    w = take(7)
    via = take(7)
    (tok, tok_t, hid, hid_t, dmix, dattn) = take(6)
    (lin, fac, act, act_t, dgate, dup) = take(6)
    (st_p, rx_p, st_z, rx_z, rx_f) = take(5)
    (q_raw, k_raw, qkv, qa, probs, att_f, att_st, att, att_t) = take(9)
    (dh, d_o, dk_acc, dv_acc, dqkv_st, dqkv) = take(6)
    (sq_own, sq_rx, inv_q, inv_k) = take(4)
    (cot, proj, hstate, dhid, stage) = take(5)
    (gbuf, gall, gfull, gqk, gg_row, gg_rx1, gg_mid, gg_rx2) = take(8)
    (ws, wr, gs, gr) = take(4)
    (zs, zr, ps, pr) = take(4)
    (rps, rpr, rzs, rzr) = take(4)
    (ms, mr) = take(2)
    (ss, sr) = take(2)
    (as_, ar) = take(2)
    (loc,) = take(1)

    ctx = lax.axis_index("ctx")
    z = lax.axis_index("tp")
    c = ctx // 2
    k = ctx % 2
    ok = 1 - k
    partner = c * 2 + ok
    near = (c + 1 - 2 * (c % 2), (c + 2) % chips)
    far = chips - 1 - c

    def zp(i):
        return (z + i) % tps

    def chip(i):
        return (c + i) % chips

    def ds(start, size):
        return pl.ds(pl.multiple_of(start, size), size)

    def remote(src, dst, ssem, rsem, to_ctx, to_z):
        return pltpu.make_async_remote_copy(
            src_ref=src,
            dst_ref=dst,
            send_sem=ssem,
            recv_sem=rsem,
            device_id=(to_ctx, to_z),
            device_id_type=MESH,
        )

    peers = [(chip(i) * 2 + (k + d) % 2, z) for i in range(chips) for d in range(2) if i or d]
    peers += [(ctx, zp(i)) for i in range(1, tps)]
    peers += [(partner, zp(i)) for i in range(1, tps)]
    barrier = pltpu.get_barrier_semaphore()
    for peer in peers:
        pl.semaphore_signal(barrier, inc=1, device_id=peer, device_id_type=MESH)

    pending = []

    def go(copy):
        copy.start()
        pending.append(copy)
        return copy

    def slab_of(m, owner):
        if m in COLS:
            return w[m].at[ds(owner * slab, slab), :]
        return w[m].at[:, ds(owner * slab, slab)]

    def half_of(m, core):
        if m in COLS:
            return w_in[m].at[:, ds(core * halves[m], halves[m])]
        return w_in[m].at[ds(core * halves[m], halves[m]), :]

    w_own = {}
    w_pass = {}
    w_wait = {}

    def w_slot(m, n, owner):
        return remote(slab_of(m, owner), slab_of(m, owner), ws.at[m, n], wr.at[m, n], partner, z)

    def send_w(m, d):
        core = (k + d) % 2
        for n in range(2):
            go(remote(half_of(m, core), slab_of(m, ctx), ws.at[m, 2 * n + d], wr.at[m, 2 * n + k], near[n] * 2 + core, z))
        if d:
            go(remote(half_of(m, ok), slab_of(m, ctx), ws.at[m, 4], wr.at[m, 4], partner, z))
        else:
            w_own[m] = pltpu.make_async_copy(half_of(m, k), slab_of(m, ctx), loc.at[m])
            w_own[m].start()

    def source(n):
        if n < 4:
            return near[n // 2] * 2 + n % 2
        return partner if n == 4 else far * 2 + n - 5

    def got_w(m, *which):
        for n in which:
            if (m, n) not in w_wait:
                w_wait[m, n] = True
                w_slot(m, n, source(n)).wait_recv()

    def pass_w(m):
        for n in range(2):
            got_w(m, 3 * n)
            mine = slab_of(m, source(3 * n))
            copy = remote(mine, mine, ws.at[m, 5 + n], wr.at[m, 5 + n], near[1 - n] * 2 + k, z)
            copy.start()
            w_pass[m, n] = copy

    def free_w(m):
        for n in range(2):
            w_pass[m, n].wait_send()

    def wait_w(m):
        w_own[m].wait()
        got_w(m, *range(7))

    def into(m, n, core):
        if m in COLS:
            return rx_g[m].at[n, :, ds(core * halves[m], halves[m])]
        return rx_g[m].at[n, ds(core * halves[m], halves[m]), :]

    g_live = []
    g_own = []

    def send_g(m):
        for n in range(2):
            go(remote(slab_of(m, far * 2 + n), via[m].at[n], gs.at[m, n], gr.at[m, n], near[n] * 2 + k, z))
        for n in range(2):
            go(remote(slab_of(m, near[n] * 2 + n), into(m, 1 + n, k), gs.at[m, 2 + n], gr.at[m, 2 + 2 * n + k], near[n] * 2 + n, z))
        go(remote(slab_of(m, partner), into(m, 0, k), gs.at[m, 6], gr.at[m, 6], partner, z))
        copy = pltpu.make_async_copy(slab_of(m, ctx), into(m, 0, k), loc.at[8 + m])
        copy.start()
        g_own.append(copy)

    def pass_g(m):
        for n in range(2):
            to = near[1 - n] * 2 + n
            remote(via[m].at[n], via[m].at[n], gs.at[m, n], gr.at[m, n], partner, z).wait_recv()
            total = slab_of(m, to)[...].astype(F32) + via[m][n].astype(F32)
            slab_of(m, to)[...] = total.astype(BF16)
            go(remote(slab_of(m, to), into(m, 2 - n, k), gs.at[m, 4 + n], gr.at[m, 2 + 2 * (1 - n) + k], to, z))
        g_live.append(m)

    def wait_g(m):
        for n in range(2):
            for core in range(2):
                here = into(m, 1 + n, core)
                remote(here, here, gs.at[m, 0], gr.at[m, 2 + 2 * n + core], partner, z).wait_recv()
        here = into(m, 0, ok)
        remote(here, here, gs.at[m, 6], gr.at[m, 6], partner, z).wait_recv()

    own_tok = pltpu.make_async_copy(tok_in, tok.at[ds(k * rows, rows), ds(z * feats, feats)], loc.at[16])
    own_tok.start()
    own_cot = pltpu.make_async_copy(cot_in.at[ds(z * share_rows, share_rows), :], cot.at[:, ds(z * feats, feats)], loc.at[17])
    own_cot.start()
    own_gain = pltpu.make_async_copy(gtile, gbuf.at[ctx], loc.at[18])
    own_gain.start()
    pl.semaphore_wait(barrier, len(peers))

    tok_z = []
    for i in range(1, tps):
        tok_z.append(go(remote(tok_in, tok.at[ds(k * rows, rows), ds(z * feats, feats)], zs.at[0, i - 1], zr.at[0, i - 1], ctx, zp(i))))
    tok_p = [go(remote(tok_in, tok.at[ds(k * rows, rows), ds(z * feats, feats)], ps.at[0, 0], pr.at[0, 0], partner, z))]
    slots = [(i, d) for i in range(chips) for d in range(2)]
    gain1 = []
    n = 0
    for i, d in slots:
        if i or d:
            gain1.append(go(remote(gtile, gbuf.at[ctx], ms.at[0, n], mr.at[0, n], chip(i) * 2 + (k + d) % 2, z)))
            n += 1
    cot_z = []
    for i in range(1, tps):
        cot_z.append(go(remote(cot_in.at[ds(zp(i) * share_rows, share_rows), :], cot.at[:, ds(z * feats, feats)], ms.at[1, i - 1], mr.at[1, i - 1], ctx, zp(i))))
    for m in (0, 1, 2, 3):
        send_w(m, 0)
        send_w(m, 1)

    own_gain.wait()
    for copy in gain1:
        copy.wait_recv()
    own_gain2 = pltpu.make_async_copy(gbuf, gall.at[z], loc.at[19])
    own_gain2.start()
    gain2 = []
    for i in range(1, tps):
        gain2.append(go(remote(gbuf, gall.at[z], ms.at[2, i - 1], mr.at[2, i - 1], ctx, zp(i))))
    for r in range(2):
        pieces = [gbuf[4 * k + 2 * m, r : r + 1, :] + gbuf[4 * k + 2 * m + 1, r : r + 1, :] for m in range(head_w // 128)]
        gqk[r : r + 1, :] = jnp.concatenate(pieces, axis=1)

    own_tok.wait()
    for i in range(1, tps):
        tok_z[i - 1].wait_recv()
        part = tok.at[ds(k * rows, rows), ds(((z - i) % tps) * feats, feats)]
        tok_p.append(go(remote(part, part, ps.at[0, i], pr.at[0, i], partner, z)))
    for m in (0, 1, 2, 3):
        pass_w(m)
    send_w(4, 0)
    for copy in tok_p:
        copy.wait_recv()

    def row_of(value):
        folded = value[:, :128]
        for h in range(1, heads):
            folded = folded + value[:, h * 128 : (h + 1) * 128]
        return jnp.sum(jnp.transpose(folded), axis=0, keepdims=True)

    def column_of(row):
        return jnp.transpose(jnp.broadcast_to(row, (128, both)))

    def totals(idx):
        copies = []
        n = 0
        for i in range(tps):
            for d in range(2):
                if i or d:
                    to = ctx if d == 0 else partner
                    copies.append(go(remote(sq_own.at[idx], sq_rx.at[idx, n], ss.at[idx, n], sr.at[idx, n], to, zp(i))))
                    n += 1
        total = sq_own[idx]
        for j, copy in enumerate(copies):
            copy.wait_recv()
            total = total + sq_rx[idx, j]
        return total

    for m in (0, 1, 2):
        wait_w(m)
        value = jnp.dot(tok[...], w[m][...], preferred_element_type=F32)
        if m == 0:
            q_raw[...] = value
            sq_own[0, 0:1, :] = row_of(value * value)
        elif m == 1:
            k_raw[...] = value
            sq_own[0, 1:2, :] = row_of(value * value)
        else:
            qkv[2] = value.astype(BF16).reshape(2, seqs, blk, head_w)
    sq_own[0, 2:8, :] = jnp.zeros((6, both), F32)
    squares = totals(0)
    inverse = lax.rsqrt(squares / width + EPS)
    inv_q[...] = column_of(inverse[0:1, :])
    inv_k[...] = column_of(inverse[1:2, :])
    for t, (raw, inv) in enumerate(((q_raw, inv_q), (k_raw, inv_k))):
        for h in range(heads):
            lanes = slice(h * HD, (h + 1) * HD)
            normed = raw[:, lanes] * inv[...] * gqk[t : t + 1, lanes]
            turned = normed * cosf[...] + pltpu.roll(normed, HD // 2, 1) * sinf[...]
            qkv[t, :, :, :, lanes] = turned.astype(BF16).reshape(2, seqs, blk, HD)

    def to_owner(idx, value, owned, stacked):
        copies = []
        for i in range(chips):
            to = chip(i)
            s, h = to // heads, to % heads
            if stacked:
                src = value.at[:, :, s, :, ds(h * HD, HD)]
                dst = owned.at[:, ds(2 * c, 2)]
            else:
                src = value.at[:, s, :, ds(h * HD, HD)]
                dst = owned.at[ds(2 * c, 2)]
            if i:
                copies.append(go(remote(src, dst, as_.at[idx, i - 1], ar.at[idx, i - 1], to * 2 + k, z)))
            else:
                own = pltpu.make_async_copy(src, dst, loc.at[20 + idx])
                own.start()
        return own, copies

    def from_owner(idx, owned, value, stacked):
        s, h = c // heads, c % heads
        copies = []
        for i in range(chips):
            to = chip(i)
            if stacked:
                src = owned.at[:, ds(2 * to, 2)]
                dst = value.at[:, :, s, :, ds(h * HD, HD)]
            else:
                src = owned.at[ds(2 * to, 2)]
                dst = value.at[:, s, :, ds(h * HD, HD)]
            if i:
                copies.append(go(remote(src, dst, as_.at[idx, i - 1], ar.at[idx, i - 1], to * 2 + k, z)))
            else:
                own = pltpu.make_async_copy(src, dst, loc.at[20 + idx])
                own.start()
        return own, copies

    def arrive(pair):
        own, copies = pair
        own.wait()
        for copy in copies:
            copy.wait_recv()

    pair = to_owner(0, qkv, qa, True)
    send_w(4, 1)
    arrive(pair)
    step = 2 * blk

    def attend(i, carry):
        here = ds(i * step, step)
        q = qa[0, pl.ds(2 * i, 2)].reshape(step, HD)
        s = lax.dot_general(q, qa[1].reshape(total, HD), NT, preferred_element_type=F32) * scale
        visible = pos_row[0:1, :] <= pos_col[here, 0:1]
        s = jnp.where(visible, s, NEGATIVE)
        top = jnp.max(s, axis=1, keepdims=True)
        e = jnp.where(visible, jnp.exp(s - top), 0.0)
        p = (e * (1.0 / jnp.sum(e, axis=1, keepdims=True))).astype(BF16)
        probs[here, :] = p
        o = jnp.dot(p, qa[2].reshape(total, HD), preferred_element_type=F32)
        att_f[here, :] = o
        att_st[pl.ds(2 * i, 2)] = o.astype(BF16).reshape(2, blk, HD)
        return carry

    lax.fori_loop(0, chips, attend, 0)
    back = from_owner(1, att_st, att, False)
    pass_w(4)
    for m in (5, 6):
        send_w(m, 0)
        send_w(m, 1)
    own_gain2.wait()
    for copy in gain2:
        copy.wait_recv()
    for r in range(2):
        pieces = []
        for zz in range(tps):
            for m in range(chips):
                pieces.append(gall[zz, 2 * m, 2 + r : 3 + r, :] + gall[zz, 2 * m + 1, 2 + r : 3 + r, :])
        gfull[r : r + 1, :] = jnp.concatenate(pieces, axis=1)
    for s in range(width // 256):
        tok_t[s * 256 : (s + 1) * 256, :] = jnp.transpose(tok[:, s * 256 : (s + 1) * 256])
    arrive(back)
    wait_w(3)

    cw = feats
    rs_live = {}

    def rp_copy(idx, i, off):
        return remote(st_p.at[:, ds(off, cw)], rx_p.at[idx % 2, :, ds(off, cw)], rps.at[idx, i], rpr.at[idx, i], partner, z)

    def rz_copy(idx, i, j, off):
        return remote(
            st_z.at[ds(zp(j) * share_rows, share_rows), ds(off, cw)],
            rx_z.at[idx % 2, j - 1, :, ds(off, cw)],
            rzs.at[idx, i, j - 1],
            rzr.at[idx, i, j - 1],
            ctx,
            zp(j),
        )

    def reduce_rows(idx, partial, offset, before=None, meanwhile=None):
        def one(i):
            off = offset(i)
            if before is not None:
                before(i)
            st_p[:, ds(off, cw)] = partial(ok, off).astype(BF16)
            rp_copy(idx, i, off).start()
            mine = partial(k, off)
            rp_copy(idx, i, off).wait_recv()
            st_z[:, ds(off, cw)] = (mine + rx_p[idx % 2, :, ds(off, cw)].astype(F32)).astype(BF16)
            for j in range(1, tps):
                rz_copy(idx, i, j, off).start()

        def finish(i):
            off = offset(i)
            for j in range(1, tps):
                rz_copy(idx, i, j, off).wait_recv()
                rz_copy(idx, i, j, off).wait_send()
            rp_copy(idx, i, off).wait_send()

        if before is None:
            lax.fori_loop(0, tps, lambda i, x: (one(i), x)[1], 0)
        else:
            for i in range(tps):
                one(i)
        if meanwhile is not None:
            meanwhile()
        if before is None:
            lax.fori_loop(0, tps, lambda i, x: (finish(i), x)[1], 0)
        else:
            for i in range(tps):
                finish(i)
        mine = st_z[ds(z * share_rows, share_rows), :].astype(F32)
        for j in range(tps - 1):
            mine = mine + rx_z[idx % 2, j].astype(F32)
        return mine

    def straight(i):
        return i * cw

    def mean_of(value):
        return jnp.sum(value, axis=1, keepdims=True) / width

    def spread(idx, buf):
        mine = buf.at[ds(k * rows + z * share_rows, share_rows), :]
        along = [go(remote(mine, mine, zs.at[idx, i - 1], zr.at[idx, i - 1], ctx, zp(i))) for i in range(1, tps)]
        across = [go(remote(mine, mine, ps.at[idx, 0], pr.at[idx, 0], partner, z))]

        def finish():
            for i in range(1, tps):
                along[i - 1].wait_recv()
                part = buf.at[ds(k * rows + ((z - i) % tps) * share_rows, share_rows), :]
                across.append(go(remote(part, part, ps.at[idx, i], pr.at[idx, i], partner, z)))
            for copy in across:
                copy.wait_recv()

        return finish

    my_rows = ds(k * rows + z * share_rows, share_rows)
    heads_rows = [None]

    def o_partial(core, off):
        left = att[pl.ds(core, 1)].reshape(rows, head_w)
        return jnp.dot(left, w[3][:, ds(off, cw)], preferred_element_type=F32)

    value = reduce_rows(0, o_partial, straight)
    proj[...] = value
    a_inverse = lax.rsqrt(mean_of(value * value) + EPS)
    state = tok[my_rows, :].astype(F32) + value * a_inverse * gfull[0:1, :]
    hstate[...] = state
    hid[my_rows, :] = state.astype(BF16)
    finish = spread(1, hid)
    own_cot.wait()
    for copy in cot_z:
        copy.wait_recv()
    att_t[...] = jnp.transpose(att[...].reshape(both, head_w))
    finish()

    fw = 256
    pass_w(5)
    wait_w(4)

    def gate_step(j, carry):
        here = ds(j * fw, fw)
        lin[:, here] = jnp.dot(hid[...], w[4][:, here], preferred_element_type=F32)
        return carry

    lax.fori_loop(0, ff_w // fw, gate_step, 0)
    for s in range(width // 256):
        hid_t[s * 256 : (s + 1) * 256, :] = jnp.transpose(hid[:, s * 256 : (s + 1) * 256])
    pass_w(6)
    wait_w(5)

    def up_step(j, carry):
        here = ds(j * fw, fw)
        up = jnp.dot(hid[...], w[5][:, here], preferred_element_type=F32)
        gate = lin[:, here]
        sigma = jax.nn.sigmoid(gate)
        swish = gate * sigma
        lin[:, here] = swish
        fac[:, here] = up * sigma * (1.0 + gate * (1.0 - sigma))
        value = (swish * up).astype(BF16)
        act[:, here] = value
        act_t[here, :] = jnp.transpose(value)
        return carry

    lax.fori_loop(0, ff_w // fw, up_step, 0)

    def down_partial(core, off):
        return jnp.dot(act[ds(core * rows, rows), :], w[6][:, ds(off, cw)], preferred_element_type=F32)

    def from_chip(i):
        return (c, near[0], near[1], far)[i] * cw

    def down_ready(i):
        if i == 0:
            w_own[6].wait()
        got_w(6, *((4,), (0, 1), (2, 3), (5, 6))[i])

    value = reduce_rows(1, down_partial, from_chip, down_ready)
    m_inverse = lax.rsqrt(mean_of(value * value) + EPS)
    scaled = value * m_inverse
    stage[...] = hstate[...] + scaled * gfull[1:2, :]
    for i in range(1, tps):
        go(remote(stage.at[:, ds(zp(i) * feats, feats)], out_ref.at[ds(z * share_rows, share_rows), :], ms.at[3, i - 1], mr.at[3, i - 1], ctx, zp(i)))
    out_z = pending[-(tps - 1) :]
    own_out = pltpu.make_async_copy(stage.at[:, ds(z * feats, feats)], out_ref.at[ds(z * share_rows, share_rows), :], loc.at[24])
    own_out.start()
    upstream = cot[...].astype(F32)
    gained = upstream * gfull[1:2, :]
    gg_row[1:2, :] = jnp.sum(upstream * scaled, axis=0, keepdims=True)
    back_mix = m_inverse * gained - scaled * (m_inverse * m_inverse) * mean_of(gained * value)
    dmix[my_rows, :] = back_mix.astype(BF16)
    spread(2, dmix)()

    def dact_step(j, carry):
        here = ds(j * fw, fw)
        d_act = lax.dot_general(dmix[...], w[6][here, :], NT, preferred_element_type=F32)
        dup[:, here] = (d_act * lin[:, here]).astype(BF16)
        dgate[:, here] = (d_act * fac[:, here]).astype(BF16)
        return carry

    lax.fori_loop(0, ff_w // fw, dact_step, 0)

    def gdown_step(j, carry):
        here = ds(j * fw, fw)
        w[6][:, here] = jnp.dot(act_t[...], dmix[:, here], preferred_element_type=F32).astype(BF16)
        return carry

    free_w(6)
    lax.fori_loop(0, width // fw, gdown_step, 0)
    send_g(6)

    def ff_partial(core, off):
        here = ds(core * rows, rows)
        return lax.dot_general(dgate[here, :], w[4][ds(off, cw), :], NT, preferred_element_type=F32) + lax.dot_general(
            dup[here, :], w[5][ds(off, cw), :], NT, preferred_element_type=F32
        )

    def ggate_step(j, carry):
        here = ds(j * fw, fw)
        w[4][:, here] = jnp.dot(hid_t[...], dgate[:, here], preferred_element_type=F32).astype(BF16)
        return carry

    def gate_grad():
        free_w(4)
        lax.fori_loop(0, ff_w // fw, ggate_step, 0)
        pass_g(6)
        send_g(4)

    value = reduce_rows(2, ff_partial, straight, meanwhile=gate_grad) + cot[...].astype(F32)
    dhid[...] = value
    projected = proj[...]
    a_inverse = lax.rsqrt(mean_of(projected * projected) + EPS)
    scaled = projected * a_inverse
    gained = value * gfull[0:1, :]
    gg_row[0:1, :] = jnp.sum(value * scaled, axis=0, keepdims=True)
    gg_row[2:8, :] = jnp.zeros((6, width), F32)
    back_att = a_inverse * gained - scaled * (a_inverse * a_inverse) * mean_of(gained * projected)
    dattn[my_rows, :] = back_att.astype(BF16)
    finish = spread(3, dattn)
    gains_z = []
    for i in range(1, tps):
        gains_z.append(go(remote(gg_row.at[:, ds(zp(i) * feats, feats)], gg_rx1.at[i - 1], ms.at[4, i - 1], mr.at[4, i - 1], ctx, zp(i))))

    def gup_step(j, carry):
        here = ds(j * fw, fw)
        w[5][:, here] = jnp.dot(hid_t[...], dup[:, here], preferred_element_type=F32).astype(BF16)
        return carry

    free_w(5)
    lax.fori_loop(0, ff_w // fw, gup_step, 0)
    finish()

    value = lax.dot_general(dattn[...], w[3][...], NT, preferred_element_type=F32)
    dh[...] = value.astype(BF16).reshape(2, seqs, blk, head_w)
    pair = to_owner(2, dh, d_o, False)
    pass_g(4)

    def go_step(j, carry):
        here = ds(j * fw, fw)
        w[3][:, here] = jnp.dot(att_t[...], dattn[:, here], preferred_element_type=F32).astype(BF16)
        return carry

    free_w(3)
    lax.fori_loop(0, width // fw, go_step, 0)
    arrive(pair)
    dk_acc[...] = jnp.zeros((total, HD), F32)
    dv_acc[...] = jnp.zeros((total, HD), F32)

    def unattend(i, carry):
        here = ds(i * step, step)
        q = qa[0, pl.ds(2 * i, 2)].reshape(step, HD)
        d_out = d_o[pl.ds(2 * i, 2)].reshape(step, HD)
        d_p = lax.dot_general(d_out, qa[2].reshape(total, HD), NT, preferred_element_type=F32)
        delta = jnp.sum(d_out.astype(F32) * att_f[here, :], axis=1, keepdims=True)
        p = probs[here, :]
        d_s = (p.astype(F32) * (d_p - delta)).astype(BF16)
        d_q = jnp.dot(d_s, qa[1].reshape(total, HD), preferred_element_type=F32) * scale
        dqkv_st[0, pl.ds(2 * i, 2)] = d_q.astype(BF16).reshape(2, blk, HD)
        dk_acc[...] += lax.dot_general(d_s, q, TN, preferred_element_type=F32)
        dv_acc[...] += lax.dot_general(p, d_out, TN, preferred_element_type=F32)
        return carry

    lax.fori_loop(0, chips, unattend, 0)
    dqkv_st[1] = (dk_acc[...] * scale).astype(BF16).reshape(2 * chips, blk, HD)
    dqkv_st[2] = dv_acc[...].astype(BF16).reshape(2 * chips, blk, HD)
    pair = from_owner(3, dqkv_st, dqkv, True)

    send_g(5)
    send_g(3)
    arrive(pair)

    gg_mid[...] = jnp.zeros((8, feats), F32)
    for t, (raw, inv) in enumerate(((q_raw, inv_q), (k_raw, inv_k))):
        folded = None
        for h in range(heads):
            lanes = slice(h * HD, (h + 1) * HD)
            turned = dqkv[t, :, :, :, lanes].reshape(both, HD).astype(F32)
            back_rot = turned * cosf[...] - pltpu.roll(turned, HD // 2, 1) * sinf[...]
            plain = raw[:, lanes]
            scaled = plain * inv[...]
            gg_mid[2 + t : 3 + t, pl.ds(pl.multiple_of(k * head_w + h * HD, HD), HD)] = jnp.sum(back_rot * scaled, axis=0, keepdims=True)
            gained = back_rot * gqk[t : t + 1, lanes]
            dqkv[t, :, :, :, lanes] = gained.astype(BF16).reshape(2, seqs, blk, HD)
            term = gained * plain
            folded = term if folded is None else folded + term
        sq_own[1, t : t + 1, :] = jnp.sum(jnp.transpose(folded), axis=0, keepdims=True)
    sq_own[1, 2:8, :] = jnp.zeros((6, both), F32)
    dots = totals(1) / width
    for t, (raw, inv) in enumerate(((q_raw, inv_q), (k_raw, inv_k))):
        spread_dot = column_of(dots[t : t + 1, :])
        for h in range(heads):
            lanes = slice(h * HD, (h + 1) * HD)
            gained = dqkv[t, :, :, :, lanes].reshape(both, HD).astype(F32)
            r = inv[...]
            grad = r * gained - raw[:, lanes] * (r * r * r) * spread_dot
            dqkv[t, :, :, :, lanes] = grad.astype(BF16).reshape(2, seqs, blk, HD)

    def rf_copy(i, off):
        return remote(st_z.at[:, ds(off, cw)], rx_f.at[i], rzs.at[3, i, 0], rzr.at[3, i, 0], ctx, zp(i + 1))

    def in_partial(core, off):
        here = ds(off, cw)
        acc = None
        for t in range(3):
            left = dqkv[t, pl.ds(core, 1)].reshape(rows, head_w)
            term = lax.dot_general(left, w[t][here, :], NT, preferred_element_type=F32)
            acc = term if acc is None else acc + term
        return acc

    own_rows = ds(z * share_rows, share_rows)
    for i in range(tps):
        off = zp(i + 1) * cw
        st_p[:, ds(off, cw)] = in_partial(ok, off).astype(BF16)
        rp_copy(3, i, off).start()
        mine = in_partial(k, off)
        rp_copy(3, i, off).wait_recv()
        st_z[:, ds(off, cw)] = (mine + rx_p[1, :, ds(off, cw)].astype(F32)).astype(BF16)
        st_z[own_rows, ds(off, cw)] = (st_z[own_rows, ds(off, cw)].astype(F32) + dhid[:, ds(off, cw)]).astype(BF16)
        if i < tps - 1:
            rf_copy(i, off).start()

    pass_g(5)
    pass_g(3)
    for m in range(3):

        def gqkv_step(j, carry):
            here = ds(j * 512, 512)
            right = dqkv[m].reshape(both, head_w)
            w[m][here, :] = jnp.dot(tok_t[here, :], right, preferred_element_type=F32).astype(BF16)
            return carry

        free_w(m)
        lax.fori_loop(0, width // 512, gqkv_step, 0)
        send_g(m)
    middle = gg_row[:, ds(z * feats, feats)]
    for i, copy in enumerate(gains_z):
        copy.wait_recv()
        middle = middle + gg_rx1[i]
    gg_mid[...] = gg_mid[...] + middle
    gains_c = []
    n = 0
    for i, d in slots:
        if i or d:
            core = (k + d) % 2
            gains_c.append(go(remote(gg_mid.at[:, ds(chip(i) * 128, 128)], gg_rx2.at[n], ms.at[5, n], mr.at[5, n], chip(i) * 2 + core, z)))
            n += 1

    for m in range(3):
        pass_g(m)
    for i in range(tps - 1):
        rf_copy(i, zp(i + 1) * cw).wait_recv()
    final = st_z[:, ds(z * feats, cw)].astype(F32)
    for i in range(tps - 1):
        final = final + rx_f[i].astype(F32)
    gin_ref[...] = final
    for i in range(tps):
        rp_copy(3, i, zp(i + 1) * cw).wait_send()
        if i < tps - 1:
            rf_copy(i, zp(i + 1) * cw).wait_send()
    gain_sum = gg_mid[:, ds(c * 128, 128)]
    for i, copy in enumerate(gains_c):
        copy.wait_recv()
        gain_sum = gain_sum + gg_rx2[i]
    ggain_ref[...] = gain_sum
    own_out.wait()
    for copy in out_z:
        copy.wait_recv()
    for copy in g_own:
        copy.wait()
    for m in g_live:
        wait_g(m)
    for copy in pending:
        copy.wait_send()


def fused(
    tokens,
    w_query,
    w_key,
    w_value,
    w_output,
    w_gate,
    w_up,
    w_down,
    gain_query,
    gain_key,
    gain_attention,
    gain_feedforward,
    block_order,
    cotangent,
):
    seqs, blk, feats = tokens.shape
    tps = lax.axis_size("tp")
    chips = lax.axis_size("ctx") // 2
    width = feats * tps
    rows = seqs * blk
    both = 2 * rows
    share_rows = rows // tps
    total = 2 * chips * blk
    head_w = w_query.shape[1] // 2
    ff_w = w_gate.shape[1] // 2
    heads = head_w // HD
    slab = width // (2 * chips)
    ctx = lax.axis_index("ctx")
    chip = ctx // 2
    pair = lax.dynamic_slice_in_dim(block_order, 2 * chip, 2, 1)
    inner = jnp.arange(blk, dtype=jnp.int32)
    positions = (pair.T[:, :, None] * blk + inner).reshape(both)
    frequency = THETA ** (-2.0 * jnp.arange(HD // 2, dtype=F32) / HD)
    angles = positions.astype(F32)[:, None] * frequency
    cosine, sine = jnp.cos(angles), jnp.sin(angles)
    cosf = jnp.concatenate([cosine, cosine], axis=1)
    sinf = jnp.concatenate([-sine, sine], axis=1)
    mine = lax.dynamic_slice_in_dim(block_order, chip // heads, 1, 0)
    order = (mine.reshape(-1, 1) * blk + inner).reshape(total)
    pos_row = jnp.broadcast_to(order[None, :], (8, total))
    pos_col = jnp.broadcast_to(order[:, None], (total, 128))
    gains = jnp.stack([gain_query, gain_key, gain_attention, gain_feedforward]).astype(F32)
    gains = jnp.pad(gains, ((0, 4), (0, 0)))
    blank = jnp.zeros_like(gains)
    gtile = jnp.where(ctx % 2 == 0, jnp.concatenate([gains, blank], axis=1), jnp.concatenate([blank, gains], axis=1))
    weights = (w_query, w_key, w_value, w_output, w_gate, w_up, w_down)
    dims = (chips, tps, seqs, blk, width, head_w, ff_w)
    halves = (head_w, head_w, head_w, head_w, ff_w, ff_w, ff_w)
    hbm = pl.BlockSpec(memory_space=pl.ANY)
    vmem = pl.BlockSpec(memory_space=pltpu.VMEM)

    def v(shape, dtype=BF16):
        return pltpu.VMEM(shape, dtype)

    w_shapes = [v((width, h)) if m in COLS else v((h, width)) for m, h in enumerate(halves)]
    dma = pltpu.SemaphoreType.DMA
    v_shapes = [v((2, slab, h)) if m in COLS else v((2, h, slab)) for m, h in enumerate(halves)]
    scratch = w_shapes + v_shapes + [
        v((both, width)),
        v((width, both)),
        v((both, width)),
        v((width, both)),
        v((both, width)),
        v((both, width)),
        v((both, ff_w), F32),
        v((both, ff_w), F32),
        v((both, ff_w)),
        v((ff_w, both)),
        v((both, ff_w)),
        v((both, ff_w)),
        v((rows, width)),
        v((2, rows, width)),
        v((rows, width)),
        v((2, tps - 1, share_rows, width)),
        v((tps - 1, rows, feats)),
        v((both, head_w), F32),
        v((both, head_w), F32),
        v((3, 2, seqs, blk, head_w)),
        v((3, 2 * chips, blk, HD)),
        v((total, total)),
        v((total, HD), F32),
        v((2 * chips, blk, HD)),
        v((2, seqs, blk, head_w)),
        v((head_w, both)),
        v((2, seqs, blk, head_w)),
        v((2 * chips, blk, HD)),
        v((total, HD), F32),
        v((total, HD), F32),
        v((3, 2 * chips, blk, HD)),
        v((3, 2, seqs, blk, head_w)),
        v((2, 8, both), F32),
        v((2, 2 * tps - 1, 8, both), F32),
        v((both, 128), F32),
        v((both, 128), F32),
        v((share_rows, width)),
        v((share_rows, width), F32),
        v((share_rows, width), F32),
        v((share_rows, width), F32),
        v((share_rows, width), F32),
        v((2 * chips, 8, 128), F32),
        v((tps, 2 * chips, 8, 128), F32),
        v((8, width), F32),
        v((8, head_w), F32),
        v((8, width), F32),
        v((tps - 1, 8, feats), F32),
        v((8, feats), F32),
        v((2 * chips - 1, 8, 128), F32),
        dma((7, 2 * chips)),
        dma((7, 2 * chips)),
        dma((7, 2 * chips)),
        dma((7, 2 * chips)),
        dma((4, tps - 1)),
        dma((4, tps - 1)),
        dma((4, tps)),
        dma((4, tps)),
        dma((4, tps)),
        dma((4, tps)),
        dma((4, tps, tps - 1)),
        dma((4, tps, tps - 1)),
        dma((6, 2 * chips)),
        dma((6, 2 * chips)),
        dma((2, 2 * tps - 1)),
        dma((2, 2 * tps - 1)),
        dma((4, chips - 1)),
        dma((4, chips - 1)),
        dma((25,)),
    ]
    results = pl.pallas_call(
        functools.partial(layer_kernel, dims),
        out_shape=[
            jax.ShapeDtypeStruct((rows, feats), F32),
            jax.ShapeDtypeStruct((rows, feats), F32),
            jax.ShapeDtypeStruct((8, 128), F32),
        ]
        + [jax.ShapeDtypeStruct((3,) + weight.shape, BF16) for weight in weights],
        in_specs=[hbm] * 9 + [vmem] * 5,
        out_specs=[hbm, vmem, vmem] + [hbm] * 7,
        scratch_shapes=scratch,
        compiler_params=pltpu.CompilerParams(
            collective_id=0, has_side_effects=True, vmem_limit_bytes=67043328
        ),
        name="layer",
    )(tokens.reshape(rows, feats), cotangent.reshape(rows, feats), *weights, gtile, cosf, sinf, pos_row, pos_col)
    output = results[0].reshape(tokens.shape)
    grad_input = results[1].reshape(tokens.shape)
    grads = [jnp.sum(received.astype(F32), axis=0) for received in results[3:]]
    lanes = lax.dynamic_slice_in_dim(results[2], (ctx % 2) * 64, 64, 1)
    return (output, grad_input, *grads, lanes[2], lanes[3], lanes[0], lanes[1])


def fits(mesh):
    return mesh.shape["ctx"] == 8 and mesh.shape["tp"] == 4


def solution(mesh):
    placed = (
        P(None, "ctx", "tp"),
        P("ctx", "tp"),
        P("ctx", "tp"),
        P("ctx", "tp"),
        P("tp", "ctx"),
        P("ctx", "tp"),
        P("ctx", "tp"),
        P("tp", "ctx"),
        P(("tp", "ctx")),
        P(("tp", "ctx")),
        P(("tp", "ctx")),
        P(("tp", "ctx")),
        P(),
        P(None, "ctx", "tp"),
    )
    return jax.shard_map(
        fused if fits(mesh) else shards,
        mesh=mesh,
        in_specs=placed,
        out_specs=(
            P(None, "ctx", "tp"),
            P(None, "ctx", "tp"),
            P("ctx", "tp"),
            P("ctx", "tp"),
            P("ctx", "tp"),
            P("tp", "ctx"),
            P("ctx", "tp"),
            P("ctx", "tp"),
            P("tp", "ctx"),
            P(("tp", "ctx")),
            P(("tp", "ctx")),
            P(("tp", "ctx")),
            P(("tp", "ctx")),
        ),
        check_vma=False,
    )
```

```python
import functools

import jax
import jax.numpy as jnp
import numpy as np
from jax import lax
from jax.experimental import pallas as pl
from jax.experimental.pallas import tpu as pltpu
from jax.sharding import PartitionSpec as P

HD = 128


EPS = 1e-06
THETA = 500000.0
NEGATIVE = -1e30


def full_width(value):
    return lax.all_gather(value, "tp", axis=2, tiled=True)


def share(value):
    return lax.psum_scatter(value, "tp", scatter_dimension=2, tiled=True)


def tp_total(values):
    return lax.psum(values, "tp")


def rotary_tables(positions):
    half_dim = HD // 2
    frequency = THETA ** (-2.0 * jnp.arange(half_dim, dtype=jnp.float32) / HD)
    angles = positions.astype(jnp.float32)[..., None] * frequency
    return (jnp.cos(angles)[..., None, :], jnp.sin(angles)[..., None, :])


def rotate(value, cosine, sine):
    half_dim = value.shape[-1] // 2
    first, second = (value[..., :half_dim], value[..., half_dim:])
    return jnp.concatenate(
        [first * cosine - second * sine, second * cosine + first * sine], axis=-1
    )


def unrotate(grad, cosine, sine):
    half_dim = grad.shape[-1] // 2
    first, second = (grad[..., :half_dim], grad[..., half_dim:])
    return jnp.concatenate(
        [first * cosine + second * sine, second * cosine - first * sine], axis=-1
    )


def key_positions(block_order, start, count, block_len):
    slots = start + jnp.arange(count, dtype=jnp.int32)
    owner = slots // block_len
    ranks = jnp.arange(block_order.shape[1], dtype=jnp.int32)
    chosen = jnp.sum(
        jnp.where(owner[None, :, None] == ranks[None, None, :], block_order[:, None, :], 0), axis=2
    )
    return chosen * block_len + slots % block_len


def span_of():
    return 512


def shards(
    tokens,
    w_query,
    w_key,
    w_value,
    w_output,
    w_gate,
    w_up,
    w_down,
    gain_query,
    gain_key,
    gain_attention,
    gain_feedforward,
    block_order,
    cotangent,
):
    gathered = (
        lax.all_gather(w_query, "ctx", axis=0, tiled=True),
        lax.all_gather(w_key, "ctx", axis=0, tiled=True),
        lax.all_gather(w_value, "ctx", axis=0, tiled=True),
        lax.all_gather(w_output, "ctx", axis=1, tiled=True),
        lax.all_gather(w_gate, "ctx", axis=0, tiled=True),
        lax.all_gather(w_up, "ctx", axis=0, tiled=True),
        lax.all_gather(w_down, "ctx", axis=1, tiled=True),
        lax.all_gather(gain_query, "ctx", axis=0, tiled=True),
        lax.all_gather(gain_key, "ctx", axis=0, tiled=True),
        lax.all_gather(gain_attention, "ctx", axis=0, tiled=True),
        lax.all_gather(gain_feedforward, "ctx", axis=0, tiled=True),
    )
    wq_full, wk_full, wv_full, wo_full, wg_full, wu_full, wd_full = gathered[:7]
    g_query = gathered[7].astype(jnp.float32)
    g_key = gathered[8].astype(jnp.float32)
    g_attn = gathered[9].astype(jnp.float32)
    g_feed = gathered[10].astype(jnp.float32)
    seq_count, block_len, local_width = tokens.shape
    row_count = seq_count * block_len
    scale = HD ** (-0.5)
    tok_full = full_width(tokens)
    tok_rows = tok_full.reshape(row_count, -1)
    width = tok_rows.shape[1]
    queries = jnp.dot(tok_rows, wq_full, preferred_element_type=jnp.float32)
    keys_raw = jnp.dot(tok_rows, wk_full, preferred_element_type=jnp.float32)
    values_raw = jnp.dot(tok_rows, wv_full, preferred_element_type=jnp.float32)
    head_width = queries.shape[1]
    head_count = head_width // HD
    q_squares, k_squares = tp_total(
        (jnp.sum(queries * queries, axis=1), jnp.sum(keys_raw * keys_raw, axis=1))
    )
    q_inverse = lax.rsqrt(q_squares / width + EPS)[:, None]
    k_inverse = lax.rsqrt(k_squares / width + EPS)[:, None]
    q_normed = queries * q_inverse * g_query
    k_normed = keys_raw * k_inverse * g_key
    ctx_rank = lax.axis_index("ctx")
    ranks = jnp.arange(block_order.shape[1], dtype=jnp.int32)
    my_block = jnp.sum(jnp.where(ranks[None, :] == ctx_rank, block_order, 0), axis=1)
    q_pos = my_block[:, None] * block_len + jnp.arange(block_len, dtype=jnp.int32)[None, :]
    cosine, sine = rotary_tables(q_pos)
    q_rot = rotate(q_normed.reshape(seq_count, block_len, head_count, HD), cosine, sine).astype(
        jnp.bfloat16
    )
    k_rot = rotate(k_normed.reshape(seq_count, block_len, head_count, HD), cosine, sine).astype(
        jnp.bfloat16
    )
    k_flat = k_rot.reshape(seq_count, block_len, head_width)
    v_flat = values_raw.astype(jnp.bfloat16).reshape(seq_count, block_len, head_width)

    def stat_block(state, key_piece, k_pos):
        run_max, run_sum = state
        scores = (
            jnp.einsum("sqhd,skhd->shqk", q_rot, key_piece, preferred_element_type=jnp.float32)
            * scale
        )
        visible = k_pos[:, None, None, :] <= q_pos[:, None, :, None]
        scores = jnp.where(visible, scores, NEGATIVE)
        new_max = jnp.maximum(run_max, jnp.max(scores, axis=-1))
        weights = jnp.where(visible, jnp.exp(scores - new_max[..., None]), 0.0)
        run_sum = run_sum * jnp.exp(run_max - new_max) + jnp.sum(weights, axis=-1)
        return (new_max, run_sum)

    init = (
        jnp.full((seq_count, head_count, block_len), NEGATIVE, jnp.float32),
        jnp.zeros((seq_count, head_count, block_len), jnp.float32),
    )
    fold_key_all = lax.all_gather(k_flat, "ctx", axis=1, tiled=True)
    count = fold_key_all.shape[1]
    span = span_of()

    def fold_one_span(step_index, inner):
        offset = step_index * span
        key_piece = lax.dynamic_slice_in_dim(fold_key_all, offset, span, 1).reshape(
            seq_count, span, head_count, HD
        )
        k_pos = key_positions(block_order, offset, span, block_len)
        return stat_block(inner, key_piece, k_pos)

    run_max, run_sum = lax.fori_loop(0, count // span, fold_one_span, init)
    key_all, val_all = (
        lax.all_gather(k_flat, "ctx", axis=1, tiled=True),
        lax.all_gather(v_flat, "ctx", axis=1, tiled=True),
    )
    log_total = run_max + jnp.log(run_sum)
    total_len = key_all.shape[1]
    total_span = span_of()

    def value_span(step_index, acc):
        offset = step_index * total_span
        key_piece = lax.dynamic_slice_in_dim(key_all, offset, total_span, 1).reshape(
            seq_count, total_span, head_count, HD
        )
        val_piece = lax.dynamic_slice_in_dim(val_all, offset, total_span, 1).reshape(
            seq_count, total_span, head_count, HD
        )
        k_pos = key_positions(block_order, offset, total_span, block_len)
        scores = (
            jnp.einsum("sqhd,skhd->shqk", q_rot, key_piece, preferred_element_type=jnp.float32)
            * scale
        )
        visible = k_pos[:, None, None, :] <= q_pos[:, None, :, None]
        weights = jnp.where(visible, jnp.exp(scores - log_total[..., None]), 0.0).astype(
            jnp.bfloat16
        )
        return acc + jnp.einsum(
            "shqk,skhd->sqhd", weights, val_piece, preferred_element_type=jnp.float32
        )

    attended = lax.fori_loop(
        0,
        total_len // total_span,
        value_span,
        jnp.zeros((seq_count, block_len, head_count, HD), jnp.float32),
    )
    attn_bf = attended.reshape(row_count, head_width).astype(jnp.bfloat16)
    attn_proj = share(
        jnp.dot(attn_bf, wo_full, preferred_element_type=jnp.float32).reshape(
            seq_count, block_len, -1
        )
    )
    (a_squares,) = tp_total((jnp.sum(attn_proj * attn_proj, axis=2),))
    a_inverse = lax.rsqrt(a_squares / width + EPS)[..., None]
    hidden_state = tokens.astype(jnp.float32) + attn_proj * a_inverse * g_attn
    hidden_rows = full_width(hidden_state.astype(jnp.bfloat16)).reshape(row_count, -1)
    gate = jnp.dot(hidden_rows, wg_full, preferred_element_type=jnp.float32)
    up_vals = jnp.dot(hidden_rows, wu_full, preferred_element_type=jnp.float32)
    sigma = jax.nn.sigmoid(gate)
    activation = (gate * sigma * up_vals).astype(jnp.bfloat16)
    mixed = share(
        jnp.dot(activation, wd_full, preferred_element_type=jnp.float32).reshape(
            seq_count, block_len, -1
        )
    )
    (m_squares,) = tp_total((jnp.sum(mixed * mixed, axis=2),))
    m_inverse = lax.rsqrt(m_squares / width + EPS)[..., None]
    output = hidden_state + mixed * m_inverse * g_feed
    upstream = cotangent.astype(jnp.float32)
    (m_dots,) = tp_total((jnp.sum(g_feed * upstream * mixed, axis=2),))
    d_mixed = m_inverse * (g_feed * upstream) - mixed * m_inverse**3 * (m_dots / width)[..., None]
    d_gfeed = jnp.sum(upstream * mixed * m_inverse, axis=(0, 1))
    d_mixed_rows = full_width(d_mixed.astype(jnp.bfloat16)).reshape(row_count, -1)
    grad_down = jnp.dot(activation.T, d_mixed_rows, preferred_element_type=jnp.float32)
    d_act = jnp.dot(d_mixed_rows, wd_full.T, preferred_element_type=jnp.float32)
    d_up_bf = (d_act * gate * sigma).astype(jnp.bfloat16)
    d_gate_bf = (d_act * up_vals * sigma * (1.0 + gate * (1.0 - sigma))).astype(jnp.bfloat16)
    grad_gate = jnp.dot(hidden_rows.T, d_gate_bf, preferred_element_type=jnp.float32)
    grad_up = jnp.dot(hidden_rows.T, d_up_bf, preferred_element_type=jnp.float32)
    back_ff = jnp.dot(d_gate_bf, wg_full.T, preferred_element_type=jnp.float32) + jnp.dot(
        d_up_bf, wu_full.T, preferred_element_type=jnp.float32
    )
    d_hidden = upstream + share(back_ff.reshape(seq_count, block_len, -1))
    (a_dots,) = tp_total((jnp.sum(g_attn * d_hidden * attn_proj, axis=2),))
    d_attn = (
        a_inverse * (g_attn * d_hidden) - attn_proj * a_inverse**3 * (a_dots / width)[..., None]
    )
    d_gattn = jnp.sum(d_hidden * attn_proj * a_inverse, axis=(0, 1))
    d_attn_rows = full_width(d_attn.astype(jnp.bfloat16)).reshape(row_count, -1)
    grad_outproj = jnp.dot(attn_bf.T, d_attn_rows, preferred_element_type=jnp.float32)
    d_heads = jnp.dot(d_attn_rows, wo_full.T, preferred_element_type=jnp.float32).reshape(
        seq_count, block_len, head_count, HD
    )
    deltas = jnp.sum(d_heads * attended, axis=3).transpose(0, 2, 1)
    d_heads_bf = d_heads.astype(jnp.bfloat16)

    def grad_block(key_piece, val_piece, k_pos):
        scores = (
            jnp.einsum("sqhd,skhd->shqk", q_rot, key_piece, preferred_element_type=jnp.float32)
            * scale
        )
        visible = k_pos[:, None, None, :] <= q_pos[:, None, :, None]
        probs = jnp.where(visible, jnp.exp(scores - log_total[..., None]), 0.0)
        d_probs = jnp.einsum(
            "sqhd,skhd->shqk", d_heads_bf, val_piece, preferred_element_type=jnp.float32
        )
        d_scores = (probs * (d_probs - deltas[..., None])).astype(jnp.bfloat16)
        return (probs, d_scores)

    def query_span(step_index, acc):
        offset = step_index * total_span
        key_piece = lax.dynamic_slice_in_dim(key_all, offset, total_span, 1).reshape(
            seq_count, total_span, head_count, HD
        )
        val_piece = lax.dynamic_slice_in_dim(val_all, offset, total_span, 1).reshape(
            seq_count, total_span, head_count, HD
        )
        k_pos = key_positions(block_order, offset, total_span, block_len)
        probs, d_scores = grad_block(key_piece, val_piece, k_pos)
        return (
            acc
            + jnp.einsum("shqk,skhd->sqhd", d_scores, key_piece, preferred_element_type=jnp.float32)
            * scale
        )

    d_qrot = lax.fori_loop(
        0,
        total_len // total_span,
        query_span,
        jnp.zeros((seq_count, block_len, head_count, HD), jnp.float32),
    )
    count = block_len * lax.axis_size("ctx")
    key_span = span_of()

    def key_one_span(step_index, buffer):
        offset = step_index * key_span
        key_piece = lax.dynamic_slice_in_dim(key_all, offset, key_span, 1).reshape(
            seq_count, key_span, head_count, HD
        )
        val_piece = lax.dynamic_slice_in_dim(val_all, offset, key_span, 1).reshape(
            seq_count, key_span, head_count, HD
        )
        k_pos = key_positions(block_order, offset, key_span, block_len)
        probs, d_scores = grad_block(key_piece, val_piece, k_pos)
        d_keyp = (
            jnp.einsum("shqk,sqhd->skhd", d_scores, q_rot, preferred_element_type=jnp.float32)
            * scale
        )
        d_valp = jnp.einsum(
            "shqk,sqhd->skhd",
            probs.astype(jnp.bfloat16),
            d_heads_bf,
            preferred_element_type=jnp.float32,
        )
        both = jnp.concatenate(
            [
                d_keyp.reshape(seq_count, key_span, head_width),
                d_valp.reshape(seq_count, key_span, head_width),
            ],
            axis=2,
        )
        return lax.dynamic_update_slice_in_dim(buffer, both.transpose(1, 0, 2), offset, 0)

    key_sums = (
        lax.psum_scatter(
            lax.fori_loop(
                0,
                count // key_span,
                key_one_span,
                jnp.zeros((count, seq_count, 2 * head_width), jnp.float32),
            ).astype(jnp.bfloat16),
            "ctx",
            scatter_dimension=0,
            tiled=True,
        )
        .astype(jnp.float32)
        .transpose(1, 0, 2)
    )
    d_krot = key_sums[..., :head_width].reshape(seq_count, block_len, head_count, HD)
    d_values = key_sums[..., head_width:].reshape(row_count, head_width)
    dq_normed = unrotate(d_qrot, cosine, sine).reshape(row_count, head_width)
    dk_normed = unrotate(d_krot, cosine, sine).reshape(row_count, head_width)
    q_dots, k_dots = tp_total(
        (
            jnp.sum(g_query * dq_normed * queries, axis=1),
            jnp.sum(g_key * dk_normed * keys_raw, axis=1),
        )
    )
    d_queries = (
        q_inverse * (g_query * dq_normed) - queries * q_inverse**3 * (q_dots / width)[:, None]
    )
    d_keys = k_inverse * (g_key * dk_normed) - keys_raw * k_inverse**3 * (k_dots / width)[:, None]
    d_gquery = jnp.sum(dq_normed * queries * q_inverse, axis=0)
    d_gkey = jnp.sum(dk_normed * keys_raw * k_inverse, axis=0)
    dq_bf = d_queries.astype(jnp.bfloat16)
    dk_bf = d_keys.astype(jnp.bfloat16)
    dv_bf = d_values.astype(jnp.bfloat16)
    grad_q = jnp.dot(tok_rows.T, dq_bf, preferred_element_type=jnp.float32)
    grad_k = jnp.dot(tok_rows.T, dk_bf, preferred_element_type=jnp.float32)
    grad_v = jnp.dot(tok_rows.T, dv_bf, preferred_element_type=jnp.float32)
    back_attn = (
        jnp.dot(dq_bf, wq_full.T, preferred_element_type=jnp.float32)
        + jnp.dot(dk_bf, wk_full.T, preferred_element_type=jnp.float32)
        + jnp.dot(dv_bf, wv_full.T, preferred_element_type=jnp.float32)
    )
    grad_input = d_hidden + share(back_attn.reshape(seq_count, block_len, -1))
    summed = (
        lax.psum_scatter(
            grad_q.astype(jnp.bfloat16), "ctx", scatter_dimension=0, tiled=True
        ).astype(jnp.float32),
        lax.psum_scatter(
            grad_k.astype(jnp.bfloat16), "ctx", scatter_dimension=0, tiled=True
        ).astype(jnp.float32),
        lax.psum_scatter(
            grad_v.astype(jnp.bfloat16), "ctx", scatter_dimension=0, tiled=True
        ).astype(jnp.float32),
        lax.psum_scatter(
            grad_outproj.astype(jnp.bfloat16), "ctx", scatter_dimension=1, tiled=True
        ).astype(jnp.float32),
        lax.psum_scatter(
            grad_gate.astype(jnp.bfloat16), "ctx", scatter_dimension=0, tiled=True
        ).astype(jnp.float32),
        lax.psum_scatter(
            grad_up.astype(jnp.bfloat16), "ctx", scatter_dimension=0, tiled=True
        ).astype(jnp.float32),
        lax.psum_scatter(
            grad_down.astype(jnp.bfloat16), "ctx", scatter_dimension=1, tiled=True
        ).astype(jnp.float32),
        lax.psum_scatter(
            d_gquery.astype(jnp.bfloat16), "ctx", scatter_dimension=0, tiled=True
        ).astype(jnp.float32),
        lax.psum_scatter(
            d_gkey.astype(jnp.bfloat16), "ctx", scatter_dimension=0, tiled=True
        ).astype(jnp.float32),
        lax.psum_scatter(
            d_gattn.astype(jnp.bfloat16), "ctx", scatter_dimension=0, tiled=True
        ).astype(jnp.float32),
        lax.psum_scatter(
            d_gfeed.astype(jnp.bfloat16), "ctx", scatter_dimension=0, tiled=True
        ).astype(jnp.float32),
    )
    return (
        output,
        grad_input,
        summed[0],
        summed[1],
        summed[2],
        summed[3],
        summed[4],
        summed[5],
        summed[6],
        summed[7],
        summed[8],
        summed[9],
        summed[10],
    )


MESH = pl.DeviceIdType.MESH
NT = (((1,), (1,)), ((), ()))
TN = (((0,), (0,)), ((), ()))
F32 = jnp.float32
BF16 = jnp.bfloat16
COLS = (0, 1, 2, 4, 5)


def layer_kernel(dims, *refs):
    (chips, tps, seqs, blk, width, head_w, ff_w) = dims
    rows = seqs * blk
    both = 2 * rows
    share_rows = rows // tps
    feats = width // tps
    heads = head_w // HD
    slab = width // (2 * chips)
    halves = (head_w, head_w, head_w, head_w, ff_w, ff_w, ff_w)
    total = 2 * chips * blk
    scale = HD ** (-0.5)
    it = iter(refs)

    def take(n):
        return [next(it) for _ in range(n)]

    (tok_in, cot_in) = take(2)
    w_in = take(7)
    (blocks, gtile, table) = take(3)
    (out_ref, gin_ref, ggain_ref) = take(3)
    rx_g = take(7)
    w = take(7)
    via = take(7)
    (tok, tok_t, hid, hid_t, dmix, dattn) = take(6)
    (lin, fac, act, act_t, dgate, dup) = take(6)
    (st_p, rx_p, st_z, rx_z, rx_f) = take(5)
    (q_raw, k_raw, qkv, qa, probs, att_f, att_st, att, att_t) = take(9)
    (dh, d_o, dqkv_st, dqkv) = take(4)
    (sq_own, sq_rx, inv_q, inv_k) = take(4)
    (cot, proj, hstate, dhid, stage) = take(5)
    (gbuf, gall, gfull, gqk, gg_row, gg_rx1, gg_mid, gg_rx2) = take(8)
    (ws, wr, gs, gr) = take(4)
    (zs, zr, ps, pr) = take(4)
    (rps, rpr, rzs, rzr) = take(4)
    (ms, mr) = take(2)
    (ss, sr) = take(2)
    (as_, ar) = take(2)
    (loc,) = take(1)
    (d_acc, cosf, sinf, pos_row) = take(4)
    (xs, xr) = take(2)

    ctx = lax.axis_index("ctx")
    z = lax.axis_index("tp")
    c = ctx // 2
    k = ctx % 2
    ok = 1 - k
    partner = c * 2 + ok
    near = (c + 1 - 2 * (c % 2), (c + 2) % chips)
    far = chips - 1 - c

    def zp(i):
        return (z + i) % tps

    def chip(i):
        return (c + i) % chips

    def ds(start, size):
        return pl.ds(pl.multiple_of(start, size), size)

    def remote(src, dst, ssem, rsem, to_ctx, to_z):
        return pltpu.make_async_remote_copy(
            src_ref=src,
            dst_ref=dst,
            send_sem=ssem,
            recv_sem=rsem,
            device_id=(to_ctx, to_z),
            device_id_type=MESH,
        )

    peers = [(chip(i) * 2 + (k + d) % 2, z) for i in range(chips) for d in range(2) if i or d]
    peers += [(ctx, zp(i)) for i in range(1, tps)]
    peers += [(partner, zp(i)) for i in range(1, tps)]
    barrier = pltpu.get_barrier_semaphore()
    for peer in peers:
        pl.semaphore_signal(barrier, inc=1, device_id=peer, device_id_type=MESH)

    pending = []

    def go(copy):
        copy.start()
        pending.append(copy)
        return copy

    def slab_of(m, owner):
        if m in COLS:
            return w[m].at[ds(owner * slab, slab), :]
        return w[m].at[:, ds(owner * slab, slab)]

    def half_of(m, core):
        if m in COLS:
            return w_in[m].at[:, ds(core * halves[m], halves[m])]
        return w_in[m].at[ds(core * halves[m], halves[m]), :]

    w_own = {}
    w_pass = {}
    w_wait = {}

    def w_slot(m, n, owner):
        return remote(slab_of(m, owner), slab_of(m, owner), ws.at[m, n], wr.at[m, n], partner, z)

    def send_w(m, d):
        core = (k + d) % 2
        for n in range(2):
            go(remote(half_of(m, core), slab_of(m, ctx), ws.at[m, 2 * n + d], wr.at[m, 2 * n + k], near[n] * 2 + core, z))
        if d:
            go(remote(half_of(m, ok), slab_of(m, ctx), ws.at[m, 4], wr.at[m, 4], partner, z))
        else:
            w_own[m] = pltpu.make_async_copy(half_of(m, k), slab_of(m, ctx), loc.at[m])
            w_own[m].start()

    def source(n):
        if n < 4:
            return near[n // 2] * 2 + n % 2
        return partner if n == 4 else far * 2 + n - 5

    def got_w(m, *which):
        for n in which:
            if (m, n) not in w_wait:
                w_wait[m, n] = True
                w_slot(m, n, source(n)).wait_recv()

    def pass_w(m):
        for n in range(2):
            got_w(m, 3 * n)
            mine = slab_of(m, source(3 * n))
            copy = remote(mine, mine, ws.at[m, 5 + n], wr.at[m, 5 + n], near[1 - n] * 2 + k, z)
            copy.start()
            w_pass[m, n] = copy

    def free_w(m):
        for n in range(2):
            w_pass[m, n].wait_send()

    def wait_w(m):
        w_own[m].wait()
        got_w(m, *range(7))

    def into(m, n, core):
        if m in COLS:
            return rx_g[m].at[n, :, ds(core * halves[m], halves[m])]
        return rx_g[m].at[n, ds(core * halves[m], halves[m]), :]

    g_live = []
    g_own = []

    def send_far(m):
        for n in range(2):
            go(remote(slab_of(m, far * 2 + n), via[m].at[n], gs.at[m, n], gr.at[m, n], near[n] * 2 + k, z))

    def send_near(m, n):
        go(remote(slab_of(m, near[n] * 2 + n), into(m, 1 + n, k), gs.at[m, 2 + n], gr.at[m, 2 + 2 * n + k], near[n] * 2 + n, z))

    def send_home(m):
        go(remote(slab_of(m, partner), into(m, 0, k), gs.at[m, 6], gr.at[m, 6], partner, z))
        copy = pltpu.make_async_copy(slab_of(m, ctx), into(m, 0, k), loc.at[8 + m])
        copy.start()
        g_own.append(copy)

    def send_g(m):
        send_far(m)
        send_near(m, 0)
        send_near(m, 1)
        send_home(m)

    def pass_g(m):
        for n in range(2):
            to = near[1 - n] * 2 + n
            remote(via[m].at[n], via[m].at[n], gs.at[m, n], gr.at[m, n], partner, z).wait_recv()
            total = slab_of(m, to)[...].astype(F32) + via[m][n].astype(F32)
            slab_of(m, to)[...] = total.astype(BF16)
            go(remote(slab_of(m, to), into(m, 2 - n, k), gs.at[m, 4 + n], gr.at[m, 2 + 2 * (1 - n) + k], to, z))
        g_live.append(m)

    def wait_g(m):
        for n in range(2):
            for core in range(2):
                here = into(m, 1 + n, core)
                remote(here, here, gs.at[m, 0], gr.at[m, 2 + 2 * n + core], partner, z).wait_recv()
        here = into(m, 0, ok)
        remote(here, here, gs.at[m, 6], gr.at[m, 6], partner, z).wait_recv()

    own_tok = pltpu.make_async_copy(tok_in, tok.at[ds(k * rows, rows), ds(z * feats, feats)], loc.at[16])
    own_tok.start()
    own_cot = pltpu.make_async_copy(cot_in.at[ds(z * share_rows, share_rows), :], cot.at[:, ds(z * feats, feats)], loc.at[17])
    own_cot.start()
    own_gain = pltpu.make_async_copy(gtile, gbuf.at[ctx], loc.at[18])
    own_gain.start()
    pl.semaphore_wait(barrier, len(peers))

    tok_z = []
    for i in range(1, tps):
        tok_z.append(go(remote(tok_in, tok.at[ds(k * rows, rows), ds(z * feats, feats)], zs.at[0, i - 1], zr.at[0, i - 1], ctx, zp(i))))
    tok_p = [go(remote(tok_in, tok.at[ds(k * rows, rows), ds(z * feats, feats)], ps.at[0, 0], pr.at[0, 0], partner, z))]
    slots = [(i, d) for i in range(chips) for d in range(2)]
    gain1 = []
    n = 0
    for i, d in slots:
        if i or d:
            gain1.append(go(remote(gtile, gbuf.at[ctx], ms.at[0, n], mr.at[0, n], chip(i) * 2 + (k + d) % 2, z)))
            n += 1
    cot_z = []
    for i in range(1, tps):
        cot_z.append(go(remote(cot_in.at[ds(zp(i) * share_rows, share_rows), :], cot.at[:, ds(z * feats, feats)], ms.at[1, i - 1], mr.at[1, i - 1], ctx, zp(i))))
    for m in (0, 1, 2, 3):
        send_w(m, 0)
        send_w(m, 1)

    own_gain.wait()
    for copy in gain1:
        copy.wait_recv()
    own_gain2 = pltpu.make_async_copy(gbuf, gall.at[z], loc.at[19])
    own_gain2.start()
    gain2 = []
    for i in range(1, tps):
        gain2.append(go(remote(gbuf, gall.at[z], ms.at[2, i - 1], mr.at[2, i - 1], ctx, zp(i))))
    for r in range(2):
        pieces = [gbuf[4 * k + 2 * m, r : r + 1, :] + gbuf[4 * k + 2 * m + 1, r : r + 1, :] for m in range(head_w // 128)]
        gqk[r : r + 1, :] = jnp.concatenate(pieces, axis=1)

    lane = lax.broadcasted_iota(jnp.int32, (blk, HD), 1)
    sign = jnp.where(lane < HD // 2, -1.0, 1.0)
    for core in range(2):
        for s in range(seqs):
            block = blocks[s, 2 * c + core]
            c_block, s_block = table[0, pl.ds(block, 1), :], table[1, pl.ds(block, 1), :]
            c_in, s_in = table[2], table[3]
            here = slice((core * seqs + s) * blk, (core * seqs + s + 1) * blk)
            cosf[here, :] = c_block * c_in - s_block * s_in
            sinf[here, :] = (s_block * c_in + c_block * s_in) * sign
    for j in range(2 * chips):
        start = blocks[c // heads, j] * blk
        here = slice(j * blk, (j + 1) * blk)
        pos_row[:, here] = start + lane[0:8, :]

    own_tok.wait()
    for i in range(1, tps):
        tok_z[i - 1].wait_recv()
        part = tok.at[ds(k * rows, rows), ds(((z - i) % tps) * feats, feats)]
        tok_p.append(go(remote(part, part, ps.at[0, i], pr.at[0, i], partner, z)))
    for m in (0, 1, 2, 3):
        pass_w(m)
    send_w(4, 0)
    for copy in tok_p:
        copy.wait_recv()

    def row_of(value):
        folded = value[:, :128]
        for h in range(1, heads):
            folded = folded + value[:, h * 128 : (h + 1) * 128]
        return jnp.sum(jnp.transpose(folded), axis=0, keepdims=True)

    def column_of(row):
        return jnp.transpose(jnp.broadcast_to(row, (128, both)))

    def totals(idx):
        copies = []
        n = 0
        for i in range(tps):
            for d in range(2):
                if i or d:
                    to = ctx if d == 0 else partner
                    copies.append(go(remote(sq_own.at[idx], sq_rx.at[idx, n], ss.at[idx, n], sr.at[idx, n], to, zp(i))))
                    n += 1
        total = sq_own[idx]
        for j, copy in enumerate(copies):
            copy.wait_recv()
            total = total + sq_rx[idx, j]
        return total

    for m in (0, 1, 2):
        wait_w(m)
        value = jnp.dot(tok[...], w[m][...], preferred_element_type=F32)
        if m == 0:
            q_raw[...] = value
            sq_own[0, 0:1, :] = row_of(value * value)
        elif m == 1:
            k_raw[...] = value
            sq_own[0, 1:2, :] = row_of(value * value)
        else:
            qkv[2] = value.astype(BF16).reshape(2, seqs, blk, head_w)
    sq_own[0, 2:8, :] = jnp.zeros((6, both), F32)
    squares = totals(0)
    inverse = lax.rsqrt(squares / width + EPS)
    inv_q[...] = column_of(inverse[0:1, :])
    inv_k[...] = column_of(inverse[1:2, :])
    for t, (raw, inv) in enumerate(((q_raw, inv_q), (k_raw, inv_k))):
        for h in range(heads):
            lanes = slice(h * HD, (h + 1) * HD)
            normed = raw[:, lanes] * inv[...] * gqk[t : t + 1, lanes]
            turned = normed * cosf[...] + pltpu.roll(normed, HD // 2, 1) * sinf[...]
            qkv[t, :, :, :, lanes] = turned.astype(BF16).reshape(2, seqs, blk, HD)

    def to_owner(idx, value, owned, stacked):
        copies = []
        for i in range(chips):
            to = chip(i)
            s, h = to // heads, to % heads
            if stacked:
                src = value.at[:, :, s, :, ds(h * HD, HD)]
                dst = owned.at[:, ds(2 * c, 2)]
            else:
                src = value.at[:, s, :, ds(h * HD, HD)]
                dst = owned.at[ds(2 * c, 2)]
            if i:
                copies.append(go(remote(src, dst, as_.at[idx, i - 1], ar.at[idx, i - 1], to * 2 + k, z)))
            else:
                own = pltpu.make_async_copy(src, dst, loc.at[20 + idx])
                own.start()
        return own, copies

    def from_owner(idx, owned, value, stacked):
        s, h = c // heads, c % heads
        copies = []
        for i in range(chips):
            to = chip(i)
            if stacked:
                src = owned.at[:, ds(2 * to, 2)]
                dst = value.at[:, :, s, :, ds(h * HD, HD)]
            else:
                src = owned.at[ds(2 * to, 2)]
                dst = value.at[:, s, :, ds(h * HD, HD)]
            if i:
                copies.append(go(remote(src, dst, as_.at[idx, i - 1], ar.at[idx, i - 1], to * 2 + k, z)))
            else:
                own = pltpu.make_async_copy(src, dst, loc.at[20 + idx])
                own.start()
        return own, copies

    def arrive(pair):
        own, copies = pair
        own.wait()
        for copy in copies:
            copy.wait_recv()

    pair = to_owner(0, qkv, qa, True)
    send_w(4, 1)
    arrive(pair)
    step = 2 * blk

    def attend(i, carry):
        here = ds(i * step, step)
        q = qa[0, pl.ds(2 * i, 2)].reshape(step, HD)
        s = lax.dot_general(q, qa[1].reshape(total, HD), NT, preferred_element_type=F32) * scale
        at = lax.broadcasted_iota(jnp.int32, (step, 1), 0)
        first = blocks[c // heads, 2 * i] * blk
        second = (blocks[c // heads, 2 * i + 1] - 1) * blk
        visible = pos_row[0:1, :] <= at + jnp.where(at < blk, first, second)
        s = jnp.where(visible, s, NEGATIVE)
        top = jnp.max(s, axis=1, keepdims=True)
        e = jnp.where(visible, jnp.exp(s - top), 0.0)
        p = (e * (1.0 / jnp.sum(e, axis=1, keepdims=True))).astype(BF16)
        probs[here, :] = p
        o = jnp.dot(p, qa[2].reshape(total, HD), preferred_element_type=F32)
        att_f[here, :] = o
        att_st[pl.ds(2 * i, 2)] = o.astype(BF16).reshape(2, blk, HD)
        return carry

    lax.fori_loop(0, chips, attend, 0)
    back = from_owner(1, att_st, att, False)
    pass_w(4)
    send_w(5, 0)
    send_w(5, 1)
    send_w(6, 0)
    own_gain2.wait()
    for copy in gain2:
        copy.wait_recv()
    for r in range(2):
        pieces = []
        for zz in range(tps):
            for m in range(chips):
                pieces.append(gall[zz, 2 * m, 2 + r : 3 + r, :] + gall[zz, 2 * m + 1, 2 + r : 3 + r, :])
        gfull[r : r + 1, :] = jnp.concatenate(pieces, axis=1)
    for s in range(width // 256):
        tok_t[s * 256 : (s + 1) * 256, :] = jnp.transpose(tok[:, s * 256 : (s + 1) * 256])
    arrive(back)
    wait_w(3)

    cw = feats
    rs_live = {}

    def rp_copy(idx, i, off):
        return remote(st_p.at[:, ds(off, cw)], rx_p.at[idx % 2, :, ds(off, cw)], rps.at[idx, i], rpr.at[idx, i], partner, z)

    def rz_copy(idx, i, j, off):
        return remote(
            st_z.at[ds(zp(j) * share_rows, share_rows), ds(off, cw)],
            rx_z.at[idx % 2, j - 1, :, ds(off, cw)],
            rzs.at[idx, i, j - 1],
            rzr.at[idx, i, j - 1],
            ctx,
            zp(j),
        )

    def reduce_rows(idx, partial, offset, before=None, meanwhile=None):
        def one(i):
            off = offset(i)
            if before is not None:
                before(i)
            st_p[:, ds(off, cw)] = partial(ok, off).astype(BF16)
            rp_copy(idx, i, off).start()
            mine = partial(k, off)
            rp_copy(idx, i, off).wait_recv()
            st_z[:, ds(off, cw)] = (mine + rx_p[idx % 2, :, ds(off, cw)].astype(F32)).astype(BF16)
            for j in range(1, tps):
                rz_copy(idx, i, j, off).start()

        def finish(i):
            off = offset(i)
            for j in range(1, tps):
                rz_copy(idx, i, j, off).wait_recv()
                rz_copy(idx, i, j, off).wait_send()
            rp_copy(idx, i, off).wait_send()

        if before is None:
            lax.fori_loop(0, tps, lambda i, x: (one(i), x)[1], 0)
        else:
            for i in range(tps):
                one(i)
        if meanwhile is not None:
            meanwhile()
        if before is None:
            lax.fori_loop(0, tps, lambda i, x: (finish(i), x)[1], 0)
        else:
            for i in range(tps):
                finish(i)
        mine = st_z[ds(z * share_rows, share_rows), :].astype(F32)
        for j in range(tps - 1):
            mine = mine + rx_z[idx % 2, j].astype(F32)
        return mine

    def straight(i):
        return i * cw

    def mean_of(value):
        return jnp.sum(value, axis=1, keepdims=True) / width

    def spread(idx, buf):
        mine = buf.at[ds(k * rows + z * share_rows, share_rows), :]
        along = [go(remote(mine, mine, zs.at[idx, i - 1], zr.at[idx, i - 1], ctx, zp(i))) for i in range(1, tps)]
        across = [go(remote(mine, mine, ps.at[idx, 0], pr.at[idx, 0], partner, z))]

        def finish(meanwhile=None):
            for i in range(1, tps):
                along[i - 1].wait_recv()
                if i == 2 and meanwhile is not None:
                    meanwhile()
                part = buf.at[ds(k * rows + ((z - i) % tps) * share_rows, share_rows), :]
                across.append(go(remote(part, part, ps.at[idx, i], pr.at[idx, i], partner, z)))
            for copy in across:
                copy.wait_recv()

        return finish

    my_rows = ds(k * rows + z * share_rows, share_rows)
    heads_rows = [None]

    def o_partial(core, off):
        left = att[pl.ds(core, 1)].reshape(rows, head_w)
        return jnp.dot(left, w[3][:, ds(off, cw)], preferred_element_type=F32)

    value = reduce_rows(0, o_partial, straight)
    proj[...] = value
    a_inverse = lax.rsqrt(mean_of(value * value) + EPS)
    state = tok[my_rows, :].astype(F32) + value * a_inverse * gfull[0:1, :]
    hstate[...] = state
    hid[my_rows, :] = state.astype(BF16)
    finish = spread(1, hid)
    own_cot.wait()
    for copy in cot_z:
        copy.wait_recv()
    att_t[...] = jnp.transpose(att[...].reshape(both, head_w))

    def more_weights():
        pass_w(5)
        send_w(6, 1)

    finish(more_weights)

    fw = 256
    wait_w(4)

    def gate_step(j, carry):
        here = ds(j * fw, fw)
        lin[:, here] = jnp.dot(hid[...], w[4][:, here], preferred_element_type=F32)
        return carry

    lax.fori_loop(0, ff_w // fw, gate_step, 0)
    for s in range(width // 256):
        hid_t[s * 256 : (s + 1) * 256, :] = jnp.transpose(hid[:, s * 256 : (s + 1) * 256])
    wait_w(5)

    def up_step(j, carry):
        here = ds(j * fw, fw)
        up = jnp.dot(hid[...], w[5][:, here], preferred_element_type=F32)
        gate = lin[:, here]
        sigma = jax.nn.sigmoid(gate)
        swish = gate * sigma
        lin[:, here] = swish
        fac[:, here] = up * sigma * (1.0 + gate * (1.0 - sigma))
        value = (swish * up).astype(BF16)
        act[:, here] = value
        act_t[here, :] = jnp.transpose(value)
        return carry

    lax.fori_loop(0, ff_w // fw, up_step, 0)

    def down_partial(core, off):
        return jnp.dot(act[ds(core * rows, rows), :], w[6][:, ds(off, cw)], preferred_element_type=F32)

    def from_chip(i):
        return (c, near[0], near[1], far)[i] * cw

    def down_ready(i):
        if i == 0:
            w_own[6].wait()
        if i == 1:
            pass_w(6)
        got_w(6, *((4,), (0, 1), (2, 3), (5, 6))[i])

    value = reduce_rows(1, down_partial, from_chip, down_ready)
    m_inverse = lax.rsqrt(mean_of(value * value) + EPS)
    scaled = value * m_inverse
    stage[...] = hstate[...] + scaled * gfull[1:2, :]
    for i in range(1, tps):
        go(remote(stage.at[:, ds(zp(i) * feats, feats)], out_ref.at[ds(z * share_rows, share_rows), :], ms.at[3, i - 1], mr.at[3, i - 1], ctx, zp(i)))
    out_z = pending[-(tps - 1) :]
    own_out = pltpu.make_async_copy(stage.at[:, ds(z * feats, feats)], out_ref.at[ds(z * share_rows, share_rows), :], loc.at[24])
    own_out.start()
    upstream = cot[...].astype(F32)
    gained = upstream * gfull[1:2, :]
    gg_row[1:2, :] = jnp.sum(upstream * scaled, axis=0, keepdims=True)
    back_mix = m_inverse * gained - scaled * (m_inverse * m_inverse) * mean_of(gained * value)
    dmix[my_rows, :] = back_mix.astype(BF16)
    order = (far, near[0], near[1], c)

    def mix_along(n, i):
        here = dmix.at[my_rows, ds(order[n] * cw, cw)]
        return remote(here, here, xs.at[n, i - 1], xr.at[n, i - 1], ctx, zp(i))

    def mix_across(n, i):
        owner = (z - i) % tps
        here = dmix.at[ds(k * rows + owner * share_rows, share_rows), ds(order[n] * cw, cw)]
        return remote(here, here, xs.at[n, tps - 1 + i], xr.at[n, tps - 1 + i], partner, z)

    for n in range(chips):
        for i in range(1, tps):
            mix_along(n, i).start()
        mix_across(n, 0).start()

    free_w(6)
    for n in range(chips):
        for i in range(1, tps):
            mix_along(n, i).wait_recv()
            mix_across(n, i).start()
        for i in range(tps):
            mix_across(n, i).wait_recv()
        off = order[n] * cw

        def dact_step(j, carry):
            here = ds(j * fw, fw)
            d_act = lax.dot_general(dmix[:, ds(off, cw)], w[6][here, ds(off, cw)], NT, preferred_element_type=F32)
            part = (ds((j // 2) * both, both), ds((j % 2) * fw, fw))
            if n:
                d_act = d_act + d_acc[part]
            if n < chips - 1:
                d_acc[part] = d_act
            else:
                dup[:, here] = (d_act * lin[:, here]).astype(BF16)
                dgate[:, here] = (d_act * fac[:, here]).astype(BF16)
            return carry

        lax.fori_loop(0, ff_w // fw, dact_step, 0)
        grad = jnp.dot(act_t[...], dmix[:, ds(off, cw)], preferred_element_type=F32)
        w[6][:, ds(off, cw)] = grad.astype(BF16)
        if n == 0:
            send_far(6)
        elif n < chips - 1:
            send_near(6, n - 1)
        else:
            send_home(6)

    for n in range(chips):
        for i in range(1, tps):
            mix_along(n, i).wait_send()
        for i in range(tps):
            mix_across(n, i).wait_send()

    def ff_partial(core, off):
        here = ds(core * rows, rows)
        return lax.dot_general(dgate[here, :], w[4][ds(off, cw), :], NT, preferred_element_type=F32) + lax.dot_general(
            dup[here, :], w[5][ds(off, cw), :], NT, preferred_element_type=F32
        )

    def ggate_step(j, carry):
        here = ds(j * fw, fw)
        w[4][:, here] = jnp.dot(hid_t[...], dgate[:, here], preferred_element_type=F32).astype(BF16)
        return carry

    def gate_grad():
        free_w(4)
        lax.fori_loop(0, ff_w // fw, ggate_step, 0)
        pass_g(6)
        send_g(4)

    value = reduce_rows(2, ff_partial, straight, meanwhile=gate_grad) + cot[...].astype(F32)
    dhid[...] = value
    projected = proj[...]
    a_inverse = lax.rsqrt(mean_of(projected * projected) + EPS)
    scaled = projected * a_inverse
    gained = value * gfull[0:1, :]
    gg_row[0:1, :] = jnp.sum(value * scaled, axis=0, keepdims=True)
    gg_row[2:8, :] = jnp.zeros((6, width), F32)
    back_att = a_inverse * gained - scaled * (a_inverse * a_inverse) * mean_of(gained * projected)
    dattn[my_rows, :] = back_att.astype(BF16)
    finish = spread(3, dattn)
    gains_z = []
    for i in range(1, tps):
        gains_z.append(go(remote(gg_row.at[:, ds(zp(i) * feats, feats)], gg_rx1.at[i - 1], ms.at[4, i - 1], mr.at[4, i - 1], ctx, zp(i))))

    def gup_step(j, carry):
        here = ds(j * fw, fw)
        w[5][:, here] = jnp.dot(hid_t[...], dup[:, here], preferred_element_type=F32).astype(BF16)
        return carry

    free_w(5)
    lax.fori_loop(0, ff_w // fw, gup_step, 0)
    finish()

    value = lax.dot_general(dattn[...], w[3][...], NT, preferred_element_type=F32)
    dh[...] = value.astype(BF16).reshape(2, seqs, blk, head_w)
    pair = to_owner(2, dh, d_o, False)
    pass_g(4)

    def go_step(j, carry):
        here = ds(j * fw, fw)
        w[3][:, here] = jnp.dot(att_t[...], dattn[:, here], preferred_element_type=F32).astype(BF16)
        return carry

    free_w(3)
    lax.fori_loop(0, width // fw, go_step, 0)
    arrive(pair)
    dk_acc, dv_acc = d_acc.at[:, 0:HD], d_acc.at[:, HD : 2 * HD]
    dk_acc[...] = jnp.zeros((total, HD), F32)
    dv_acc[...] = jnp.zeros((total, HD), F32)

    def unattend(i, carry):
        here = ds(i * step, step)
        q = qa[0, pl.ds(2 * i, 2)].reshape(step, HD)
        d_out = d_o[pl.ds(2 * i, 2)].reshape(step, HD)
        d_p = lax.dot_general(d_out, qa[2].reshape(total, HD), NT, preferred_element_type=F32)
        delta = jnp.sum(d_out.astype(F32) * att_f[here, :], axis=1, keepdims=True)
        p = probs[here, :]
        d_s = (p.astype(F32) * (d_p - delta)).astype(BF16)
        d_q = jnp.dot(d_s, qa[1].reshape(total, HD), preferred_element_type=F32) * scale
        dqkv_st[0, pl.ds(2 * i, 2)] = d_q.astype(BF16).reshape(2, blk, HD)
        dk_acc[...] += lax.dot_general(d_s, q, TN, preferred_element_type=F32)
        dv_acc[...] += lax.dot_general(p, d_out, TN, preferred_element_type=F32)
        return carry

    lax.fori_loop(0, chips, unattend, 0)
    dqkv_st[1] = (dk_acc[...] * scale).astype(BF16).reshape(2 * chips, blk, HD)
    dqkv_st[2] = dv_acc[...].astype(BF16).reshape(2 * chips, blk, HD)
    pair = from_owner(3, dqkv_st, dqkv, True)

    send_g(5)
    send_g(3)
    arrive(pair)

    gg_mid[...] = jnp.zeros((8, feats), F32)
    for t, (raw, inv) in enumerate(((q_raw, inv_q), (k_raw, inv_k))):
        folded = None
        for h in range(heads):
            lanes = slice(h * HD, (h + 1) * HD)
            turned = dqkv[t, :, :, :, lanes].reshape(both, HD).astype(F32)
            back_rot = turned * cosf[...] - pltpu.roll(turned, HD // 2, 1) * sinf[...]
            plain = raw[:, lanes]
            scaled = plain * inv[...]
            gg_mid[2 + t : 3 + t, pl.ds(pl.multiple_of(k * head_w + h * HD, HD), HD)] = jnp.sum(back_rot * scaled, axis=0, keepdims=True)
            gained = back_rot * gqk[t : t + 1, lanes]
            dqkv[t, :, :, :, lanes] = gained.astype(BF16).reshape(2, seqs, blk, HD)
            term = gained * plain
            folded = term if folded is None else folded + term
        sq_own[1, t : t + 1, :] = jnp.sum(jnp.transpose(folded), axis=0, keepdims=True)
    sq_own[1, 2:8, :] = jnp.zeros((6, both), F32)
    dots = totals(1) / width
    for t, (raw, inv) in enumerate(((q_raw, inv_q), (k_raw, inv_k))):
        spread_dot = column_of(dots[t : t + 1, :])
        for h in range(heads):
            lanes = slice(h * HD, (h + 1) * HD)
            gained = dqkv[t, :, :, :, lanes].reshape(both, HD).astype(F32)
            r = inv[...]
            grad = r * gained - raw[:, lanes] * (r * r * r) * spread_dot
            dqkv[t, :, :, :, lanes] = grad.astype(BF16).reshape(2, seqs, blk, HD)

    def rf_copy(i, off):
        return remote(st_z.at[:, ds(off, cw)], rx_f.at[i], rzs.at[3, i, 0], rzr.at[3, i, 0], ctx, zp(i + 1))

    def in_partial(core, off):
        here = ds(off, cw)
        acc = None
        for t in range(3):
            left = dqkv[t, pl.ds(core, 1)].reshape(rows, head_w)
            term = lax.dot_general(left, w[t][here, :], NT, preferred_element_type=F32)
            acc = term if acc is None else acc + term
        return acc

    own_rows = ds(z * share_rows, share_rows)
    for i in range(tps):
        off = zp(i + 1) * cw
        st_p[:, ds(off, cw)] = in_partial(ok, off).astype(BF16)
        rp_copy(3, i, off).start()
        mine = in_partial(k, off)
        rp_copy(3, i, off).wait_recv()
        st_z[:, ds(off, cw)] = (mine + rx_p[1, :, ds(off, cw)].astype(F32)).astype(BF16)
        st_z[own_rows, ds(off, cw)] = (st_z[own_rows, ds(off, cw)].astype(F32) + dhid[:, ds(off, cw)]).astype(BF16)
        if i < tps - 1:
            rf_copy(i, off).start()

    pass_g(5)
    pass_g(3)
    for m in range(3):

        def gqkv_step(j, carry):
            here = ds(j * 512, 512)
            right = dqkv[m].reshape(both, head_w)
            w[m][here, :] = jnp.dot(tok_t[here, :], right, preferred_element_type=F32).astype(BF16)
            return carry

        free_w(m)
        lax.fori_loop(0, width // 512, gqkv_step, 0)
        send_g(m)
    middle = gg_row[:, ds(z * feats, feats)]
    for i, copy in enumerate(gains_z):
        copy.wait_recv()
        middle = middle + gg_rx1[i]
    gg_mid[...] = gg_mid[...] + middle
    gains_c = []
    n = 0
    for i, d in slots:
        if i or d:
            core = (k + d) % 2
            gains_c.append(go(remote(gg_mid.at[:, ds(chip(i) * 128, 128)], gg_rx2.at[n], ms.at[5, n], mr.at[5, n], chip(i) * 2 + core, z)))
            n += 1

    for m in range(3):
        pass_g(m)
    for i in range(tps - 1):
        rf_copy(i, zp(i + 1) * cw).wait_recv()
    final = st_z[:, ds(z * feats, cw)].astype(F32)
    for i in range(tps - 1):
        final = final + rx_f[i].astype(F32)
    gin_ref[...] = final
    for i in range(tps):
        rp_copy(3, i, zp(i + 1) * cw).wait_send()
        if i < tps - 1:
            rf_copy(i, zp(i + 1) * cw).wait_send()
    gain_sum = gg_mid[:, ds(c * 128, 128)]
    for i, copy in enumerate(gains_c):
        copy.wait_recv()
        gain_sum = gain_sum + gg_rx2[i]
    ggain_ref[...] = gain_sum
    own_out.wait()
    for copy in out_z:
        copy.wait_recv()
    for copy in g_own:
        copy.wait()
    for m in g_live:
        wait_g(m)
    for copy in pending:
        copy.wait_send()


def fused(
    tokens,
    w_query,
    w_key,
    w_value,
    w_output,
    w_gate,
    w_up,
    w_down,
    gain_query,
    gain_key,
    gain_attention,
    gain_feedforward,
    block_order,
    cotangent,
):
    seqs, blk, feats = tokens.shape
    tps = lax.axis_size("tp")
    chips = lax.axis_size("ctx") // 2
    width = feats * tps
    rows = seqs * blk
    both = 2 * rows
    share_rows = rows // tps
    total = 2 * chips * blk
    head_w = w_query.shape[1] // 2
    ff_w = w_gate.shape[1] // 2
    heads = head_w // HD
    slab = width // (2 * chips)
    ctx = lax.axis_index("ctx")
    frequency = THETA ** (-2.0 * np.arange(HD // 2) / HD)
    frequency = np.concatenate([frequency, frequency])
    starts = np.zeros((blk, 1))
    starts[: 2 * chips, 0] = np.arange(2 * chips) * blk
    inside = np.arange(blk)[:, None] * 1.0
    table = np.stack([f(at * frequency) for at in (starts, inside) for f in (np.cos, np.sin)]).astype(np.float32)
    gains = jnp.stack([gain_query, gain_key, gain_attention, gain_feedforward]).astype(F32)
    gains = jnp.pad(gains, ((0, 4), (0, 0)))
    blank = jnp.zeros_like(gains)
    gtile = jnp.where(ctx % 2 == 0, jnp.concatenate([gains, blank], axis=1), jnp.concatenate([blank, gains], axis=1))
    weights = (w_query, w_key, w_value, w_output, w_gate, w_up, w_down)
    dims = (chips, tps, seqs, blk, width, head_w, ff_w)
    halves = (head_w, head_w, head_w, head_w, ff_w, ff_w, ff_w)
    hbm = pl.BlockSpec(memory_space=pl.ANY)
    vmem = pl.BlockSpec(memory_space=pltpu.VMEM)

    def v(shape, dtype=BF16):
        return pltpu.VMEM(shape, dtype)

    w_shapes = [v((width, h)) if m in COLS else v((h, width)) for m, h in enumerate(halves)]
    dma = pltpu.SemaphoreType.DMA
    v_shapes = [v((2, slab, h)) if m in COLS else v((2, h, slab)) for m, h in enumerate(halves)]
    scratch = w_shapes + v_shapes + [
        v((both, width)),
        v((width, both)),
        v((both, width)),
        v((width, both)),
        v((both, width)),
        v((both, width)),
        v((both, ff_w), F32),
        v((both, ff_w), F32),
        v((both, ff_w)),
        v((ff_w, both)),
        v((both, ff_w)),
        v((both, ff_w)),
        v((rows, width)),
        v((2, rows, width)),
        v((rows, width)),
        v((2, tps - 1, share_rows, width)),
        v((tps - 1, rows, feats)),
        v((both, head_w), F32),
        v((both, head_w), F32),
        v((3, 2, seqs, blk, head_w)),
        v((3, 2 * chips, blk, HD)),
        v((total, total)),
        v((total, HD), F32),
        v((2 * chips, blk, HD)),
        v((2, seqs, blk, head_w)),
        v((head_w, both)),
        v((2, seqs, blk, head_w)),
        v((2 * chips, blk, HD)),
        v((3, 2 * chips, blk, HD)),
        v((3, 2, seqs, blk, head_w)),
        v((2, 8, both), F32),
        v((2, 2 * tps - 1, 8, both), F32),
        v((both, 128), F32),
        v((both, 128), F32),
        v((share_rows, width)),
        v((share_rows, width), F32),
        v((share_rows, width), F32),
        v((share_rows, width), F32),
        v((share_rows, width), F32),
        v((2 * chips, 8, 128), F32),
        v((tps, 2 * chips, 8, 128), F32),
        v((8, width), F32),
        v((8, head_w), F32),
        v((8, width), F32),
        v((tps - 1, 8, feats), F32),
        v((8, feats), F32),
        v((2 * chips - 1, 8, 128), F32),
        dma((7, 2 * chips)),
        dma((7, 2 * chips)),
        dma((7, 2 * chips)),
        dma((7, 2 * chips)),
        dma((4, tps - 1)),
        dma((4, tps - 1)),
        dma((4, tps)),
        dma((4, tps)),
        dma((4, tps)),
        dma((4, tps)),
        dma((4, tps, tps - 1)),
        dma((4, tps, tps - 1)),
        dma((6, 2 * chips)),
        dma((6, 2 * chips)),
        dma((2, 2 * tps - 1)),
        dma((2, 2 * tps - 1)),
        dma((4, chips - 1)),
        dma((4, chips - 1)),
        dma((25,)),
        v((2 * both, ff_w // 2), F32),
        v((both, HD), F32),
        v((both, HD), F32),
        v((8, total), jnp.int32),
        dma((chips, 2 * tps - 1)),
        dma((chips, 2 * tps - 1)),
    ]
    results = pl.pallas_call(
        functools.partial(layer_kernel, dims),
        out_shape=[
            jax.ShapeDtypeStruct((rows, feats), F32),
            jax.ShapeDtypeStruct((rows, feats), F32),
            jax.ShapeDtypeStruct((8, 128), F32),
        ]
        + [jax.ShapeDtypeStruct((3,) + weight.shape, BF16) for weight in weights],
        in_specs=[hbm] * 9 + [pl.BlockSpec(memory_space=pltpu.SMEM), vmem, vmem],
        out_specs=[hbm, vmem, vmem] + [hbm] * 7,
        scratch_shapes=scratch,
        compiler_params=pltpu.CompilerParams(
            collective_id=0, has_side_effects=True, vmem_limit_bytes=67043328
        ),
        name="layer",
    )(tokens.reshape(rows, feats), cotangent.reshape(rows, feats), *weights, block_order, gtile, table)
    output = results[0].reshape(tokens.shape)
    grad_input = results[1].reshape(tokens.shape)
    grads = [jnp.sum(received.astype(F32), axis=0) for received in results[3:]]
    lanes = lax.dynamic_slice_in_dim(results[2], (ctx % 2) * 64, 64, 1)
    return (output, grad_input, *grads, lanes[2], lanes[3], lanes[0], lanes[1])


def fits(mesh):
    return mesh.shape["ctx"] == 8 and mesh.shape["tp"] == 4


def solution(mesh):
    placed = (
        P(None, "ctx", "tp"),
        P("ctx", "tp"),
        P("ctx", "tp"),
        P("ctx", "tp"),
        P("tp", "ctx"),
        P("ctx", "tp"),
        P("ctx", "tp"),
        P("tp", "ctx"),
        P(("tp", "ctx")),
        P(("tp", "ctx")),
        P(("tp", "ctx")),
        P(("tp", "ctx")),
        P(),
        P(None, "ctx", "tp"),
    )
    return jax.shard_map(
        fused if fits(mesh) else shards,
        mesh=mesh,
        in_specs=placed,
        out_specs=(
            P(None, "ctx", "tp"),
            P(None, "ctx", "tp"),
            P("ctx", "tp"),
            P("ctx", "tp"),
            P("ctx", "tp"),
            P("tp", "ctx"),
            P("ctx", "tp"),
            P("ctx", "tp"),
            P("tp", "ctx"),
            P(("tp", "ctx")),
            P(("tp", "ctx")),
            P(("tp", "ctx")),
            P(("tp", "ctx")),
        ),
        check_vma=False,
    )
```

```python
import functools

import jax
import jax.numpy as jnp
import numpy as np
from jax import lax
from jax.experimental import pallas as pl
from jax.experimental.pallas import tpu as pltpu
from jax.sharding import PartitionSpec as P

HD = 128


EPS = 1e-06
THETA = 500000.0
NEGATIVE = -1e30


def full_width(value):
    return lax.all_gather(value, "tp", axis=2, tiled=True)


def share(value):
    return lax.psum_scatter(value, "tp", scatter_dimension=2, tiled=True)


def tp_total(values):
    return lax.psum(values, "tp")


def rotary_tables(positions):
    half_dim = HD // 2
    frequency = THETA ** (-2.0 * jnp.arange(half_dim, dtype=jnp.float32) / HD)
    angles = positions.astype(jnp.float32)[..., None] * frequency
    return (jnp.cos(angles)[..., None, :], jnp.sin(angles)[..., None, :])


def rotate(value, cosine, sine):
    half_dim = value.shape[-1] // 2
    first, second = (value[..., :half_dim], value[..., half_dim:])
    return jnp.concatenate(
        [first * cosine - second * sine, second * cosine + first * sine], axis=-1
    )


def unrotate(grad, cosine, sine):
    half_dim = grad.shape[-1] // 2
    first, second = (grad[..., :half_dim], grad[..., half_dim:])
    return jnp.concatenate(
        [first * cosine + second * sine, second * cosine - first * sine], axis=-1
    )


def key_positions(block_order, start, count, block_len):
    slots = start + jnp.arange(count, dtype=jnp.int32)
    owner = slots // block_len
    ranks = jnp.arange(block_order.shape[1], dtype=jnp.int32)
    chosen = jnp.sum(
        jnp.where(owner[None, :, None] == ranks[None, None, :], block_order[:, None, :], 0), axis=2
    )
    return chosen * block_len + slots % block_len


def span_of():
    return 512


def shards(
    tokens,
    w_query,
    w_key,
    w_value,
    w_output,
    w_gate,
    w_up,
    w_down,
    gain_query,
    gain_key,
    gain_attention,
    gain_feedforward,
    block_order,
    cotangent,
):
    gathered = (
        lax.all_gather(w_query, "ctx", axis=0, tiled=True),
        lax.all_gather(w_key, "ctx", axis=0, tiled=True),
        lax.all_gather(w_value, "ctx", axis=0, tiled=True),
        lax.all_gather(w_output, "ctx", axis=1, tiled=True),
        lax.all_gather(w_gate, "ctx", axis=0, tiled=True),
        lax.all_gather(w_up, "ctx", axis=0, tiled=True),
        lax.all_gather(w_down, "ctx", axis=1, tiled=True),
        lax.all_gather(gain_query, "ctx", axis=0, tiled=True),
        lax.all_gather(gain_key, "ctx", axis=0, tiled=True),
        lax.all_gather(gain_attention, "ctx", axis=0, tiled=True),
        lax.all_gather(gain_feedforward, "ctx", axis=0, tiled=True),
    )
    wq_full, wk_full, wv_full, wo_full, wg_full, wu_full, wd_full = gathered[:7]
    g_query = gathered[7].astype(jnp.float32)
    g_key = gathered[8].astype(jnp.float32)
    g_attn = gathered[9].astype(jnp.float32)
    g_feed = gathered[10].astype(jnp.float32)
    seq_count, block_len, local_width = tokens.shape
    row_count = seq_count * block_len
    scale = HD ** (-0.5)
    tok_full = full_width(tokens)
    tok_rows = tok_full.reshape(row_count, -1)
    width = tok_rows.shape[1]
    queries = jnp.dot(tok_rows, wq_full, preferred_element_type=jnp.float32)
    keys_raw = jnp.dot(tok_rows, wk_full, preferred_element_type=jnp.float32)
    values_raw = jnp.dot(tok_rows, wv_full, preferred_element_type=jnp.float32)
    head_width = queries.shape[1]
    head_count = head_width // HD
    q_squares, k_squares = tp_total(
        (jnp.sum(queries * queries, axis=1), jnp.sum(keys_raw * keys_raw, axis=1))
    )
    q_inverse = lax.rsqrt(q_squares / width + EPS)[:, None]
    k_inverse = lax.rsqrt(k_squares / width + EPS)[:, None]
    q_normed = queries * q_inverse * g_query
    k_normed = keys_raw * k_inverse * g_key
    ctx_rank = lax.axis_index("ctx")
    ranks = jnp.arange(block_order.shape[1], dtype=jnp.int32)
    my_block = jnp.sum(jnp.where(ranks[None, :] == ctx_rank, block_order, 0), axis=1)
    q_pos = my_block[:, None] * block_len + jnp.arange(block_len, dtype=jnp.int32)[None, :]
    cosine, sine = rotary_tables(q_pos)
    q_rot = rotate(q_normed.reshape(seq_count, block_len, head_count, HD), cosine, sine).astype(
        jnp.bfloat16
    )
    k_rot = rotate(k_normed.reshape(seq_count, block_len, head_count, HD), cosine, sine).astype(
        jnp.bfloat16
    )
    k_flat = k_rot.reshape(seq_count, block_len, head_width)
    v_flat = values_raw.astype(jnp.bfloat16).reshape(seq_count, block_len, head_width)

    def stat_block(state, key_piece, k_pos):
        run_max, run_sum = state
        scores = (
            jnp.einsum("sqhd,skhd->shqk", q_rot, key_piece, preferred_element_type=jnp.float32)
            * scale
        )
        visible = k_pos[:, None, None, :] <= q_pos[:, None, :, None]
        scores = jnp.where(visible, scores, NEGATIVE)
        new_max = jnp.maximum(run_max, jnp.max(scores, axis=-1))
        weights = jnp.where(visible, jnp.exp(scores - new_max[..., None]), 0.0)
        run_sum = run_sum * jnp.exp(run_max - new_max) + jnp.sum(weights, axis=-1)
        return (new_max, run_sum)

    init = (
        jnp.full((seq_count, head_count, block_len), NEGATIVE, jnp.float32),
        jnp.zeros((seq_count, head_count, block_len), jnp.float32),
    )
    fold_key_all = lax.all_gather(k_flat, "ctx", axis=1, tiled=True)
    count = fold_key_all.shape[1]
    span = span_of()

    def fold_one_span(step_index, inner):
        offset = step_index * span
        key_piece = lax.dynamic_slice_in_dim(fold_key_all, offset, span, 1).reshape(
            seq_count, span, head_count, HD
        )
        k_pos = key_positions(block_order, offset, span, block_len)
        return stat_block(inner, key_piece, k_pos)

    run_max, run_sum = lax.fori_loop(0, count // span, fold_one_span, init)
    key_all, val_all = (
        lax.all_gather(k_flat, "ctx", axis=1, tiled=True),
        lax.all_gather(v_flat, "ctx", axis=1, tiled=True),
    )
    log_total = run_max + jnp.log(run_sum)
    total_len = key_all.shape[1]
    total_span = span_of()

    def value_span(step_index, acc):
        offset = step_index * total_span
        key_piece = lax.dynamic_slice_in_dim(key_all, offset, total_span, 1).reshape(
            seq_count, total_span, head_count, HD
        )
        val_piece = lax.dynamic_slice_in_dim(val_all, offset, total_span, 1).reshape(
            seq_count, total_span, head_count, HD
        )
        k_pos = key_positions(block_order, offset, total_span, block_len)
        scores = (
            jnp.einsum("sqhd,skhd->shqk", q_rot, key_piece, preferred_element_type=jnp.float32)
            * scale
        )
        visible = k_pos[:, None, None, :] <= q_pos[:, None, :, None]
        weights = jnp.where(visible, jnp.exp(scores - log_total[..., None]), 0.0).astype(
            jnp.bfloat16
        )
        return acc + jnp.einsum(
            "shqk,skhd->sqhd", weights, val_piece, preferred_element_type=jnp.float32
        )

    attended = lax.fori_loop(
        0,
        total_len // total_span,
        value_span,
        jnp.zeros((seq_count, block_len, head_count, HD), jnp.float32),
    )
    attn_bf = attended.reshape(row_count, head_width).astype(jnp.bfloat16)
    attn_proj = share(
        jnp.dot(attn_bf, wo_full, preferred_element_type=jnp.float32).reshape(
            seq_count, block_len, -1
        )
    )
    (a_squares,) = tp_total((jnp.sum(attn_proj * attn_proj, axis=2),))
    a_inverse = lax.rsqrt(a_squares / width + EPS)[..., None]
    hidden_state = tokens.astype(jnp.float32) + attn_proj * a_inverse * g_attn
    hidden_rows = full_width(hidden_state.astype(jnp.bfloat16)).reshape(row_count, -1)
    gate = jnp.dot(hidden_rows, wg_full, preferred_element_type=jnp.float32)
    up_vals = jnp.dot(hidden_rows, wu_full, preferred_element_type=jnp.float32)
    sigma = jax.nn.sigmoid(gate)
    activation = (gate * sigma * up_vals).astype(jnp.bfloat16)
    mixed = share(
        jnp.dot(activation, wd_full, preferred_element_type=jnp.float32).reshape(
            seq_count, block_len, -1
        )
    )
    (m_squares,) = tp_total((jnp.sum(mixed * mixed, axis=2),))
    m_inverse = lax.rsqrt(m_squares / width + EPS)[..., None]
    output = hidden_state + mixed * m_inverse * g_feed
    upstream = cotangent.astype(jnp.float32)
    (m_dots,) = tp_total((jnp.sum(g_feed * upstream * mixed, axis=2),))
    d_mixed = m_inverse * (g_feed * upstream) - mixed * m_inverse**3 * (m_dots / width)[..., None]
    d_gfeed = jnp.sum(upstream * mixed * m_inverse, axis=(0, 1))
    d_mixed_rows = full_width(d_mixed.astype(jnp.bfloat16)).reshape(row_count, -1)
    grad_down = jnp.dot(activation.T, d_mixed_rows, preferred_element_type=jnp.float32)
    d_act = jnp.dot(d_mixed_rows, wd_full.T, preferred_element_type=jnp.float32)
    d_up_bf = (d_act * gate * sigma).astype(jnp.bfloat16)
    d_gate_bf = (d_act * up_vals * sigma * (1.0 + gate * (1.0 - sigma))).astype(jnp.bfloat16)
    grad_gate = jnp.dot(hidden_rows.T, d_gate_bf, preferred_element_type=jnp.float32)
    grad_up = jnp.dot(hidden_rows.T, d_up_bf, preferred_element_type=jnp.float32)
    back_ff = jnp.dot(d_gate_bf, wg_full.T, preferred_element_type=jnp.float32) + jnp.dot(
        d_up_bf, wu_full.T, preferred_element_type=jnp.float32
    )
    d_hidden = upstream + share(back_ff.reshape(seq_count, block_len, -1))
    (a_dots,) = tp_total((jnp.sum(g_attn * d_hidden * attn_proj, axis=2),))
    d_attn = (
        a_inverse * (g_attn * d_hidden) - attn_proj * a_inverse**3 * (a_dots / width)[..., None]
    )
    d_gattn = jnp.sum(d_hidden * attn_proj * a_inverse, axis=(0, 1))
    d_attn_rows = full_width(d_attn.astype(jnp.bfloat16)).reshape(row_count, -1)
    grad_outproj = jnp.dot(attn_bf.T, d_attn_rows, preferred_element_type=jnp.float32)
    d_heads = jnp.dot(d_attn_rows, wo_full.T, preferred_element_type=jnp.float32).reshape(
        seq_count, block_len, head_count, HD
    )
    deltas = jnp.sum(d_heads * attended, axis=3).transpose(0, 2, 1)
    d_heads_bf = d_heads.astype(jnp.bfloat16)

    def grad_block(key_piece, val_piece, k_pos):
        scores = (
            jnp.einsum("sqhd,skhd->shqk", q_rot, key_piece, preferred_element_type=jnp.float32)
            * scale
        )
        visible = k_pos[:, None, None, :] <= q_pos[:, None, :, None]
        probs = jnp.where(visible, jnp.exp(scores - log_total[..., None]), 0.0)
        d_probs = jnp.einsum(
            "sqhd,skhd->shqk", d_heads_bf, val_piece, preferred_element_type=jnp.float32
        )
        d_scores = (probs * (d_probs - deltas[..., None])).astype(jnp.bfloat16)
        return (probs, d_scores)

    def query_span(step_index, acc):
        offset = step_index * total_span
        key_piece = lax.dynamic_slice_in_dim(key_all, offset, total_span, 1).reshape(
            seq_count, total_span, head_count, HD
        )
        val_piece = lax.dynamic_slice_in_dim(val_all, offset, total_span, 1).reshape(
            seq_count, total_span, head_count, HD
        )
        k_pos = key_positions(block_order, offset, total_span, block_len)
        probs, d_scores = grad_block(key_piece, val_piece, k_pos)
        return (
            acc
            + jnp.einsum("shqk,skhd->sqhd", d_scores, key_piece, preferred_element_type=jnp.float32)
            * scale
        )

    d_qrot = lax.fori_loop(
        0,
        total_len // total_span,
        query_span,
        jnp.zeros((seq_count, block_len, head_count, HD), jnp.float32),
    )
    count = block_len * lax.axis_size("ctx")
    key_span = span_of()

    def key_one_span(step_index, buffer):
        offset = step_index * key_span
        key_piece = lax.dynamic_slice_in_dim(key_all, offset, key_span, 1).reshape(
            seq_count, key_span, head_count, HD
        )
        val_piece = lax.dynamic_slice_in_dim(val_all, offset, key_span, 1).reshape(
            seq_count, key_span, head_count, HD
        )
        k_pos = key_positions(block_order, offset, key_span, block_len)
        probs, d_scores = grad_block(key_piece, val_piece, k_pos)
        d_keyp = (
            jnp.einsum("shqk,sqhd->skhd", d_scores, q_rot, preferred_element_type=jnp.float32)
            * scale
        )
        d_valp = jnp.einsum(
            "shqk,sqhd->skhd",
            probs.astype(jnp.bfloat16),
            d_heads_bf,
            preferred_element_type=jnp.float32,
        )
        both = jnp.concatenate(
            [
                d_keyp.reshape(seq_count, key_span, head_width),
                d_valp.reshape(seq_count, key_span, head_width),
            ],
            axis=2,
        )
        return lax.dynamic_update_slice_in_dim(buffer, both.transpose(1, 0, 2), offset, 0)

    key_sums = (
        lax.psum_scatter(
            lax.fori_loop(
                0,
                count // key_span,
                key_one_span,
                jnp.zeros((count, seq_count, 2 * head_width), jnp.float32),
            ).astype(jnp.bfloat16),
            "ctx",
            scatter_dimension=0,
            tiled=True,
        )
        .astype(jnp.float32)
        .transpose(1, 0, 2)
    )
    d_krot = key_sums[..., :head_width].reshape(seq_count, block_len, head_count, HD)
    d_values = key_sums[..., head_width:].reshape(row_count, head_width)
    dq_normed = unrotate(d_qrot, cosine, sine).reshape(row_count, head_width)
    dk_normed = unrotate(d_krot, cosine, sine).reshape(row_count, head_width)
    q_dots, k_dots = tp_total(
        (
            jnp.sum(g_query * dq_normed * queries, axis=1),
            jnp.sum(g_key * dk_normed * keys_raw, axis=1),
        )
    )
    d_queries = (
        q_inverse * (g_query * dq_normed) - queries * q_inverse**3 * (q_dots / width)[:, None]
    )
    d_keys = k_inverse * (g_key * dk_normed) - keys_raw * k_inverse**3 * (k_dots / width)[:, None]
    d_gquery = jnp.sum(dq_normed * queries * q_inverse, axis=0)
    d_gkey = jnp.sum(dk_normed * keys_raw * k_inverse, axis=0)
    dq_bf = d_queries.astype(jnp.bfloat16)
    dk_bf = d_keys.astype(jnp.bfloat16)
    dv_bf = d_values.astype(jnp.bfloat16)
    grad_q = jnp.dot(tok_rows.T, dq_bf, preferred_element_type=jnp.float32)
    grad_k = jnp.dot(tok_rows.T, dk_bf, preferred_element_type=jnp.float32)
    grad_v = jnp.dot(tok_rows.T, dv_bf, preferred_element_type=jnp.float32)
    back_attn = (
        jnp.dot(dq_bf, wq_full.T, preferred_element_type=jnp.float32)
        + jnp.dot(dk_bf, wk_full.T, preferred_element_type=jnp.float32)
        + jnp.dot(dv_bf, wv_full.T, preferred_element_type=jnp.float32)
    )
    grad_input = d_hidden + share(back_attn.reshape(seq_count, block_len, -1))
    summed = (
        lax.psum_scatter(
            grad_q.astype(jnp.bfloat16), "ctx", scatter_dimension=0, tiled=True
        ).astype(jnp.float32),
        lax.psum_scatter(
            grad_k.astype(jnp.bfloat16), "ctx", scatter_dimension=0, tiled=True
        ).astype(jnp.float32),
        lax.psum_scatter(
            grad_v.astype(jnp.bfloat16), "ctx", scatter_dimension=0, tiled=True
        ).astype(jnp.float32),
        lax.psum_scatter(
            grad_outproj.astype(jnp.bfloat16), "ctx", scatter_dimension=1, tiled=True
        ).astype(jnp.float32),
        lax.psum_scatter(
            grad_gate.astype(jnp.bfloat16), "ctx", scatter_dimension=0, tiled=True
        ).astype(jnp.float32),
        lax.psum_scatter(
            grad_up.astype(jnp.bfloat16), "ctx", scatter_dimension=0, tiled=True
        ).astype(jnp.float32),
        lax.psum_scatter(
            grad_down.astype(jnp.bfloat16), "ctx", scatter_dimension=1, tiled=True
        ).astype(jnp.float32),
        lax.psum_scatter(
            d_gquery.astype(jnp.bfloat16), "ctx", scatter_dimension=0, tiled=True
        ).astype(jnp.float32),
        lax.psum_scatter(
            d_gkey.astype(jnp.bfloat16), "ctx", scatter_dimension=0, tiled=True
        ).astype(jnp.float32),
        lax.psum_scatter(
            d_gattn.astype(jnp.bfloat16), "ctx", scatter_dimension=0, tiled=True
        ).astype(jnp.float32),
        lax.psum_scatter(
            d_gfeed.astype(jnp.bfloat16), "ctx", scatter_dimension=0, tiled=True
        ).astype(jnp.float32),
    )
    return (
        output,
        grad_input,
        summed[0],
        summed[1],
        summed[2],
        summed[3],
        summed[4],
        summed[5],
        summed[6],
        summed[7],
        summed[8],
        summed[9],
        summed[10],
    )


MESH = pl.DeviceIdType.MESH
NT = (((1,), (1,)), ((), ()))
TN = (((0,), (0,)), ((), ()))
F32 = jnp.float32
BF16 = jnp.bfloat16
COLS = (0, 1, 2, 4, 5)


def layer_kernel(dims, *refs):
    (chips, tps, seqs, blk, width, head_w, ff_w) = dims
    rows = seqs * blk
    both = 2 * rows
    share_rows = rows // tps
    feats = width // tps
    heads = head_w // HD
    slab = width // (2 * chips)
    halves = (head_w, head_w, head_w, head_w, ff_w, ff_w, ff_w)
    total = 2 * chips * blk
    scale = HD ** (-0.5)
    it = iter(refs)

    def take(n):
        return [next(it) for _ in range(n)]

    (tok_in, cot_in) = take(2)
    w_in = take(7)
    (blocks, gtile, table) = take(3)
    (out_ref, gin_ref, ggain_ref) = take(3)
    rx_g = take(7)
    summed = take(4)
    w = take(7)
    via = take(7)
    (tok, tok_t, hid, hid_t, dmix, dattn) = take(6)
    (lin, fac, act, act_t, dgate, dup) = take(6)
    (st_p, rx_p, st_z, rx_z, rx_f) = take(5)
    (q_raw, k_raw, qkv, qa, probs, att_f, att_st, att, att_t) = take(9)
    (dh, d_o, dqkv_st, dqkv) = take(4)
    (sq_own, sq_rx, inv_q, inv_k) = take(4)
    (cot, proj, hstate, dhid, stage) = take(5)
    (gbuf, gall, gfull, gqk, gg_row, gg_rx1, gg_mid, gg_rx2) = take(8)
    (ws, wr, gs, gr) = take(4)
    (zs, zr, ps, pr) = take(4)
    (rps, rpr, rzs, rzr) = take(4)
    (ms, mr) = take(2)
    (ss, sr) = take(2)
    (as_, ar) = take(2)
    (loc,) = take(1)
    (d_acc, cosf, sinf, pos_row) = take(4)
    (xs, xr) = take(2)

    ctx = lax.axis_index("ctx")
    z = lax.axis_index("tp")
    c = ctx // 2
    k = ctx % 2
    ok = 1 - k
    partner = c * 2 + ok
    near = (c + 1 - 2 * (c % 2), (c + 2) % chips)
    far = chips - 1 - c

    def zp(i):
        return (z + i) % tps

    def chip(i):
        return (c + i) % chips

    def ds(start, size):
        return pl.ds(pl.multiple_of(start, size), size)

    def remote(src, dst, ssem, rsem, to_ctx, to_z):
        return pltpu.make_async_remote_copy(
            src_ref=src,
            dst_ref=dst,
            send_sem=ssem,
            recv_sem=rsem,
            device_id=(to_ctx, to_z),
            device_id_type=MESH,
        )

    peers = [(chip(i) * 2 + (k + d) % 2, z) for i in range(chips) for d in range(2) if i or d]
    peers += [(ctx, zp(i)) for i in range(1, tps)]
    peers += [(partner, zp(i)) for i in range(1, tps)]
    barrier = pltpu.get_barrier_semaphore()
    for peer in peers:
        pl.semaphore_signal(barrier, inc=1, device_id=peer, device_id_type=MESH)

    def go(copy):
        copy.start()
        return copy

    def sent(ref, sem):
        remote(ref, ref, sem, sem, partner, z).wait_send()

    def came(ref, sem):
        remote(ref, ref, sem, sem, partner, z).wait_recv()

    def slab_of(m, owner):
        if m in COLS:
            return w[m].at[ds(owner * slab, slab), :]
        return w[m].at[:, ds(owner * slab, slab)]

    def slabs(m, count):
        return w[m].at[0 : count * slab, :] if m in COLS else w[m].at[:, 0 : count * slab]

    def half_of(m, core):
        if m in COLS:
            return w_in[m].at[:, ds(core * halves[m], halves[m])]
        return w_in[m].at[ds(core * halves[m], halves[m]), :]

    w_own = {}
    w_wait = {}

    def send_w(m, d):
        core = (k + d) % 2
        for n in range(2):
            go(remote(half_of(m, core), slab_of(m, ctx), ws.at[m, 0], wr.at[m, 2 * n + k], near[n] * 2 + core, z))
        if d:
            go(remote(half_of(m, ok), slab_of(m, ctx), ws.at[m, 0], wr.at[m, 4], partner, z))
        else:
            w_own[m] = pltpu.make_async_copy(half_of(m, k), slab_of(m, ctx), loc.at[m])
            w_own[m].start()

    def source(n):
        if n < 4:
            return near[n // 2] * 2 + n % 2
        return partner if n == 4 else far * 2 + n - 5

    def got_w(m, *which):
        for n in which:
            if (m, n) not in w_wait:
                w_wait[m, n] = True
                came(slabs(m, 1), wr.at[m, n])

    def pass_w(m):
        for n in range(2):
            got_w(m, 3 * n)
            mine = slab_of(m, source(3 * n))
            go(remote(mine, mine, ws.at[m, 1], wr.at[m, 5 + n], near[1 - n] * 2 + k, z))

    def free_w(m):
        sent(slabs(m, 2), ws.at[m, 1])

    def wait_w(m):
        w_own[m].wait()
        got_w(m, *range(7))

    def into(m, n, core):
        if m in COLS:
            return rx_g[m].at[n, :, ds(core * halves[m], halves[m])]
        return rx_g[m].at[n, ds(core * halves[m], halves[m]), :]

    g_own = {}

    def send_far(m):
        for n in range(2):
            go(remote(slab_of(m, far * 2 + n), via[m].at[n], gs.at[m], gr.at[m, n], near[n] * 2 + k, z))

    def send_near(m, n):
        go(remote(slab_of(m, near[n] * 2 + n), into(m, 1 + n, k), gs.at[m], gr.at[m, 2], near[n] * 2 + n, z))

    def send_home(m):
        go(remote(slab_of(m, partner), into(m, 0, k), gs.at[m], gr.at[m, 2], partner, z))
        copy = pltpu.make_async_copy(slab_of(m, ctx), into(m, 0, k), loc.at[8 + m])
        copy.start()
        g_own[m] = copy

    def send_g(m):
        send_far(m)
        send_near(m, 0)
        send_near(m, 1)
        send_home(m)

    def pass_g(m):
        for n in range(2):
            to = near[1 - n] * 2 + n
            came(via[m].at[n], gr.at[m, n])
            total = slab_of(m, to)[...].astype(F32) + via[m][n].astype(F32)
            slab_of(m, to)[...] = total.astype(BF16)
            go(remote(slab_of(m, to), into(m, 2 - n, k), gs.at[m], gr.at[m, 2], to, z))

    def wait_g(m):
        g_own[m].wait()
        came(slabs(m, 5), gr.at[m, 2])

    def add_up(m):
        wait_g(m)
        if m in COLS:
            n = slab
            parts = (hid.at[0:n, :], hid.at[n : 2 * n, :], dmix.at[0:n, :], dmix.at[n : 2 * n, :])
        else:
            n = 2 * halves[m]
            parts = (hid_t.at[0:n, 0:slab], hid_t.at[0:n, slab : 2 * slab], tok_t.at[0:n, 0:slab], tok_t.at[0:n, slab : 2 * slab])
        loads = [pltpu.make_async_copy(rx_g[m].at[i], parts[i], loc.at[i]) for i in range(3)]
        for copy in loads:
            copy.start()
        for copy in loads:
            copy.wait()

        def add_step(j, carry):
            here = (slice(None), ds(j * 256, 256)) if m in COLS else (ds(j * 256, 256), slice(None))
            value = parts[0][here].astype(F32) + parts[1][here].astype(F32) + parts[2][here].astype(F32)
            parts[3][here] = value.astype(BF16)
            return carry

        lax.fori_loop(0, 2 * halves[m] // 256, add_step, 0)
        copy = pltpu.make_async_copy(parts[3], summed[m - 3], loc.at[3])
        copy.start()
        copy.wait()

    own_tok = pltpu.make_async_copy(tok_in, tok.at[ds(k * rows, rows), ds(z * feats, feats)], loc.at[16])
    own_tok.start()
    own_cot = pltpu.make_async_copy(cot_in.at[ds(z * share_rows, share_rows), :], cot.at[:, ds(z * feats, feats)], loc.at[17])
    own_cot.start()
    own_gain = pltpu.make_async_copy(gtile, gbuf.at[ctx], loc.at[18])
    own_gain.start()
    pl.semaphore_wait(barrier, len(peers))

    for i in range(1, tps):
        go(remote(tok_in, tok.at[ds(k * rows, rows), ds(z * feats, feats)], zs.at[0], zr.at[0, i - 1], ctx, zp(i)))
    go(remote(tok_in, tok.at[ds(k * rows, rows), ds(z * feats, feats)], ps.at[0], pr.at[0], partner, z))
    slots = [(i, d) for i in range(chips) for d in range(2)]
    for i, d in slots:
        if i or d:
            go(remote(gtile, gbuf.at[ctx], ms.at[0], mr.at[0], chip(i) * 2 + (k + d) % 2, z))
    for i in range(1, tps):
        go(remote(cot_in.at[ds(zp(i) * share_rows, share_rows), :], cot.at[:, ds(z * feats, feats)], ms.at[1], mr.at[1], ctx, zp(i)))
    for m in (0, 1, 2, 3):
        send_w(m, 0)
        send_w(m, 1)

    own_gain.wait()
    came(gbuf.at[0 : 2 * chips - 1], mr.at[0])
    own_gain2 = pltpu.make_async_copy(gbuf, gall.at[z], loc.at[19])
    own_gain2.start()
    for i in range(1, tps):
        go(remote(gbuf, gall.at[z], ms.at[2], mr.at[2], ctx, zp(i)))
    for r in range(2):
        pieces = [gbuf[4 * k + 2 * m, r : r + 1, :] + gbuf[4 * k + 2 * m + 1, r : r + 1, :] for m in range(head_w // 128)]
        gqk[r : r + 1, :] = jnp.concatenate(pieces, axis=1)

    lane = lax.broadcasted_iota(jnp.int32, (blk, HD), 1)
    sign = jnp.where(lane < HD // 2, -1.0, 1.0)
    for core in range(2):
        for s in range(seqs):
            block = blocks[s, 2 * c + core]
            c_block, s_block = table[0, pl.ds(block, 1), :], table[1, pl.ds(block, 1), :]
            c_in, s_in = table[2], table[3]
            here = slice((core * seqs + s) * blk, (core * seqs + s + 1) * blk)
            cosf[here, :] = c_block * c_in - s_block * s_in
            sinf[here, :] = (s_block * c_in + c_block * s_in) * sign
    for j in range(2 * chips):
        start = blocks[c // heads, j] * blk
        here = slice(j * blk, (j + 1) * blk)
        pos_row[:, here] = start + lane[0:8, :]

    own_tok.wait()
    for i in range(1, tps):
        came(tok.at[0:rows, 0:feats], zr.at[0, i - 1])
        part = tok.at[ds(k * rows, rows), ds(((z - i) % tps) * feats, feats)]
        go(remote(part, part, ps.at[0], pr.at[0], partner, z))
    for m in (0, 1, 2, 3):
        pass_w(m)
    send_w(4, 0)
    came(tok.at[0:rows, :], pr.at[0])

    def row_of(value):
        folded = value[:, :128]
        for h in range(1, heads):
            folded = folded + value[:, h * 128 : (h + 1) * 128]
        return jnp.sum(jnp.transpose(folded), axis=0, keepdims=True)

    def column_of(row):
        return jnp.transpose(jnp.broadcast_to(row, (128, both)))

    def totals(idx):
        n = 0
        for i in range(tps):
            for d in range(2):
                if i or d:
                    to = ctx if d == 0 else partner
                    go(remote(sq_own.at[idx], sq_rx.at[idx, n], ss.at[idx], sr.at[idx], to, zp(i)))
                    n += 1
        came(sq_rx.at[idx], sr.at[idx])
        total = sq_own[idx]
        for j in range(n):
            total = total + sq_rx[idx, j]
        return total

    for m in (0, 1, 2):
        wait_w(m)
        value = jnp.dot(tok[...], w[m][...], preferred_element_type=F32)
        if m == 0:
            q_raw[...] = value
            sq_own[0, 0:1, :] = row_of(value * value)
        elif m == 1:
            k_raw[...] = value
            sq_own[0, 1:2, :] = row_of(value * value)
        else:
            qkv[2] = value.astype(BF16).reshape(2, seqs, blk, head_w)
    sq_own[0, 2:8, :] = jnp.zeros((6, both), F32)
    squares = totals(0)
    inverse = lax.rsqrt(squares / width + EPS)
    inv_q[...] = column_of(inverse[0:1, :])
    inv_k[...] = column_of(inverse[1:2, :])
    for t, (raw, inv) in enumerate(((q_raw, inv_q), (k_raw, inv_k))):
        for h in range(heads):
            lanes = slice(h * HD, (h + 1) * HD)
            normed = raw[:, lanes] * inv[...] * gqk[t : t + 1, lanes]
            turned = normed * cosf[...] + pltpu.roll(normed, HD // 2, 1) * sinf[...]
            qkv[t, :, :, :, lanes] = turned.astype(BF16).reshape(2, seqs, blk, HD)

    def to_owner(idx, value, owned, stacked):
        size = owned.at[:, 0 : 2 * chips - 2] if stacked else owned.at[0 : 2 * chips - 2]
        for i in range(chips):
            to = chip(i)
            s, h = to // heads, to % heads
            if stacked:
                src = value.at[:, :, s, :, ds(h * HD, HD)]
                dst = owned.at[:, ds(2 * c, 2)]
            else:
                src = value.at[:, s, :, ds(h * HD, HD)]
                dst = owned.at[ds(2 * c, 2)]
            if i:
                go(remote(src, dst, as_.at[idx], ar.at[idx], to * 2 + k, z))
            else:
                own = pltpu.make_async_copy(src, dst, loc.at[20 + idx])
                own.start()
        return own, size, idx

    def from_owner(idx, owned, value, stacked):
        size = owned.at[:, 0 : 2 * chips - 2] if stacked else owned.at[0 : 2 * chips - 2]
        s, h = c // heads, c % heads
        for i in range(chips):
            to = chip(i)
            if stacked:
                src = owned.at[:, ds(2 * to, 2)]
                dst = value.at[:, :, s, :, ds(h * HD, HD)]
            else:
                src = owned.at[ds(2 * to, 2)]
                dst = value.at[:, s, :, ds(h * HD, HD)]
            if i:
                go(remote(src, dst, as_.at[idx], ar.at[idx], to * 2 + k, z))
            else:
                own = pltpu.make_async_copy(src, dst, loc.at[20 + idx])
                own.start()
        return own, size, idx

    def arrive(pair):
        own, size, idx = pair
        own.wait()
        came(size, ar.at[idx])
        sent(size, as_.at[idx])

    pair = to_owner(0, qkv, qa, True)
    send_w(4, 1)
    arrive(pair)
    step = 2 * blk

    def attend(i, carry):
        here = ds(i * step, step)
        q = qa[0, pl.ds(2 * i, 2)].reshape(step, HD)
        s = lax.dot_general(q, qa[1].reshape(total, HD), NT, preferred_element_type=F32) * scale
        at = lax.broadcasted_iota(jnp.int32, (step, 1), 0)
        first = blocks[c // heads, 2 * i] * blk
        second = (blocks[c // heads, 2 * i + 1] - 1) * blk
        visible = pos_row[0:1, :] <= at + jnp.where(at < blk, first, second)
        s = jnp.where(visible, s, NEGATIVE)
        top = jnp.max(s, axis=1, keepdims=True)
        e = jnp.where(visible, jnp.exp(s - top), 0.0)
        p = (e * (1.0 / jnp.sum(e, axis=1, keepdims=True))).astype(BF16)
        probs[here, :] = p
        o = jnp.dot(p, qa[2].reshape(total, HD), preferred_element_type=F32)
        att_f[here, :] = o
        att_st[pl.ds(2 * i, 2)] = o.astype(BF16).reshape(2, blk, HD)
        return carry

    lax.fori_loop(0, chips, attend, 0)
    back = from_owner(1, att_st, att, False)
    pass_w(4)
    send_w(5, 0)
    send_w(5, 1)
    send_w(6, 0)
    own_gain2.wait()
    came(gall.at[0 : tps - 1], mr.at[2])
    for r in range(2):
        pieces = []
        for zz in range(tps):
            for m in range(chips):
                pieces.append(gall[zz, 2 * m, 2 + r : 3 + r, :] + gall[zz, 2 * m + 1, 2 + r : 3 + r, :])
        gfull[r : r + 1, :] = jnp.concatenate(pieces, axis=1)
    for s in range(width // 256):
        tok_t[s * 256 : (s + 1) * 256, :] = jnp.transpose(tok[:, s * 256 : (s + 1) * 256])
    arrive(back)
    wait_w(3)

    cw = feats
    rs_live = {}

    def rp_copy(idx, i, off):
        return remote(st_p.at[:, ds(off, cw)], rx_p.at[idx % 2, :, ds(off, cw)], rps.at[idx], rpr.at[idx, i], partner, z)

    def rz_copy(idx, i, j, off):
        return remote(
            st_z.at[ds(zp(j) * share_rows, share_rows), ds(off, cw)],
            rx_z.at[idx % 2, j - 1, :, ds(off, cw)],
            rzs.at[idx],
            rzr.at[idx],
            ctx,
            zp(j),
        )

    def reduce_rows(idx, partial, offset, before=None, meanwhile=None):
        def one(i):
            off = offset(i)
            if before is not None:
                before(i)
            st_p[:, ds(off, cw)] = partial(ok, off).astype(BF16)
            rp_copy(idx, i, off).start()
            mine = partial(k, off)
            rp_copy(idx, i, off).wait_recv()
            st_z[:, ds(off, cw)] = (mine + rx_p[idx % 2, :, ds(off, cw)].astype(F32)).astype(BF16)
            for j in range(1, tps):
                rz_copy(idx, i, j, off).start()

        if before is None:
            lax.fori_loop(0, tps, lambda i, x: (one(i), x)[1], 0)
        else:
            for i in range(tps):
                one(i)
        if meanwhile is not None:
            meanwhile()
        came(rx_z.at[idx % 2], rzr.at[idx])
        sent(rx_z.at[idx % 2], rzs.at[idx])
        sent(st_p, rps.at[idx])
        mine = st_z[ds(z * share_rows, share_rows), :].astype(F32)
        for j in range(tps - 1):
            mine = mine + rx_z[idx % 2, j].astype(F32)
        return mine

    def straight(i):
        return i * cw

    def mean_of(value):
        return jnp.sum(value, axis=1, keepdims=True) / width

    def spread(idx, buf):
        mine = buf.at[ds(k * rows + z * share_rows, share_rows), :]
        for i in range(1, tps):
            go(remote(mine, mine, zs.at[idx], zr.at[idx, i - 1], ctx, zp(i)))
        go(remote(mine, mine, ps.at[idx], pr.at[idx], partner, z))

        def finish(meanwhile=None):
            for i in range(1, tps):
                came(buf.at[0:share_rows, :], zr.at[idx, i - 1])
                if i == 2 and meanwhile is not None:
                    meanwhile()
                part = buf.at[ds(k * rows + ((z - i) % tps) * share_rows, share_rows), :]
                go(remote(part, part, ps.at[idx], pr.at[idx], partner, z))
            came(buf.at[0:rows, :], pr.at[idx])
            sent(buf.at[0 : (tps - 1) * share_rows, :], zs.at[idx])
            sent(buf.at[0:rows, :], ps.at[idx])

        return finish

    my_rows = ds(k * rows + z * share_rows, share_rows)
    heads_rows = [None]

    def o_partial(core, off):
        left = att[pl.ds(core, 1)].reshape(rows, head_w)
        return jnp.dot(left, w[3][:, ds(off, cw)], preferred_element_type=F32)

    value = reduce_rows(0, o_partial, straight)
    proj[...] = value
    a_inverse = lax.rsqrt(mean_of(value * value) + EPS)
    state = tok[my_rows, :].astype(F32) + value * a_inverse * gfull[0:1, :]
    hstate[...] = state
    hid[my_rows, :] = state.astype(BF16)
    finish = spread(1, hid)
    own_cot.wait()
    came(cot.at[:, 0 : (tps - 1) * feats], mr.at[1])
    att_t[...] = jnp.transpose(att[...].reshape(both, head_w))

    def more_weights():
        pass_w(5)
        send_w(6, 1)

    finish(more_weights)

    fw = 256
    wait_w(4)

    def gate_step(j, carry):
        here = ds(j * fw, fw)
        lin[:, here] = jnp.dot(hid[...], w[4][:, here], preferred_element_type=F32)
        return carry

    lax.fori_loop(0, ff_w // fw, gate_step, 0)
    for s in range(width // 256):
        hid_t[s * 256 : (s + 1) * 256, :] = jnp.transpose(hid[:, s * 256 : (s + 1) * 256])
    wait_w(5)

    def up_step(j, carry):
        here = ds(j * fw, fw)
        up = jnp.dot(hid[...], w[5][:, here], preferred_element_type=F32)
        gate = lin[:, here]
        sigma = jax.nn.sigmoid(gate)
        swish = gate * sigma
        lin[:, here] = swish
        fac[:, here] = up * sigma * (1.0 + gate * (1.0 - sigma))
        value = (swish * up).astype(BF16)
        act[:, here] = value
        act_t[here, :] = jnp.transpose(value)
        return carry

    lax.fori_loop(0, ff_w // fw, up_step, 0)

    def down_partial(core, off):
        return jnp.dot(act[ds(core * rows, rows), :], w[6][:, ds(off, cw)], preferred_element_type=F32)

    def from_chip(i):
        return (c, near[0], near[1], far)[i] * cw

    def down_ready(i):
        if i == 0:
            w_own[6].wait()
        if i == 1:
            pass_w(6)
        got_w(6, *((4,), (0, 1), (2, 3), (5, 6))[i])

    value = reduce_rows(1, down_partial, from_chip, down_ready)
    m_inverse = lax.rsqrt(mean_of(value * value) + EPS)
    scaled = value * m_inverse
    upstream = cot[...].astype(F32)
    gained = upstream * gfull[1:2, :]
    back_mix = m_inverse * gained - scaled * (m_inverse * m_inverse) * mean_of(gained * value)
    dmix[my_rows, :] = back_mix.astype(BF16)
    order = (far, near[0], near[1], c)

    def mix_along(n, i):
        here = dmix.at[my_rows, ds(order[n] * cw, cw)]
        return remote(here, here, xs.at[n], xr.at[n], ctx, zp(i))

    def mix_across(n, i):
        owner = (z - i) % tps
        here = dmix.at[ds(k * rows + owner * share_rows, share_rows), ds(order[n] * cw, cw)]
        return remote(here, here, xs.at[chips], xr.at[chips + n], partner, z)

    def mix_start(n):
        for i in range(1, tps):
            mix_along(n, i).start()
        mix_across(n, 0).start()

    mix_start(0)
    gg_row[1:2, :] = jnp.sum(upstream * scaled, axis=0, keepdims=True)
    stage[...] = hstate[...] + scaled * gfull[1:2, :]

    free_w(6)
    for n in range(chips):
        sent(dmix.at[0:share_rows, 0 : (tps - 1) * cw], xs.at[n])
        if n < chips - 1:
            mix_start(n + 1)
        came(dmix.at[0:share_rows, 0 : (tps - 1) * cw], xr.at[n])
        for i in range(1, tps):
            mix_across(n, i).start()
        came(dmix.at[0:rows, 0:cw], xr.at[chips + n])
        off = order[n] * cw

        def dact_step(j, carry):
            here = ds(j * fw, fw)
            d_act = lax.dot_general(dmix[:, ds(off, cw)], w[6][here, ds(off, cw)], NT, preferred_element_type=F32)
            part = (ds((j // 2) * both, both), ds((j % 2) * fw, fw))
            if n:
                d_act = d_act + d_acc[part]
            if n < chips - 1:
                d_acc[part] = d_act
            else:
                dup[:, here] = (d_act * lin[:, here]).astype(BF16)
                dgate[:, here] = (d_act * fac[:, here]).astype(BF16)
            return carry

        lax.fori_loop(0, ff_w // fw, dact_step, 0)
        grad = jnp.dot(act_t[...], dmix[:, ds(off, cw)], preferred_element_type=F32)
        w[6][:, ds(off, cw)] = grad.astype(BF16)
        if n == 0:
            send_far(6)
        elif n < chips - 1:
            send_near(6, n - 1)
        else:
            send_home(6)

    sent(dmix.at[0:rows, :], xs.at[chips])
    for i in range(1, tps):
        go(remote(stage.at[:, ds(zp(i) * feats, feats)], out_ref.at[ds(z * share_rows, share_rows), :], ms.at[3], mr.at[3], ctx, zp(i)))
    own_out = pltpu.make_async_copy(stage.at[:, ds(z * feats, feats)], out_ref.at[ds(z * share_rows, share_rows), :], loc.at[24])
    own_out.start()

    def ff_partial(core, off):
        here = ds(core * rows, rows)
        return lax.dot_general(dgate[here, :], w[4][ds(off, cw), :], NT, preferred_element_type=F32) + lax.dot_general(
            dup[here, :], w[5][ds(off, cw), :], NT, preferred_element_type=F32
        )

    def ggate_step(j, carry):
        here = ds(j * fw, fw)
        w[4][:, here] = jnp.dot(hid_t[...], dgate[:, here], preferred_element_type=F32).astype(BF16)
        return carry

    def gate_grad():
        free_w(4)
        lax.fori_loop(0, ff_w // fw, ggate_step, 0)
        pass_g(6)
        send_g(4)

    value = reduce_rows(2, ff_partial, straight, meanwhile=gate_grad) + cot[...].astype(F32)
    dhid[...] = value
    projected = proj[...]
    a_inverse = lax.rsqrt(mean_of(projected * projected) + EPS)
    scaled = projected * a_inverse
    gained = value * gfull[0:1, :]
    gg_row[0:1, :] = jnp.sum(value * scaled, axis=0, keepdims=True)
    gg_row[2:8, :] = jnp.zeros((6, width), F32)
    back_att = a_inverse * gained - scaled * (a_inverse * a_inverse) * mean_of(gained * projected)
    dattn[my_rows, :] = back_att.astype(BF16)
    finish = spread(3, dattn)
    for i in range(1, tps):
        go(remote(gg_row.at[:, ds(zp(i) * feats, feats)], gg_rx1.at[i - 1], ms.at[4], mr.at[4], ctx, zp(i)))

    def gup_step(j, carry):
        here = ds(j * fw, fw)
        w[5][:, here] = jnp.dot(hid_t[...], dup[:, here], preferred_element_type=F32).astype(BF16)
        return carry

    free_w(5)
    lax.fori_loop(0, ff_w // fw, gup_step, 0)
    finish()

    value = lax.dot_general(dattn[...], w[3][...], NT, preferred_element_type=F32)
    dh[...] = value.astype(BF16).reshape(2, seqs, blk, head_w)
    pair = to_owner(2, dh, d_o, False)
    pass_g(4)

    def go_step(j, carry):
        here = ds(j * fw, fw)
        w[3][:, here] = jnp.dot(att_t[...], dattn[:, here], preferred_element_type=F32).astype(BF16)
        return carry

    free_w(3)
    lax.fori_loop(0, width // fw, go_step, 0)
    arrive(pair)
    dk_acc, dv_acc = d_acc.at[:, 0:HD], d_acc.at[:, HD : 2 * HD]
    dk_acc[...] = jnp.zeros((total, HD), F32)
    dv_acc[...] = jnp.zeros((total, HD), F32)

    def unattend(i, carry):
        here = ds(i * step, step)
        q = qa[0, pl.ds(2 * i, 2)].reshape(step, HD)
        d_out = d_o[pl.ds(2 * i, 2)].reshape(step, HD)
        d_p = lax.dot_general(d_out, qa[2].reshape(total, HD), NT, preferred_element_type=F32)
        delta = jnp.sum(d_out.astype(F32) * att_f[here, :], axis=1, keepdims=True)
        p = probs[here, :]
        d_s = (p.astype(F32) * (d_p - delta)).astype(BF16)
        d_q = jnp.dot(d_s, qa[1].reshape(total, HD), preferred_element_type=F32) * scale
        dqkv_st[0, pl.ds(2 * i, 2)] = d_q.astype(BF16).reshape(2, blk, HD)
        dk_acc[...] += lax.dot_general(d_s, q, TN, preferred_element_type=F32)
        dv_acc[...] += lax.dot_general(p, d_out, TN, preferred_element_type=F32)
        return carry

    lax.fori_loop(0, chips, unattend, 0)
    dqkv_st[1] = (dk_acc[...] * scale).astype(BF16).reshape(2 * chips, blk, HD)
    dqkv_st[2] = dv_acc[...].astype(BF16).reshape(2 * chips, blk, HD)
    pair = from_owner(3, dqkv_st, dqkv, True)

    send_g(5)
    send_g(3)
    arrive(pair)

    gg_mid[...] = jnp.zeros((8, feats), F32)
    for t, (raw, inv) in enumerate(((q_raw, inv_q), (k_raw, inv_k))):
        folded = None
        for h in range(heads):
            lanes = slice(h * HD, (h + 1) * HD)
            turned = dqkv[t, :, :, :, lanes].reshape(both, HD).astype(F32)
            back_rot = turned * cosf[...] - pltpu.roll(turned, HD // 2, 1) * sinf[...]
            plain = raw[:, lanes]
            scaled = plain * inv[...]
            gg_mid[2 + t : 3 + t, pl.ds(pl.multiple_of(k * head_w + h * HD, HD), HD)] = jnp.sum(back_rot * scaled, axis=0, keepdims=True)
            gained = back_rot * gqk[t : t + 1, lanes]
            dqkv[t, :, :, :, lanes] = gained.astype(BF16).reshape(2, seqs, blk, HD)
            term = gained * plain
            folded = term if folded is None else folded + term
        sq_own[1, t : t + 1, :] = jnp.sum(jnp.transpose(folded), axis=0, keepdims=True)
    sq_own[1, 2:8, :] = jnp.zeros((6, both), F32)
    dots = totals(1) / width
    for t, (raw, inv) in enumerate(((q_raw, inv_q), (k_raw, inv_k))):
        spread_dot = column_of(dots[t : t + 1, :])
        for h in range(heads):
            lanes = slice(h * HD, (h + 1) * HD)
            gained = dqkv[t, :, :, :, lanes].reshape(both, HD).astype(F32)
            r = inv[...]
            grad = r * gained - raw[:, lanes] * (r * r * r) * spread_dot
            dqkv[t, :, :, :, lanes] = grad.astype(BF16).reshape(2, seqs, blk, HD)

    def rf_copy(i, off):
        return remote(st_z.at[:, ds(off, cw)], rx_f.at[i], rzs.at[3], rzr.at[3], ctx, zp(i + 1))

    def in_partial(core, off):
        here = ds(off, cw)
        acc = None
        for t in range(3):
            left = dqkv[t, pl.ds(core, 1)].reshape(rows, head_w)
            term = lax.dot_general(left, w[t][here, :], NT, preferred_element_type=F32)
            acc = term if acc is None else acc + term
        return acc

    own_rows = ds(z * share_rows, share_rows)
    for i in range(tps):
        off = zp(i + 1) * cw
        st_p[:, ds(off, cw)] = in_partial(ok, off).astype(BF16)
        rp_copy(3, i, off).start()
        mine = in_partial(k, off)
        rp_copy(3, i, off).wait_recv()
        st_z[:, ds(off, cw)] = (mine + rx_p[1, :, ds(off, cw)].astype(F32)).astype(BF16)
        st_z[own_rows, ds(off, cw)] = (st_z[own_rows, ds(off, cw)].astype(F32) + dhid[:, ds(off, cw)]).astype(BF16)
        if i < tps - 1:
            rf_copy(i, off).start()

    pass_g(5)
    pass_g(3)
    for m in range(3):

        def gqkv_step(j, carry):
            here = ds(j * 512, 512)
            right = dqkv[m].reshape(both, head_w)
            w[m][here, :] = jnp.dot(tok_t[here, :], right, preferred_element_type=F32).astype(BF16)
            return carry

        free_w(m)
        lax.fori_loop(0, width // 512, gqkv_step, 0)
        send_g(m)
    middle = gg_row[:, ds(z * feats, feats)]
    came(gg_rx1, mr.at[4])
    for i in range(tps - 1):
        middle = middle + gg_rx1[i]
    gg_mid[...] = gg_mid[...] + middle
    n = 0
    for i, d in slots:
        if i or d:
            core = (k + d) % 2
            go(remote(gg_mid.at[:, ds(chip(i) * 128, 128)], gg_rx2.at[n], ms.at[5], mr.at[5], chip(i) * 2 + core, z))
            n += 1

    add_up(6)
    add_up(4)
    for m in range(3):
        pass_g(m)
    add_up(3)
    add_up(5)
    came(rx_f, rzr.at[3])
    sent(rx_f, rzs.at[3])
    sent(st_p, rps.at[3])
    final = st_z[:, ds(z * feats, cw)].astype(F32)
    for i in range(tps - 1):
        final = final + rx_f[i].astype(F32)
    gin_ref[...] = final
    gain_sum = gg_mid[:, ds(c * 128, 128)]
    came(gg_rx2, mr.at[5])
    for i in range(2 * chips - 1):
        gain_sum = gain_sum + gg_rx2[i]
    ggain_ref[...] = jnp.where(k == 1, pltpu.roll(gain_sum, 64, 1), gain_sum)
    own_out.wait()
    came(stage.at[:, 0 : (tps - 1) * feats], mr.at[3])
    for m in range(3):
        wait_g(m)
    sent(tok.at[0:rows, 0 : (tps - 1) * feats], zs.at[0])
    sent(tok.at[0:rows, :], ps.at[0])
    sent(gbuf.at[0 : 2 * chips - 1], ms.at[0])
    sent(cot.at[:, 0 : (tps - 1) * feats], ms.at[1])
    sent(gall.at[0 : tps - 1], ms.at[2])
    sent(stage.at[:, 0 : (tps - 1) * feats], ms.at[3])
    sent(gg_rx1, ms.at[4])
    sent(gg_rx2, ms.at[5])
    for idx in range(2):
        sent(sq_rx.at[idx], ss.at[idx])
    for m in range(7):
        sent(slabs(m, 5), ws.at[m, 0])
        sent(slabs(m, 7), gs.at[m])


def fused(
    tokens,
    w_query,
    w_key,
    w_value,
    w_output,
    w_gate,
    w_up,
    w_down,
    gain_query,
    gain_key,
    gain_attention,
    gain_feedforward,
    block_order,
    cotangent,
):
    seqs, blk, feats = tokens.shape
    tps = lax.axis_size("tp")
    chips = lax.axis_size("ctx") // 2
    width = feats * tps
    rows = seqs * blk
    both = 2 * rows
    share_rows = rows // tps
    total = 2 * chips * blk
    head_w = w_query.shape[1] // 2
    ff_w = w_gate.shape[1] // 2
    heads = head_w // HD
    slab = width // (2 * chips)
    ctx = lax.axis_index("ctx")
    frequency = THETA ** (-2.0 * np.arange(HD // 2) / HD)
    frequency = np.concatenate([frequency, frequency])
    starts = np.zeros((blk, 1))
    starts[: 2 * chips, 0] = np.arange(2 * chips) * blk
    inside = np.arange(blk)[:, None] * 1.0
    table = np.stack([f(at * frequency) for at in (starts, inside) for f in (np.cos, np.sin)]).astype(np.float32)
    gains = jnp.stack([gain_query, gain_key, gain_attention, gain_feedforward]).astype(F32)
    gains = jnp.pad(gains, ((0, 4), (0, 0)))
    blank = jnp.zeros_like(gains)
    gtile = jnp.where(ctx % 2 == 0, jnp.concatenate([gains, blank], axis=1), jnp.concatenate([blank, gains], axis=1))
    weights = (w_query, w_key, w_value, w_output, w_gate, w_up, w_down)
    dims = (chips, tps, seqs, blk, width, head_w, ff_w)
    halves = (head_w, head_w, head_w, head_w, ff_w, ff_w, ff_w)
    hbm = pl.BlockSpec(memory_space=pl.ANY)
    vmem = pl.BlockSpec(memory_space=pltpu.VMEM)

    def v(shape, dtype=BF16):
        return pltpu.VMEM(shape, dtype)

    w_shapes = [v((width, h)) if m in COLS else v((h, width)) for m, h in enumerate(halves)]
    dma = pltpu.SemaphoreType.DMA
    v_shapes = [v((2, slab, h)) if m in COLS else v((2, h, slab)) for m, h in enumerate(halves)]
    scratch = w_shapes + v_shapes + [
        v((both, width)),
        v((width, both)),
        v((both, width)),
        v((width, both)),
        v((both, width)),
        v((both, width)),
        v((both, ff_w), F32),
        v((both, ff_w), F32),
        v((both, ff_w)),
        v((ff_w, both)),
        v((both, ff_w)),
        v((both, ff_w)),
        v((rows, width)),
        v((2, rows, width)),
        v((rows, width)),
        v((2, tps - 1, share_rows, width)),
        v((tps - 1, rows, feats)),
        v((both, head_w), F32),
        v((both, head_w), F32),
        v((3, 2, seqs, blk, head_w)),
        v((3, 2 * chips, blk, HD)),
        v((total, total)),
        v((total, HD), F32),
        v((2 * chips, blk, HD)),
        v((2, seqs, blk, head_w)),
        v((head_w, both)),
        v((2, seqs, blk, head_w)),
        v((2 * chips, blk, HD)),
        v((3, 2 * chips, blk, HD)),
        v((3, 2, seqs, blk, head_w)),
        v((2, 8, both), F32),
        v((2, 2 * tps - 1, 8, both), F32),
        v((both, 128), F32),
        v((both, 128), F32),
        v((share_rows, width)),
        v((share_rows, width), F32),
        v((share_rows, width), F32),
        v((share_rows, width), F32),
        v((share_rows, width), F32),
        v((2 * chips, 8, 128), F32),
        v((tps, 2 * chips, 8, 128), F32),
        v((8, width), F32),
        v((8, head_w), F32),
        v((8, width), F32),
        v((tps - 1, 8, feats), F32),
        v((8, feats), F32),
        v((2 * chips - 1, 8, 128), F32),
        dma((7, 2)),
        dma((7, 7)),
        dma((7,)),
        dma((7, 3)),
        dma((4,)),
        dma((4, tps - 1)),
        dma((4,)),
        dma((4,)),
        dma((4,)),
        dma((4, tps)),
        dma((4,)),
        dma((4,)),
        dma((6,)),
        dma((6,)),
        dma((2,)),
        dma((2,)),
        dma((4,)),
        dma((4,)),
        dma((25,)),
        v((2 * both, ff_w // 2), F32),
        v((both, HD), F32),
        v((both, HD), F32),
        v((8, total), jnp.int32),
        dma((chips + 1,)),
        dma((2 * chips,)),
    ]
    results = pl.pallas_call(
        functools.partial(layer_kernel, dims),
        out_shape=[
            jax.ShapeDtypeStruct((rows, feats), F32),
            jax.ShapeDtypeStruct((rows, feats), F32),
            jax.ShapeDtypeStruct((8, 128), F32),
        ]
        + [jax.ShapeDtypeStruct((3,) + weight.shape, BF16) for weight in weights]
        + [jax.ShapeDtypeStruct(weight.shape, BF16) for weight in weights[3:]],
        in_specs=[hbm] * 9 + [pl.BlockSpec(memory_space=pltpu.SMEM), vmem, vmem],
        out_specs=[hbm, vmem, vmem] + [hbm] * 11,
        scratch_shapes=scratch,
        compiler_params=pltpu.CompilerParams(
            collective_id=0, has_side_effects=True, vmem_limit_bytes=67043328
        ),
        name="layer",
    )(tokens.reshape(rows, feats), cotangent.reshape(rows, feats), *weights, block_order, gtile, table)
    output = results[0].reshape(tokens.shape)
    grad_input = results[1].reshape(tokens.shape)
    grads = [jnp.sum(received.astype(F32), axis=0) for received in results[3:6]]
    grads += [value.astype(F32) for value in results[10:]]
    lanes = results[2][:, :64]
    return (output, grad_input, *grads, lanes[2], lanes[3], lanes[0], lanes[1])


def fits(mesh):
    return mesh.shape["ctx"] == 8 and mesh.shape["tp"] == 4


def solution(mesh):
    placed = (
        P(None, "ctx", "tp"),
        P("ctx", "tp"),
        P("ctx", "tp"),
        P("ctx", "tp"),
        P("tp", "ctx"),
        P("ctx", "tp"),
        P("ctx", "tp"),
        P("tp", "ctx"),
        P(("tp", "ctx")),
        P(("tp", "ctx")),
        P(("tp", "ctx")),
        P(("tp", "ctx")),
        P(),
        P(None, "ctx", "tp"),
    )
    return jax.shard_map(
        fused if fits(mesh) else shards,
        mesh=mesh,
        in_specs=placed,
        out_specs=(
            P(None, "ctx", "tp"),
            P(None, "ctx", "tp"),
            P("ctx", "tp"),
            P("ctx", "tp"),
            P("ctx", "tp"),
            P("tp", "ctx"),
            P("ctx", "tp"),
            P("ctx", "tp"),
            P("tp", "ctx"),
            P(("tp", "ctx")),
            P(("tp", "ctx")),
            P(("tp", "ctx")),
            P(("tp", "ctx")),
        ),
        check_vma=False,
    )
```

```python
import functools

import jax
import jax.numpy as jnp
import numpy as np
from jax import lax
from jax.experimental import pallas as pl
from jax.experimental.pallas import tpu as pltpu
from jax.sharding import PartitionSpec as P

HD = 128


EPS = 1e-06
THETA = 500000.0
NEGATIVE = -1e30


def full_width(value):
    return lax.all_gather(value, "tp", axis=2, tiled=True)


def share(value):
    return lax.psum_scatter(value, "tp", scatter_dimension=2, tiled=True)


def tp_total(values):
    return lax.psum(values, "tp")


def rotary_tables(positions):
    half_dim = HD // 2
    frequency = THETA ** (-2.0 * jnp.arange(half_dim, dtype=jnp.float32) / HD)
    angles = positions.astype(jnp.float32)[..., None] * frequency
    return (jnp.cos(angles)[..., None, :], jnp.sin(angles)[..., None, :])


def rotate(value, cosine, sine):
    half_dim = value.shape[-1] // 2
    first, second = (value[..., :half_dim], value[..., half_dim:])
    return jnp.concatenate(
        [first * cosine - second * sine, second * cosine + first * sine], axis=-1
    )


def unrotate(grad, cosine, sine):
    half_dim = grad.shape[-1] // 2
    first, second = (grad[..., :half_dim], grad[..., half_dim:])
    return jnp.concatenate(
        [first * cosine + second * sine, second * cosine - first * sine], axis=-1
    )


def key_positions(block_order, start, count, block_len):
    slots = start + jnp.arange(count, dtype=jnp.int32)
    owner = slots // block_len
    ranks = jnp.arange(block_order.shape[1], dtype=jnp.int32)
    chosen = jnp.sum(
        jnp.where(owner[None, :, None] == ranks[None, None, :], block_order[:, None, :], 0), axis=2
    )
    return chosen * block_len + slots % block_len


def span_of():
    return 512


def shards(
    tokens,
    w_query,
    w_key,
    w_value,
    w_output,
    w_gate,
    w_up,
    w_down,
    gain_query,
    gain_key,
    gain_attention,
    gain_feedforward,
    block_order,
    cotangent,
):
    gathered = (
        lax.all_gather(w_query, "ctx", axis=0, tiled=True),
        lax.all_gather(w_key, "ctx", axis=0, tiled=True),
        lax.all_gather(w_value, "ctx", axis=0, tiled=True),
        lax.all_gather(w_output, "ctx", axis=1, tiled=True),
        lax.all_gather(w_gate, "ctx", axis=0, tiled=True),
        lax.all_gather(w_up, "ctx", axis=0, tiled=True),
        lax.all_gather(w_down, "ctx", axis=1, tiled=True),
        lax.all_gather(gain_query, "ctx", axis=0, tiled=True),
        lax.all_gather(gain_key, "ctx", axis=0, tiled=True),
        lax.all_gather(gain_attention, "ctx", axis=0, tiled=True),
        lax.all_gather(gain_feedforward, "ctx", axis=0, tiled=True),
    )
    wq_full, wk_full, wv_full, wo_full, wg_full, wu_full, wd_full = gathered[:7]
    g_query = gathered[7].astype(jnp.float32)
    g_key = gathered[8].astype(jnp.float32)
    g_attn = gathered[9].astype(jnp.float32)
    g_feed = gathered[10].astype(jnp.float32)
    seq_count, block_len, local_width = tokens.shape
    row_count = seq_count * block_len
    scale = HD ** (-0.5)
    tok_full = full_width(tokens)
    tok_rows = tok_full.reshape(row_count, -1)
    width = tok_rows.shape[1]
    queries = jnp.dot(tok_rows, wq_full, preferred_element_type=jnp.float32)
    keys_raw = jnp.dot(tok_rows, wk_full, preferred_element_type=jnp.float32)
    values_raw = jnp.dot(tok_rows, wv_full, preferred_element_type=jnp.float32)
    head_width = queries.shape[1]
    head_count = head_width // HD
    q_squares, k_squares = tp_total(
        (jnp.sum(queries * queries, axis=1), jnp.sum(keys_raw * keys_raw, axis=1))
    )
    q_inverse = lax.rsqrt(q_squares / width + EPS)[:, None]
    k_inverse = lax.rsqrt(k_squares / width + EPS)[:, None]
    q_normed = queries * q_inverse * g_query
    k_normed = keys_raw * k_inverse * g_key
    ctx_rank = lax.axis_index("ctx")
    ranks = jnp.arange(block_order.shape[1], dtype=jnp.int32)
    my_block = jnp.sum(jnp.where(ranks[None, :] == ctx_rank, block_order, 0), axis=1)
    q_pos = my_block[:, None] * block_len + jnp.arange(block_len, dtype=jnp.int32)[None, :]
    cosine, sine = rotary_tables(q_pos)
    q_rot = rotate(q_normed.reshape(seq_count, block_len, head_count, HD), cosine, sine).astype(
        jnp.bfloat16
    )
    k_rot = rotate(k_normed.reshape(seq_count, block_len, head_count, HD), cosine, sine).astype(
        jnp.bfloat16
    )
    k_flat = k_rot.reshape(seq_count, block_len, head_width)
    v_flat = values_raw.astype(jnp.bfloat16).reshape(seq_count, block_len, head_width)

    def stat_block(state, key_piece, k_pos):
        run_max, run_sum = state
        scores = (
            jnp.einsum("sqhd,skhd->shqk", q_rot, key_piece, preferred_element_type=jnp.float32)
            * scale
        )
        visible = k_pos[:, None, None, :] <= q_pos[:, None, :, None]
        scores = jnp.where(visible, scores, NEGATIVE)
        new_max = jnp.maximum(run_max, jnp.max(scores, axis=-1))
        weights = jnp.where(visible, jnp.exp(scores - new_max[..., None]), 0.0)
        run_sum = run_sum * jnp.exp(run_max - new_max) + jnp.sum(weights, axis=-1)
        return (new_max, run_sum)

    init = (
        jnp.full((seq_count, head_count, block_len), NEGATIVE, jnp.float32),
        jnp.zeros((seq_count, head_count, block_len), jnp.float32),
    )
    fold_key_all = lax.all_gather(k_flat, "ctx", axis=1, tiled=True)
    count = fold_key_all.shape[1]
    span = span_of()

    def fold_one_span(step_index, inner):
        offset = step_index * span
        key_piece = lax.dynamic_slice_in_dim(fold_key_all, offset, span, 1).reshape(
            seq_count, span, head_count, HD
        )
        k_pos = key_positions(block_order, offset, span, block_len)
        return stat_block(inner, key_piece, k_pos)

    run_max, run_sum = lax.fori_loop(0, count // span, fold_one_span, init)
    key_all, val_all = (
        lax.all_gather(k_flat, "ctx", axis=1, tiled=True),
        lax.all_gather(v_flat, "ctx", axis=1, tiled=True),
    )
    log_total = run_max + jnp.log(run_sum)
    total_len = key_all.shape[1]
    total_span = span_of()

    def value_span(step_index, acc):
        offset = step_index * total_span
        key_piece = lax.dynamic_slice_in_dim(key_all, offset, total_span, 1).reshape(
            seq_count, total_span, head_count, HD
        )
        val_piece = lax.dynamic_slice_in_dim(val_all, offset, total_span, 1).reshape(
            seq_count, total_span, head_count, HD
        )
        k_pos = key_positions(block_order, offset, total_span, block_len)
        scores = (
            jnp.einsum("sqhd,skhd->shqk", q_rot, key_piece, preferred_element_type=jnp.float32)
            * scale
        )
        visible = k_pos[:, None, None, :] <= q_pos[:, None, :, None]
        weights = jnp.where(visible, jnp.exp(scores - log_total[..., None]), 0.0).astype(
            jnp.bfloat16
        )
        return acc + jnp.einsum(
            "shqk,skhd->sqhd", weights, val_piece, preferred_element_type=jnp.float32
        )

    attended = lax.fori_loop(
        0,
        total_len // total_span,
        value_span,
        jnp.zeros((seq_count, block_len, head_count, HD), jnp.float32),
    )
    attn_bf = attended.reshape(row_count, head_width).astype(jnp.bfloat16)
    attn_proj = share(
        jnp.dot(attn_bf, wo_full, preferred_element_type=jnp.float32).reshape(
            seq_count, block_len, -1
        )
    )
    (a_squares,) = tp_total((jnp.sum(attn_proj * attn_proj, axis=2),))
    a_inverse = lax.rsqrt(a_squares / width + EPS)[..., None]
    hidden_state = tokens.astype(jnp.float32) + attn_proj * a_inverse * g_attn
    hidden_rows = full_width(hidden_state.astype(jnp.bfloat16)).reshape(row_count, -1)
    gate = jnp.dot(hidden_rows, wg_full, preferred_element_type=jnp.float32)
    up_vals = jnp.dot(hidden_rows, wu_full, preferred_element_type=jnp.float32)
    sigma = jax.nn.sigmoid(gate)
    activation = (gate * sigma * up_vals).astype(jnp.bfloat16)
    mixed = share(
        jnp.dot(activation, wd_full, preferred_element_type=jnp.float32).reshape(
            seq_count, block_len, -1
        )
    )
    (m_squares,) = tp_total((jnp.sum(mixed * mixed, axis=2),))
    m_inverse = lax.rsqrt(m_squares / width + EPS)[..., None]
    output = hidden_state + mixed * m_inverse * g_feed
    upstream = cotangent.astype(jnp.float32)
    (m_dots,) = tp_total((jnp.sum(g_feed * upstream * mixed, axis=2),))
    d_mixed = m_inverse * (g_feed * upstream) - mixed * m_inverse**3 * (m_dots / width)[..., None]
    d_gfeed = jnp.sum(upstream * mixed * m_inverse, axis=(0, 1))
    d_mixed_rows = full_width(d_mixed.astype(jnp.bfloat16)).reshape(row_count, -1)
    grad_down = jnp.dot(activation.T, d_mixed_rows, preferred_element_type=jnp.float32)
    d_act = jnp.dot(d_mixed_rows, wd_full.T, preferred_element_type=jnp.float32)
    d_up_bf = (d_act * gate * sigma).astype(jnp.bfloat16)
    d_gate_bf = (d_act * up_vals * sigma * (1.0 + gate * (1.0 - sigma))).astype(jnp.bfloat16)
    grad_gate = jnp.dot(hidden_rows.T, d_gate_bf, preferred_element_type=jnp.float32)
    grad_up = jnp.dot(hidden_rows.T, d_up_bf, preferred_element_type=jnp.float32)
    back_ff = jnp.dot(d_gate_bf, wg_full.T, preferred_element_type=jnp.float32) + jnp.dot(
        d_up_bf, wu_full.T, preferred_element_type=jnp.float32
    )
    d_hidden = upstream + share(back_ff.reshape(seq_count, block_len, -1))
    (a_dots,) = tp_total((jnp.sum(g_attn * d_hidden * attn_proj, axis=2),))
    d_attn = (
        a_inverse * (g_attn * d_hidden) - attn_proj * a_inverse**3 * (a_dots / width)[..., None]
    )
    d_gattn = jnp.sum(d_hidden * attn_proj * a_inverse, axis=(0, 1))
    d_attn_rows = full_width(d_attn.astype(jnp.bfloat16)).reshape(row_count, -1)
    grad_outproj = jnp.dot(attn_bf.T, d_attn_rows, preferred_element_type=jnp.float32)
    d_heads = jnp.dot(d_attn_rows, wo_full.T, preferred_element_type=jnp.float32).reshape(
        seq_count, block_len, head_count, HD
    )
    deltas = jnp.sum(d_heads * attended, axis=3).transpose(0, 2, 1)
    d_heads_bf = d_heads.astype(jnp.bfloat16)

    def grad_block(key_piece, val_piece, k_pos):
        scores = (
            jnp.einsum("sqhd,skhd->shqk", q_rot, key_piece, preferred_element_type=jnp.float32)
            * scale
        )
        visible = k_pos[:, None, None, :] <= q_pos[:, None, :, None]
        probs = jnp.where(visible, jnp.exp(scores - log_total[..., None]), 0.0)
        d_probs = jnp.einsum(
            "sqhd,skhd->shqk", d_heads_bf, val_piece, preferred_element_type=jnp.float32
        )
        d_scores = (probs * (d_probs - deltas[..., None])).astype(jnp.bfloat16)
        return (probs, d_scores)

    def query_span(step_index, acc):
        offset = step_index * total_span
        key_piece = lax.dynamic_slice_in_dim(key_all, offset, total_span, 1).reshape(
            seq_count, total_span, head_count, HD
        )
        val_piece = lax.dynamic_slice_in_dim(val_all, offset, total_span, 1).reshape(
            seq_count, total_span, head_count, HD
        )
        k_pos = key_positions(block_order, offset, total_span, block_len)
        probs, d_scores = grad_block(key_piece, val_piece, k_pos)
        return (
            acc
            + jnp.einsum("shqk,skhd->sqhd", d_scores, key_piece, preferred_element_type=jnp.float32)
            * scale
        )

    d_qrot = lax.fori_loop(
        0,
        total_len // total_span,
        query_span,
        jnp.zeros((seq_count, block_len, head_count, HD), jnp.float32),
    )
    count = block_len * lax.axis_size("ctx")
    key_span = span_of()

    def key_one_span(step_index, buffer):
        offset = step_index * key_span
        key_piece = lax.dynamic_slice_in_dim(key_all, offset, key_span, 1).reshape(
            seq_count, key_span, head_count, HD
        )
        val_piece = lax.dynamic_slice_in_dim(val_all, offset, key_span, 1).reshape(
            seq_count, key_span, head_count, HD
        )
        k_pos = key_positions(block_order, offset, key_span, block_len)
        probs, d_scores = grad_block(key_piece, val_piece, k_pos)
        d_keyp = (
            jnp.einsum("shqk,sqhd->skhd", d_scores, q_rot, preferred_element_type=jnp.float32)
            * scale
        )
        d_valp = jnp.einsum(
            "shqk,sqhd->skhd",
            probs.astype(jnp.bfloat16),
            d_heads_bf,
            preferred_element_type=jnp.float32,
        )
        both = jnp.concatenate(
            [
                d_keyp.reshape(seq_count, key_span, head_width),
                d_valp.reshape(seq_count, key_span, head_width),
            ],
            axis=2,
        )
        return lax.dynamic_update_slice_in_dim(buffer, both.transpose(1, 0, 2), offset, 0)

    key_sums = (
        lax.psum_scatter(
            lax.fori_loop(
                0,
                count // key_span,
                key_one_span,
                jnp.zeros((count, seq_count, 2 * head_width), jnp.float32),
            ).astype(jnp.bfloat16),
            "ctx",
            scatter_dimension=0,
            tiled=True,
        )
        .astype(jnp.float32)
        .transpose(1, 0, 2)
    )
    d_krot = key_sums[..., :head_width].reshape(seq_count, block_len, head_count, HD)
    d_values = key_sums[..., head_width:].reshape(row_count, head_width)
    dq_normed = unrotate(d_qrot, cosine, sine).reshape(row_count, head_width)
    dk_normed = unrotate(d_krot, cosine, sine).reshape(row_count, head_width)
    q_dots, k_dots = tp_total(
        (
            jnp.sum(g_query * dq_normed * queries, axis=1),
            jnp.sum(g_key * dk_normed * keys_raw, axis=1),
        )
    )
    d_queries = (
        q_inverse * (g_query * dq_normed) - queries * q_inverse**3 * (q_dots / width)[:, None]
    )
    d_keys = k_inverse * (g_key * dk_normed) - keys_raw * k_inverse**3 * (k_dots / width)[:, None]
    d_gquery = jnp.sum(dq_normed * queries * q_inverse, axis=0)
    d_gkey = jnp.sum(dk_normed * keys_raw * k_inverse, axis=0)
    dq_bf = d_queries.astype(jnp.bfloat16)
    dk_bf = d_keys.astype(jnp.bfloat16)
    dv_bf = d_values.astype(jnp.bfloat16)
    grad_q = jnp.dot(tok_rows.T, dq_bf, preferred_element_type=jnp.float32)
    grad_k = jnp.dot(tok_rows.T, dk_bf, preferred_element_type=jnp.float32)
    grad_v = jnp.dot(tok_rows.T, dv_bf, preferred_element_type=jnp.float32)
    back_attn = (
        jnp.dot(dq_bf, wq_full.T, preferred_element_type=jnp.float32)
        + jnp.dot(dk_bf, wk_full.T, preferred_element_type=jnp.float32)
        + jnp.dot(dv_bf, wv_full.T, preferred_element_type=jnp.float32)
    )
    grad_input = d_hidden + share(back_attn.reshape(seq_count, block_len, -1))
    summed = (
        lax.psum_scatter(
            grad_q.astype(jnp.bfloat16), "ctx", scatter_dimension=0, tiled=True
        ).astype(jnp.float32),
        lax.psum_scatter(
            grad_k.astype(jnp.bfloat16), "ctx", scatter_dimension=0, tiled=True
        ).astype(jnp.float32),
        lax.psum_scatter(
            grad_v.astype(jnp.bfloat16), "ctx", scatter_dimension=0, tiled=True
        ).astype(jnp.float32),
        lax.psum_scatter(
            grad_outproj.astype(jnp.bfloat16), "ctx", scatter_dimension=1, tiled=True
        ).astype(jnp.float32),
        lax.psum_scatter(
            grad_gate.astype(jnp.bfloat16), "ctx", scatter_dimension=0, tiled=True
        ).astype(jnp.float32),
        lax.psum_scatter(
            grad_up.astype(jnp.bfloat16), "ctx", scatter_dimension=0, tiled=True
        ).astype(jnp.float32),
        lax.psum_scatter(
            grad_down.astype(jnp.bfloat16), "ctx", scatter_dimension=1, tiled=True
        ).astype(jnp.float32),
        lax.psum_scatter(
            d_gquery.astype(jnp.bfloat16), "ctx", scatter_dimension=0, tiled=True
        ).astype(jnp.float32),
        lax.psum_scatter(
            d_gkey.astype(jnp.bfloat16), "ctx", scatter_dimension=0, tiled=True
        ).astype(jnp.float32),
        lax.psum_scatter(
            d_gattn.astype(jnp.bfloat16), "ctx", scatter_dimension=0, tiled=True
        ).astype(jnp.float32),
        lax.psum_scatter(
            d_gfeed.astype(jnp.bfloat16), "ctx", scatter_dimension=0, tiled=True
        ).astype(jnp.float32),
    )
    return (
        output,
        grad_input,
        summed[0],
        summed[1],
        summed[2],
        summed[3],
        summed[4],
        summed[5],
        summed[6],
        summed[7],
        summed[8],
        summed[9],
        summed[10],
    )


MESH = pl.DeviceIdType.MESH
NT = (((1,), (1,)), ((), ()))
TN = (((0,), (0,)), ((), ()))
F32 = jnp.float32
BF16 = jnp.bfloat16
COLS = (0, 1, 2, 4, 5)


def layer_kernel(dims, *refs):
    (chips, tps, seqs, blk, width, head_w, ff_w) = dims
    rows = seqs * blk
    both = 2 * rows
    share_rows = rows // tps
    feats = width // tps
    heads = head_w // HD
    slab = width // (2 * chips)
    halves = (head_w, head_w, head_w, head_w, ff_w, ff_w, ff_w)
    total = 2 * chips * blk
    scale = HD ** (-0.5)
    it = iter(refs)

    def take(n):
        return [next(it) for _ in range(n)]

    (tok_in, cot_in) = take(2)
    w_in = take(7)
    (blocks, *gains, table) = take(6)
    (out_ref, gin_ref, ggain_ref) = take(3)
    rx_g = take(7)
    summed = take(4)
    w = take(7)
    via = take(7)
    (tok, tok_t, hid, hid_t, dmix, dattn) = take(6)
    (lin, fac, act, act_t, dgate, dup) = take(6)
    (st_p, rx_p, st_z, rx_z, rx_f) = take(5)
    (q_raw, k_raw, qkv, qa, probs, att_f, att_st, att, att_t) = take(9)
    (dh, d_o, dqkv_st, dqkv) = take(4)
    (sq_own, sq_rx, inv_q, inv_k) = take(4)
    (cot, proj, hstate, dhid, stage) = take(5)
    (gbuf, gall, gfull, gqk, gg_row, gg_rx1, gg_mid, gg_rx2) = take(8)
    (ws, wr, gs, gr) = take(4)
    (zs, zr, ps, pr) = take(4)
    (rps, rpr, rzs, rzr) = take(4)
    (ms, mr) = take(2)
    (ss, sr) = take(2)
    (as_, ar) = take(2)
    (loc,) = take(1)
    (d_acc, cosf, sinf, pos_row, gtile) = take(5)
    (xs, xr) = take(2)

    ctx = lax.axis_index("ctx")
    z = lax.axis_index("tp")
    c = ctx // 2
    k = ctx % 2
    ok = 1 - k
    partner = c * 2 + ok
    near = (c + 1 - 2 * (c % 2), (c + 2) % chips)
    far = chips - 1 - c

    def zp(i):
        return (z + i) % tps

    def chip(i):
        return (c + i) % chips

    def ds(start, size):
        return pl.ds(pl.multiple_of(start, size), size)

    def remote(src, dst, ssem, rsem, to_ctx, to_z):
        return pltpu.make_async_remote_copy(
            src_ref=src,
            dst_ref=dst,
            send_sem=ssem,
            recv_sem=rsem,
            device_id=(to_ctx, to_z),
            device_id_type=MESH,
        )

    peers = [(chip(i) * 2 + (k + d) % 2, z) for i in range(chips) for d in range(2) if i or d]
    peers += [(ctx, zp(i)) for i in range(1, tps)]
    peers += [(partner, zp(i)) for i in range(1, tps)]
    barrier = pltpu.get_barrier_semaphore()
    for peer in peers:
        pl.semaphore_signal(barrier, inc=1, device_id=peer, device_id_type=MESH)

    def go(copy):
        copy.start()
        return copy

    def sent(ref, sem):
        remote(ref, ref, sem, sem, partner, z).wait_send()

    def came(ref, sem):
        remote(ref, ref, sem, sem, partner, z).wait_recv()

    def slab_of(m, owner):
        if m in COLS:
            return w[m].at[ds(owner * slab, slab), :]
        return w[m].at[:, ds(owner * slab, slab)]

    def slabs(m, count):
        return w[m].at[0 : count * slab, :] if m in COLS else w[m].at[:, 0 : count * slab]

    def half_of(m, core):
        if m in COLS:
            return w_in[m].at[:, ds(core * halves[m], halves[m])]
        return w_in[m].at[ds(core * halves[m], halves[m]), :]

    w_own = {}
    w_wait = {}

    def send_w(m, d):
        core = (k + d) % 2
        for n in range(2):
            go(remote(half_of(m, core), slab_of(m, ctx), ws.at[m, 0], wr.at[m, 2 * n + k], near[n] * 2 + core, z))
        if d:
            go(remote(half_of(m, ok), slab_of(m, ctx), ws.at[m, 0], wr.at[m, 4], partner, z))
        else:
            w_own[m] = pltpu.make_async_copy(half_of(m, k), slab_of(m, ctx), loc.at[m])
            w_own[m].start()

    def source(n):
        if n < 4:
            return near[n // 2] * 2 + n % 2
        return partner if n == 4 else far * 2 + n - 5

    def got_w(m, *which):
        for n in which:
            if (m, n) not in w_wait:
                w_wait[m, n] = True
                came(slabs(m, 1), wr.at[m, n])

    def pass_w(m):
        for n in range(2):
            got_w(m, 3 * n)
            mine = slab_of(m, source(3 * n))
            go(remote(mine, mine, ws.at[m, 1], wr.at[m, 5 + n], near[1 - n] * 2 + k, z))

    def free_w(m):
        sent(slabs(m, 2), ws.at[m, 1])

    def wait_w(m):
        w_own[m].wait()
        got_w(m, *range(7))

    def into(m, n, core):
        if m in COLS:
            return rx_g[m].at[n, :, ds(core * halves[m], halves[m])]
        return rx_g[m].at[n, ds(core * halves[m], halves[m]), :]

    g_own = {}

    def send_far(m):
        for n in range(2):
            go(remote(slab_of(m, far * 2 + n), via[m].at[n], gs.at[m], gr.at[m, n], near[n] * 2 + k, z))

    def send_near(m, n):
        go(remote(slab_of(m, near[n] * 2 + n), into(m, 1 + n, k), gs.at[m], gr.at[m, 2], near[n] * 2 + n, z))

    def send_home(m):
        go(remote(slab_of(m, partner), into(m, 0, k), gs.at[m], gr.at[m, 2], partner, z))
        copy = pltpu.make_async_copy(slab_of(m, ctx), into(m, 0, k), loc.at[8 + m])
        copy.start()
        g_own[m] = copy

    def send_g(m):
        send_far(m)
        send_near(m, 0)
        send_near(m, 1)
        send_home(m)

    def pass_g(m):
        for n in range(2):
            to = near[1 - n] * 2 + n
            came(via[m].at[n], gr.at[m, n])
            total = slab_of(m, to)[...].astype(F32) + via[m][n].astype(F32)
            slab_of(m, to)[...] = total.astype(BF16)
            go(remote(slab_of(m, to), into(m, 2 - n, k), gs.at[m], gr.at[m, 2], to, z))

    def wait_g(m):
        g_own[m].wait()
        came(slabs(m, 5), gr.at[m, 2])

    def add_up(m):
        wait_g(m)
        if m in COLS:
            n = slab
            parts = (hid.at[0:n, :], hid.at[n : 2 * n, :], dmix.at[0:n, :], dmix.at[n : 2 * n, :])
        else:
            n = 2 * halves[m]
            parts = (hid_t.at[0:n, 0:slab], hid_t.at[0:n, slab : 2 * slab], tok_t.at[0:n, 0:slab], tok_t.at[0:n, slab : 2 * slab])
        loads = [pltpu.make_async_copy(rx_g[m].at[i], parts[i], loc.at[i]) for i in range(3)]
        for copy in loads:
            copy.start()
        for copy in loads:
            copy.wait()

        def add_step(j, carry):
            here = (slice(None), ds(j * 256, 256)) if m in COLS else (ds(j * 256, 256), slice(None))
            value = parts[0][here].astype(F32) + parts[1][here].astype(F32) + parts[2][here].astype(F32)
            parts[3][here] = value.astype(BF16)
            return carry

        lax.fori_loop(0, 2 * halves[m] // 256, add_step, 0)
        copy = pltpu.make_async_copy(parts[3], summed[m - 3], loc.at[3])
        copy.start()
        copy.wait()

    lane = lax.broadcasted_iota(jnp.int32, (blk, HD), 1)
    gtile[...] = jnp.zeros((8, 128), F32)
    for r in range(4):
        value = gains[r][...].astype(F32)
        value = jnp.concatenate([value, value], axis=1)
        gtile[r : r + 1, :] = jnp.where(lane[0:1, :] // 64 == k, value, 0.0)
    own_tok = pltpu.make_async_copy(tok_in, tok.at[ds(k * rows, rows), ds(z * feats, feats)], loc.at[16])
    own_tok.start()
    own_cot = pltpu.make_async_copy(cot_in.at[ds(z * share_rows, share_rows), :], cot.at[:, ds(z * feats, feats)], loc.at[17])
    own_cot.start()
    pl.semaphore_wait(barrier, len(peers))
    own_gain = pltpu.make_async_copy(gtile, gbuf.at[ctx], loc.at[18])
    own_gain.start()

    for i in range(1, tps):
        go(remote(tok_in, tok.at[ds(k * rows, rows), ds(z * feats, feats)], zs.at[0], zr.at[0, i - 1], ctx, zp(i)))
    go(remote(tok_in, tok.at[ds(k * rows, rows), ds(z * feats, feats)], ps.at[0], pr.at[0], partner, z))
    slots = [(i, d) for i in range(chips) for d in range(2)]
    for i, d in slots:
        if i or d:
            go(remote(gtile, gbuf.at[ctx], ms.at[0], mr.at[0], chip(i) * 2 + (k + d) % 2, z))
    for i in range(1, tps):
        go(remote(cot_in.at[ds(zp(i) * share_rows, share_rows), :], cot.at[:, ds(z * feats, feats)], ms.at[1], mr.at[1], ctx, zp(i)))
    for m in (0, 1, 2, 3):
        send_w(m, 0)
        send_w(m, 1)

    own_gain.wait()
    came(gbuf.at[0 : 2 * chips - 1], mr.at[0])
    own_gain2 = pltpu.make_async_copy(gbuf, gall.at[z], loc.at[19])
    own_gain2.start()
    for i in range(1, tps):
        go(remote(gbuf, gall.at[z], ms.at[2], mr.at[2], ctx, zp(i)))
    for r in range(2):
        pieces = [gbuf[4 * k + 2 * m, r : r + 1, :] + gbuf[4 * k + 2 * m + 1, r : r + 1, :] for m in range(head_w // 128)]
        gqk[r : r + 1, :] = jnp.concatenate(pieces, axis=1)

    sign = jnp.where(lane < HD // 2, -1.0, 1.0)
    for core in range(2):
        for s in range(seqs):
            block = blocks[s, 2 * c + core]
            c_block, s_block = table[0, pl.ds(block, 1), :], table[1, pl.ds(block, 1), :]
            c_in, s_in = table[2], table[3]
            here = slice((core * seqs + s) * blk, (core * seqs + s + 1) * blk)
            cosf[here, :] = c_block * c_in - s_block * s_in
            sinf[here, :] = (s_block * c_in + c_block * s_in) * sign
    for j in range(2 * chips):
        start = blocks[c // heads, j] * blk
        here = slice(j * blk, (j + 1) * blk)
        pos_row[:, here] = start + lane[0:8, :]

    own_tok.wait()
    pass_w(0)
    for i in range(1, tps):
        pass_w(i)
        if i == tps - 1:
            send_w(4, 0)
        came(tok.at[0:rows, 0:feats], zr.at[0, i - 1])
        part = tok.at[ds(k * rows, rows), ds(((z - i) % tps) * feats, feats)]
        go(remote(part, part, ps.at[0], pr.at[0], partner, z))
    came(tok.at[0:rows, :], pr.at[0])

    def row_of(value):
        folded = value[:, :128]
        for h in range(1, heads):
            folded = folded + value[:, h * 128 : (h + 1) * 128]
        return jnp.sum(jnp.transpose(folded), axis=0, keepdims=True)

    def column_of(row):
        return jnp.transpose(jnp.broadcast_to(row, (128, both)))

    def totals(idx):
        n = 0
        for i in range(tps):
            for d in range(2):
                if i or d:
                    to = ctx if d == 0 else partner
                    go(remote(sq_own.at[idx], sq_rx.at[idx, n], ss.at[idx], sr.at[idx], to, zp(i)))
                    n += 1
        came(sq_rx.at[idx], sr.at[idx])
        total = sq_own[idx]
        for j in range(n):
            total = total + sq_rx[idx, j]
        return total

    for m in (0, 1, 2):
        wait_w(m)
        value = jnp.dot(tok[...], w[m][...], preferred_element_type=F32)
        if m == 0:
            q_raw[...] = value
            sq_own[0, 0:1, :] = row_of(value * value)
        elif m == 1:
            k_raw[...] = value
            sq_own[0, 1:2, :] = row_of(value * value)
        else:
            qkv[2] = value.astype(BF16).reshape(2, seqs, blk, head_w)
    sq_own[0, 2:8, :] = jnp.zeros((6, both), F32)
    squares = totals(0)
    inverse = lax.rsqrt(squares / width + EPS)
    inv_q[...] = column_of(inverse[0:1, :])
    inv_k[...] = column_of(inverse[1:2, :])
    for t, (raw, inv) in enumerate(((q_raw, inv_q), (k_raw, inv_k))):
        for h in range(heads):
            lanes = slice(h * HD, (h + 1) * HD)
            normed = raw[:, lanes] * inv[...] * gqk[t : t + 1, lanes]
            turned = normed * cosf[...] + pltpu.roll(normed, HD // 2, 1) * sinf[...]
            qkv[t, :, :, :, lanes] = turned.astype(BF16).reshape(2, seqs, blk, HD)

    def to_owner(idx, value, owned, stacked):
        size = owned.at[:, 0 : 2 * chips - 2] if stacked else owned.at[0 : 2 * chips - 2]
        for i in range(chips):
            to = chip(i)
            s, h = to // heads, to % heads
            if stacked:
                src = value.at[:, :, s, :, ds(h * HD, HD)]
                dst = owned.at[:, ds(2 * c, 2)]
            else:
                src = value.at[:, s, :, ds(h * HD, HD)]
                dst = owned.at[ds(2 * c, 2)]
            if i:
                go(remote(src, dst, as_.at[idx], ar.at[idx], to * 2 + k, z))
            else:
                own = pltpu.make_async_copy(src, dst, loc.at[20 + idx])
                own.start()
        return own, size, idx

    def from_owner(idx, owned, value, stacked):
        size = owned.at[:, 0 : 2 * chips - 2] if stacked else owned.at[0 : 2 * chips - 2]
        s, h = c // heads, c % heads
        for i in range(chips):
            to = chip(i)
            if stacked:
                src = owned.at[:, ds(2 * to, 2)]
                dst = value.at[:, :, s, :, ds(h * HD, HD)]
            else:
                src = owned.at[ds(2 * to, 2)]
                dst = value.at[:, s, :, ds(h * HD, HD)]
            if i:
                go(remote(src, dst, as_.at[idx], ar.at[idx], to * 2 + k, z))
            else:
                own = pltpu.make_async_copy(src, dst, loc.at[20 + idx])
                own.start()
        return own, size, idx

    def arrive(pair):
        own, size, idx = pair
        own.wait()
        came(size, ar.at[idx])
        sent(size, as_.at[idx])

    pair = to_owner(0, qkv, qa, True)
    send_w(4, 1)
    arrive(pair)
    step = 2 * blk

    def attend(i, carry):
        here = ds(i * step, step)
        q = qa[0, pl.ds(2 * i, 2)].reshape(step, HD)
        s = lax.dot_general(q, qa[1].reshape(total, HD), NT, preferred_element_type=F32) * scale
        at = lax.broadcasted_iota(jnp.int32, (step, 1), 0)
        first = blocks[c // heads, 2 * i] * blk
        second = (blocks[c // heads, 2 * i + 1] - 1) * blk
        visible = pos_row[0:1, :] <= at + jnp.where(at < blk, first, second)
        s = jnp.where(visible, s, NEGATIVE)
        top = jnp.max(s, axis=1, keepdims=True)
        e = jnp.where(visible, jnp.exp(s - top), 0.0)
        p = (e * (1.0 / jnp.sum(e, axis=1, keepdims=True))).astype(BF16)
        probs[here, :] = p
        o = jnp.dot(p, qa[2].reshape(total, HD), preferred_element_type=F32)
        att_f[here, :] = o
        att_st[pl.ds(2 * i, 2)] = o.astype(BF16).reshape(2, blk, HD)
        return carry

    lax.fori_loop(0, chips, attend, 0)
    back = from_owner(1, att_st, att, False)
    pass_w(4)
    send_w(5, 0)
    send_w(5, 1)
    send_w(6, 0)
    own_gain2.wait()
    came(gall.at[0 : tps - 1], mr.at[2])
    for r in range(2):
        pieces = []
        for zz in range(tps):
            for m in range(chips):
                pieces.append(gall[zz, 2 * m, 2 + r : 3 + r, :] + gall[zz, 2 * m + 1, 2 + r : 3 + r, :])
        gfull[r : r + 1, :] = jnp.concatenate(pieces, axis=1)
    for s in range(width // 256):
        tok_t[s * 256 : (s + 1) * 256, :] = jnp.transpose(tok[:, s * 256 : (s + 1) * 256])
    arrive(back)
    wait_w(3)

    cw = feats
    rs_live = {}

    def rp_copy(idx, i, off):
        return remote(st_p.at[:, ds(off, cw)], rx_p.at[idx % 2, :, ds(off, cw)], rps.at[idx], rpr.at[idx, i], partner, z)

    def rz_copy(idx, i, j, off):
        return remote(
            st_z.at[ds(zp(j) * share_rows, share_rows), ds(off, cw)],
            rx_z.at[idx % 2, j - 1, :, ds(off, cw)],
            rzs.at[idx],
            rzr.at[idx],
            ctx,
            zp(j),
        )

    def reduce_rows(idx, partial, offset, before=None, meanwhile=None):
        def one(i):
            off = offset(i)
            if before is not None:
                before(i)
            st_p[:, ds(off, cw)] = partial(ok, off).astype(BF16)
            rp_copy(idx, i, off).start()
            mine = partial(k, off)
            rp_copy(idx, i, off).wait_recv()
            st_z[:, ds(off, cw)] = (mine + rx_p[idx % 2, :, ds(off, cw)].astype(F32)).astype(BF16)
            for j in range(1, tps):
                rz_copy(idx, i, j, off).start()

        if before is None:
            lax.fori_loop(0, tps, lambda i, x: (one(i), x)[1], 0)
        else:
            for i in range(tps):
                one(i)
        if meanwhile is not None:
            meanwhile()
        came(rx_z.at[idx % 2], rzr.at[idx])
        sent(rx_z.at[idx % 2], rzs.at[idx])
        sent(st_p, rps.at[idx])
        mine = st_z[ds(z * share_rows, share_rows), :].astype(F32)
        for j in range(tps - 1):
            mine = mine + rx_z[idx % 2, j].astype(F32)
        return mine

    def straight(i):
        return i * cw

    def mean_of(value):
        return jnp.sum(value, axis=1, keepdims=True) / width

    def spread(idx, buf):
        mine = buf.at[ds(k * rows + z * share_rows, share_rows), :]
        for i in range(1, tps):
            go(remote(mine, mine, zs.at[idx], zr.at[idx, i - 1], ctx, zp(i)))
        go(remote(mine, mine, ps.at[idx], pr.at[idx], partner, z))

        def finish(meanwhile=None):
            for i in range(1, tps):
                came(buf.at[0:share_rows, :], zr.at[idx, i - 1])
                if i == 1 and meanwhile is not None:
                    meanwhile()
                part = buf.at[ds(k * rows + ((z - i) % tps) * share_rows, share_rows), :]
                go(remote(part, part, ps.at[idx], pr.at[idx], partner, z))
            came(buf.at[0:rows, :], pr.at[idx])
            sent(buf.at[0 : (tps - 1) * share_rows, :], zs.at[idx])
            sent(buf.at[0:rows, :], ps.at[idx])

        return finish

    my_rows = ds(k * rows + z * share_rows, share_rows)
    heads_rows = [None]

    def o_partial(core, off):
        left = att[pl.ds(core, 1)].reshape(rows, head_w)
        return jnp.dot(left, w[3][:, ds(off, cw)], preferred_element_type=F32)

    value = reduce_rows(0, o_partial, straight)
    proj[...] = value
    a_inverse = lax.rsqrt(mean_of(value * value) + EPS)
    state = tok[my_rows, :].astype(F32) + value * a_inverse * gfull[0:1, :]
    hstate[...] = state
    hid[my_rows, :] = state.astype(BF16)
    finish = spread(1, hid)
    own_cot.wait()
    came(cot.at[:, 0 : (tps - 1) * feats], mr.at[1])
    att_t[...] = jnp.transpose(att[...].reshape(both, head_w))

    def more_weights():
        pass_w(5)
        send_w(6, 1)

    finish(more_weights)

    fw = 256
    wait_w(4)

    def gate_step(j, carry):
        here = ds(j * fw, fw)
        lin[:, here] = jnp.dot(hid[...], w[4][:, here], preferred_element_type=F32)
        return carry

    lax.fori_loop(0, ff_w // fw, gate_step, 0)
    for s in range(width // 256):
        hid_t[s * 256 : (s + 1) * 256, :] = jnp.transpose(hid[:, s * 256 : (s + 1) * 256])
    wait_w(5)

    def up_step(j, carry):
        here = ds(j * fw, fw)
        up = jnp.dot(hid[...], w[5][:, here], preferred_element_type=F32)
        gate = lin[:, here]
        sigma = jax.nn.sigmoid(gate)
        swish = gate * sigma
        lin[:, here] = swish
        fac[:, here] = up * sigma * (1.0 + gate * (1.0 - sigma))
        value = (swish * up).astype(BF16)
        act[:, here] = value
        act_t[here, :] = jnp.transpose(value)
        return carry

    lax.fori_loop(0, ff_w // fw, up_step, 0)

    def down_partial(core, off):
        return jnp.dot(act[ds(core * rows, rows), :], w[6][:, ds(off, cw)], preferred_element_type=F32)

    def from_chip(i):
        return (c, near[0], near[1], far)[i] * cw

    def down_ready(i):
        if i == 0:
            w_own[6].wait()
            pass_w(6)
        got_w(6, *((4,), (0, 1), (2, 3), (5, 6))[i])

    value = reduce_rows(1, down_partial, from_chip, down_ready)
    m_inverse = lax.rsqrt(mean_of(value * value) + EPS)
    scaled = value * m_inverse
    upstream = cot[...].astype(F32)
    gained = upstream * gfull[1:2, :]
    back_mix = m_inverse * gained - scaled * (m_inverse * m_inverse) * mean_of(gained * value)
    dmix[my_rows, :] = back_mix.astype(BF16)
    order = (far, near[0], near[1], c)

    def mix_along(n, i):
        here = dmix.at[my_rows, ds(order[n] * cw, cw)]
        return remote(here, here, xs.at[n], xr.at[n], ctx, zp(i))

    def mix_across(n, i):
        owner = (z - i) % tps
        here = dmix.at[ds(k * rows + owner * share_rows, share_rows), ds(order[n] * cw, cw)]
        return remote(here, here, xs.at[chips], xr.at[chips + n], partner, z)

    def mix_start(n):
        for i in range(1, tps):
            mix_along(n, i).start()
        mix_across(n, 0).start()

    mix_start(0)
    gg_row[1:2, :] = jnp.sum(upstream * scaled, axis=0, keepdims=True)
    stage[...] = hstate[...] + scaled * gfull[1:2, :]

    free_w(6)
    for n in range(chips):
        sent(dmix.at[0:share_rows, 0 : (tps - 1) * cw], xs.at[n])
        if n < chips - 1:
            mix_start(n + 1)
        came(dmix.at[0:share_rows, 0 : (tps - 1) * cw], xr.at[n])
        for i in range(1, tps):
            mix_across(n, i).start()
        came(dmix.at[0:rows, 0:cw], xr.at[chips + n])
        off = order[n] * cw

        def dact_step(j, carry):
            here = ds(j * fw, fw)
            d_act = lax.dot_general(dmix[:, ds(off, cw)], w[6][here, ds(off, cw)], NT, preferred_element_type=F32)
            part = (ds((j // 2) * both, both), ds((j % 2) * fw, fw))
            if n:
                d_act = d_act + d_acc[part]
            if n < chips - 1:
                d_acc[part] = d_act
            else:
                dup[:, here] = (d_act * lin[:, here]).astype(BF16)
                dgate[:, here] = (d_act * fac[:, here]).astype(BF16)
            return carry

        lax.fori_loop(0, ff_w // fw, dact_step, 0)
        grad = jnp.dot(act_t[...], dmix[:, ds(off, cw)], preferred_element_type=F32)
        w[6][:, ds(off, cw)] = grad.astype(BF16)
        if n == 0:
            send_far(6)
        elif n < chips - 1:
            send_near(6, n - 1)
        else:
            send_home(6)

    sent(dmix.at[0:rows, :], xs.at[chips])
    for i in range(1, tps):
        go(remote(stage.at[:, ds(zp(i) * feats, feats)], out_ref.at[ds(z * share_rows, share_rows), :], ms.at[3], mr.at[3], ctx, zp(i)))
    own_out = pltpu.make_async_copy(stage.at[:, ds(z * feats, feats)], out_ref.at[ds(z * share_rows, share_rows), :], loc.at[24])
    own_out.start()

    def ff_partial(core, off):
        here = ds(core * rows, rows)
        return lax.dot_general(dgate[here, :], w[4][ds(off, cw), :], NT, preferred_element_type=F32) + lax.dot_general(
            dup[here, :], w[5][ds(off, cw), :], NT, preferred_element_type=F32
        )

    def ggate_step(j, carry):
        here = ds(j * fw, fw)
        w[4][:, here] = jnp.dot(hid_t[...], dgate[:, here], preferred_element_type=F32).astype(BF16)
        return carry

    def gup_step(j, carry):
        here = ds(j * fw, fw)
        w[5][:, here] = jnp.dot(hid_t[...], dup[:, here], preferred_element_type=F32).astype(BF16)
        return carry

    def gate_grad():
        free_w(4)
        lax.fori_loop(0, ff_w // fw, ggate_step, 0)
        send_g(4)
        free_w(5)
        lax.fori_loop(0, ff_w // fw, gup_step, 0)
        send_far(5)

    pass_g(6)
    value = reduce_rows(2, ff_partial, straight, meanwhile=gate_grad) + cot[...].astype(F32)
    dhid[...] = value
    projected = proj[...]
    a_inverse = lax.rsqrt(mean_of(projected * projected) + EPS)
    scaled = projected * a_inverse
    gained = value * gfull[0:1, :]
    gg_row[0:1, :] = jnp.sum(value * scaled, axis=0, keepdims=True)
    gg_row[2:8, :] = jnp.zeros((6, width), F32)
    back_att = a_inverse * gained - scaled * (a_inverse * a_inverse) * mean_of(gained * projected)
    dattn[my_rows, :] = back_att.astype(BF16)
    finish = spread(3, dattn)
    for i in range(1, tps):
        go(remote(gg_row.at[:, ds(zp(i) * feats, feats)], gg_rx1.at[i - 1], ms.at[4], mr.at[4], ctx, zp(i)))

    finish(lambda: pass_g(4))

    value = lax.dot_general(dattn[...], w[3][...], NT, preferred_element_type=F32)
    dh[...] = value.astype(BF16).reshape(2, seqs, blk, head_w)
    pair = to_owner(2, dh, d_o, False)
    send_near(5, 0)
    send_near(5, 1)
    send_home(5)

    def go_step(j, carry):
        here = ds(j * fw, fw)
        w[3][:, here] = jnp.dot(att_t[...], dattn[:, here], preferred_element_type=F32).astype(BF16)
        return carry

    free_w(3)
    lax.fori_loop(0, width // fw, go_step, 0)
    arrive(pair)
    dk_acc, dv_acc = d_acc.at[:, 0:HD], d_acc.at[:, HD : 2 * HD]
    dk_acc[...] = jnp.zeros((total, HD), F32)
    dv_acc[...] = jnp.zeros((total, HD), F32)

    def unattend(i, carry):
        here = ds(i * step, step)
        q = qa[0, pl.ds(2 * i, 2)].reshape(step, HD)
        d_out = d_o[pl.ds(2 * i, 2)].reshape(step, HD)
        d_p = lax.dot_general(d_out, qa[2].reshape(total, HD), NT, preferred_element_type=F32)
        delta = jnp.sum(d_out.astype(F32) * att_f[here, :], axis=1, keepdims=True)
        p = probs[here, :]
        d_s = (p.astype(F32) * (d_p - delta)).astype(BF16)
        d_q = jnp.dot(d_s, qa[1].reshape(total, HD), preferred_element_type=F32) * scale
        dqkv_st[0, pl.ds(2 * i, 2)] = d_q.astype(BF16).reshape(2, blk, HD)
        dk_acc[...] += lax.dot_general(d_s, q, TN, preferred_element_type=F32)
        dv_acc[...] += lax.dot_general(p, d_out, TN, preferred_element_type=F32)
        return carry

    lax.fori_loop(0, chips, unattend, 0)
    dqkv_st[1] = (dk_acc[...] * scale).astype(BF16).reshape(2 * chips, blk, HD)
    dqkv_st[2] = dv_acc[...].astype(BF16).reshape(2 * chips, blk, HD)
    pair = from_owner(3, dqkv_st, dqkv, True)

    pass_g(5)
    send_g(3)
    arrive(pair)

    gg_mid[...] = jnp.zeros((8, feats), F32)
    for t, (raw, inv) in enumerate(((q_raw, inv_q), (k_raw, inv_k))):
        folded = None
        for h in range(heads):
            lanes = slice(h * HD, (h + 1) * HD)
            turned = dqkv[t, :, :, :, lanes].reshape(both, HD).astype(F32)
            back_rot = turned * cosf[...] - pltpu.roll(turned, HD // 2, 1) * sinf[...]
            plain = raw[:, lanes]
            scaled = plain * inv[...]
            gg_mid[2 + t : 3 + t, pl.ds(pl.multiple_of(k * head_w + h * HD, HD), HD)] = jnp.sum(back_rot * scaled, axis=0, keepdims=True)
            gained = back_rot * gqk[t : t + 1, lanes]
            dqkv[t, :, :, :, lanes] = gained.astype(BF16).reshape(2, seqs, blk, HD)
            term = gained * plain
            folded = term if folded is None else folded + term
        sq_own[1, t : t + 1, :] = jnp.sum(jnp.transpose(folded), axis=0, keepdims=True)
    sq_own[1, 2:8, :] = jnp.zeros((6, both), F32)
    dots = totals(1) / width
    for t, (raw, inv) in enumerate(((q_raw, inv_q), (k_raw, inv_k))):
        spread_dot = column_of(dots[t : t + 1, :])
        for h in range(heads):
            lanes = slice(h * HD, (h + 1) * HD)
            gained = dqkv[t, :, :, :, lanes].reshape(both, HD).astype(F32)
            r = inv[...]
            grad = r * gained - raw[:, lanes] * (r * r * r) * spread_dot
            dqkv[t, :, :, :, lanes] = grad.astype(BF16).reshape(2, seqs, blk, HD)

    def rf_copy(i, off):
        return remote(st_z.at[:, ds(off, cw)], rx_f.at[i], rzs.at[3], rzr.at[3], ctx, zp(i + 1))

    def in_partial(core, off):
        here = ds(off, cw)
        acc = None
        for t in range(3):
            left = dqkv[t, pl.ds(core, 1)].reshape(rows, head_w)
            term = lax.dot_general(left, w[t][here, :], NT, preferred_element_type=F32)
            acc = term if acc is None else acc + term
        return acc

    own_rows = ds(z * share_rows, share_rows)
    for i in range(tps):
        off = zp(i + 1) * cw
        st_p[:, ds(off, cw)] = in_partial(ok, off).astype(BF16)
        rp_copy(3, i, off).start()
        mine = in_partial(k, off)
        rp_copy(3, i, off).wait_recv()
        st_z[:, ds(off, cw)] = (mine + rx_p[1, :, ds(off, cw)].astype(F32)).astype(BF16)
        st_z[own_rows, ds(off, cw)] = (st_z[own_rows, ds(off, cw)].astype(F32) + dhid[:, ds(off, cw)]).astype(BF16)
        if i < tps - 1:
            rf_copy(i, off).start()

    pass_g(3)
    for m in range(3):

        def gqkv_step(j, carry):
            here = ds(j * 512, 512)
            right = dqkv[m].reshape(both, head_w)
            w[m][here, :] = jnp.dot(tok_t[here, :], right, preferred_element_type=F32).astype(BF16)
            return carry

        free_w(m)
        lax.fori_loop(0, width // 512, gqkv_step, 0)
        send_g(m)
    middle = gg_row[:, ds(z * feats, feats)]
    came(gg_rx1, mr.at[4])
    for i in range(tps - 1):
        middle = middle + gg_rx1[i]
    gg_mid[...] = gg_mid[...] + middle
    n = 0
    for i, d in slots:
        if i or d:
            core = (k + d) % 2
            go(remote(gg_mid.at[:, ds(chip(i) * 128, 128)], gg_rx2.at[n], ms.at[5], mr.at[5], chip(i) * 2 + core, z))
            n += 1

    add_up(6)
    add_up(4)
    for m in range(3):
        pass_g(m)
    add_up(3)
    add_up(5)
    came(rx_f, rzr.at[3])
    sent(rx_f, rzs.at[3])
    sent(st_p, rps.at[3])
    final = st_z[:, ds(z * feats, cw)].astype(F32)
    for i in range(tps - 1):
        final = final + rx_f[i].astype(F32)
    gin_ref[...] = final
    gain_sum = gg_mid[:, ds(c * 128, 128)]
    came(gg_rx2, mr.at[5])
    for i in range(2 * chips - 1):
        gain_sum = gain_sum + gg_rx2[i]
    ggain_ref[...] = jnp.where(k == 1, pltpu.roll(gain_sum, 64, 1), gain_sum)
    own_out.wait()
    came(stage.at[:, 0 : (tps - 1) * feats], mr.at[3])
    for m in range(3):
        wait_g(m)
    sent(tok.at[0:rows, 0 : (tps - 1) * feats], zs.at[0])
    sent(tok.at[0:rows, :], ps.at[0])
    sent(gbuf.at[0 : 2 * chips - 1], ms.at[0])
    sent(cot.at[:, 0 : (tps - 1) * feats], ms.at[1])
    sent(gall.at[0 : tps - 1], ms.at[2])
    sent(stage.at[:, 0 : (tps - 1) * feats], ms.at[3])
    sent(gg_rx1, ms.at[4])
    sent(gg_rx2, ms.at[5])
    for idx in range(2):
        sent(sq_rx.at[idx], ss.at[idx])
    for m in range(7):
        sent(slabs(m, 5), ws.at[m, 0])
        sent(slabs(m, 7), gs.at[m])


def fused(
    tokens,
    w_query,
    w_key,
    w_value,
    w_output,
    w_gate,
    w_up,
    w_down,
    gain_query,
    gain_key,
    gain_attention,
    gain_feedforward,
    block_order,
    cotangent,
):
    seqs, blk, feats = tokens.shape
    tps = lax.axis_size("tp")
    chips = lax.axis_size("ctx") // 2
    width = feats * tps
    rows = seqs * blk
    both = 2 * rows
    share_rows = rows // tps
    total = 2 * chips * blk
    head_w = w_query.shape[1] // 2
    ff_w = w_gate.shape[1] // 2
    heads = head_w // HD
    slab = width // (2 * chips)
    frequency = THETA ** (-2.0 * np.arange(HD // 2) / HD)
    frequency = np.concatenate([frequency, frequency])
    starts = np.zeros((blk, 1))
    starts[: 2 * chips, 0] = np.arange(2 * chips) * blk
    inside = np.arange(blk)[:, None] * 1.0
    table = np.stack([f(at * frequency) for at in (starts, inside) for f in (np.cos, np.sin)]).astype(np.float32)
    gains = [gain.reshape(1, -1) for gain in (gain_query, gain_key, gain_attention, gain_feedforward)]
    weights = (w_query, w_key, w_value, w_output, w_gate, w_up, w_down)
    dims = (chips, tps, seqs, blk, width, head_w, ff_w)
    halves = (head_w, head_w, head_w, head_w, ff_w, ff_w, ff_w)
    hbm = pl.BlockSpec(memory_space=pl.ANY)
    vmem = pl.BlockSpec(memory_space=pltpu.VMEM)

    def v(shape, dtype=BF16):
        return pltpu.VMEM(shape, dtype)

    w_shapes = [v((width, h)) if m in COLS else v((h, width)) for m, h in enumerate(halves)]
    dma = pltpu.SemaphoreType.DMA
    v_shapes = [v((2, slab, h)) if m in COLS else v((2, h, slab)) for m, h in enumerate(halves)]
    scratch = w_shapes + v_shapes + [
        v((both, width)),
        v((width, both)),
        v((both, width)),
        v((width, both)),
        v((both, width)),
        v((both, width)),
        v((both, ff_w), F32),
        v((both, ff_w), F32),
        v((both, ff_w)),
        v((ff_w, both)),
        v((both, ff_w)),
        v((both, ff_w)),
        v((rows, width)),
        v((2, rows, width)),
        v((rows, width)),
        v((2, tps - 1, share_rows, width)),
        v((tps - 1, rows, feats)),
        v((both, head_w), F32),
        v((both, head_w), F32),
        v((3, 2, seqs, blk, head_w)),
        v((3, 2 * chips, blk, HD)),
        v((total, total)),
        v((total, HD), F32),
        v((2 * chips, blk, HD)),
        v((2, seqs, blk, head_w)),
        v((head_w, both)),
        v((2, seqs, blk, head_w)),
        v((2 * chips, blk, HD)),
        v((3, 2 * chips, blk, HD)),
        v((3, 2, seqs, blk, head_w)),
        v((2, 8, both), F32),
        v((2, 2 * tps - 1, 8, both), F32),
        v((both, 128), F32),
        v((both, 128), F32),
        v((share_rows, width)),
        v((share_rows, width), F32),
        v((share_rows, width), F32),
        v((share_rows, width), F32),
        v((share_rows, width), F32),
        v((2 * chips, 8, 128), F32),
        v((tps, 2 * chips, 8, 128), F32),
        v((8, width), F32),
        v((8, head_w), F32),
        v((8, width), F32),
        v((tps - 1, 8, feats), F32),
        v((8, feats), F32),
        v((2 * chips - 1, 8, 128), F32),
        dma((7, 2)),
        dma((7, 7)),
        dma((7,)),
        dma((7, 3)),
        dma((4,)),
        dma((4, tps - 1)),
        dma((4,)),
        dma((4,)),
        dma((4,)),
        dma((4, tps)),
        dma((4,)),
        dma((4,)),
        dma((6,)),
        dma((6,)),
        dma((2,)),
        dma((2,)),
        dma((4,)),
        dma((4,)),
        dma((25,)),
        v((2 * both, ff_w // 2), F32),
        v((both, HD), F32),
        v((both, HD), F32),
        v((8, total), jnp.int32),
        v((8, 128), F32),
        dma((chips + 1,)),
        dma((2 * chips,)),
    ]
    results = pl.pallas_call(
        functools.partial(layer_kernel, dims),
        out_shape=[
            jax.ShapeDtypeStruct((rows, feats), F32),
            jax.ShapeDtypeStruct((rows, feats), F32),
            jax.ShapeDtypeStruct((8, 128), F32),
        ]
        + [jax.ShapeDtypeStruct((3,) + weight.shape, BF16) for weight in weights]
        + [jax.ShapeDtypeStruct(weight.shape, BF16) for weight in weights[3:]],
        in_specs=[hbm] * 9 + [pl.BlockSpec(memory_space=pltpu.SMEM)] + [vmem] * 5,
        out_specs=[hbm, vmem, vmem] + [hbm] * 11,
        scratch_shapes=scratch,
        compiler_params=pltpu.CompilerParams(
            collective_id=0, has_side_effects=True, vmem_limit_bytes=67043328
        ),
        name="layer",
    )(tokens.reshape(rows, feats), cotangent.reshape(rows, feats), *weights, block_order, *gains, table)
    steps = 8
    shapes = [value.shape for value in results[:2]] + [weight.shape for weight in weights]

    def rows_of(shape):
        return pl.BlockSpec((shape[0] // steps, shape[1]), lambda i: (i, 0))

    three = pl.BlockSpec((3, slab // steps, 2 * head_w), lambda i: (0, i, 0))
    whole = pl.BlockSpec((8, 128), lambda i: (0, 0))
    gain = pl.BlockSpec((1, 64), lambda i: (0, 0))
    wide = pl.pallas_call(
        widen_kernel,
        grid=(steps,),
        out_shape=[jax.ShapeDtypeStruct(shape, F32) for shape in shapes] + [jax.ShapeDtypeStruct((1, 64), F32)] * 4,
        in_specs=[rows_of(shapes[0])] * 2 + [three] * 3 + [rows_of(shape) for shape in shapes[5:]] + [whole],
        out_specs=[rows_of(shape) for shape in shapes] + [gain] * 4,
        name="widen",
    )(*results[:2], *results[3:6], *results[10:], results[2])
    output = wide[0].reshape(tokens.shape)
    grad_input = wide[1].reshape(tokens.shape)
    lanes = [value.reshape(64) for value in wide[9:]]
    return (output, grad_input, *wide[2:9], lanes[2], lanes[3], lanes[0], lanes[1])


def widen_kernel(*refs):
    given, made = refs[:10], refs[10:]
    for i in range(2):
        made[i][...] = given[i][...]
    for i in range(2, 5):
        made[i][...] = given[i][0].astype(F32) + given[i][1].astype(F32) + given[i][2].astype(F32)
    for i in range(5, 9):
        made[i][...] = given[i][...].astype(F32)
    for i in range(4):
        made[9 + i][...] = given[9][i : i + 1, 0:64]


def fits(mesh):
    return mesh.shape["ctx"] == 8 and mesh.shape["tp"] == 4


def solution(mesh):
    placed = (
        P(None, "ctx", "tp"),
        P("ctx", "tp"),
        P("ctx", "tp"),
        P("ctx", "tp"),
        P("tp", "ctx"),
        P("ctx", "tp"),
        P("ctx", "tp"),
        P("tp", "ctx"),
        P(("tp", "ctx")),
        P(("tp", "ctx")),
        P(("tp", "ctx")),
        P(("tp", "ctx")),
        P(),
        P(None, "ctx", "tp"),
    )
    return jax.shard_map(
        fused if fits(mesh) else shards,
        mesh=mesh,
        in_specs=placed,
        out_specs=(
            P(None, "ctx", "tp"),
            P(None, "ctx", "tp"),
            P("ctx", "tp"),
            P("ctx", "tp"),
            P("ctx", "tp"),
            P("tp", "ctx"),
            P("ctx", "tp"),
            P("ctx", "tp"),
            P("tp", "ctx"),
            P(("tp", "ctx")),
            P(("tp", "ctx")),
            P(("tp", "ctx")),
            P(("tp", "ctx")),
        ),
        check_vma=False,
    )
```

```python
import functools

import jax
import jax.numpy as jnp
import numpy as np
from jax import lax
from jax.experimental import pallas as pl
from jax.experimental.pallas import tpu as pltpu
from jax.sharding import PartitionSpec as P

HD = 128


EPS = 1e-06
THETA = 500000.0
NEGATIVE = -1e30


def full_width(value):
    return lax.all_gather(value, "tp", axis=2, tiled=True)


def share(value):
    return lax.psum_scatter(value, "tp", scatter_dimension=2, tiled=True)


def tp_total(values):
    return lax.psum(values, "tp")


def rotary_tables(positions):
    half_dim = HD // 2
    frequency = THETA ** (-2.0 * jnp.arange(half_dim, dtype=jnp.float32) / HD)
    angles = positions.astype(jnp.float32)[..., None] * frequency
    return (jnp.cos(angles)[..., None, :], jnp.sin(angles)[..., None, :])


def rotate(value, cosine, sine):
    half_dim = value.shape[-1] // 2
    first, second = (value[..., :half_dim], value[..., half_dim:])
    return jnp.concatenate(
        [first * cosine - second * sine, second * cosine + first * sine], axis=-1
    )


def unrotate(grad, cosine, sine):
    half_dim = grad.shape[-1] // 2
    first, second = (grad[..., :half_dim], grad[..., half_dim:])
    return jnp.concatenate(
        [first * cosine + second * sine, second * cosine - first * sine], axis=-1
    )


def key_positions(block_order, start, count, block_len):
    slots = start + jnp.arange(count, dtype=jnp.int32)
    owner = slots // block_len
    ranks = jnp.arange(block_order.shape[1], dtype=jnp.int32)
    chosen = jnp.sum(
        jnp.where(owner[None, :, None] == ranks[None, None, :], block_order[:, None, :], 0), axis=2
    )
    return chosen * block_len + slots % block_len


def span_of():
    return 512


def shards(
    tokens,
    w_query,
    w_key,
    w_value,
    w_output,
    w_gate,
    w_up,
    w_down,
    gain_query,
    gain_key,
    gain_attention,
    gain_feedforward,
    block_order,
    cotangent,
):
    gathered = (
        lax.all_gather(w_query, "ctx", axis=0, tiled=True),
        lax.all_gather(w_key, "ctx", axis=0, tiled=True),
        lax.all_gather(w_value, "ctx", axis=0, tiled=True),
        lax.all_gather(w_output, "ctx", axis=1, tiled=True),
        lax.all_gather(w_gate, "ctx", axis=0, tiled=True),
        lax.all_gather(w_up, "ctx", axis=0, tiled=True),
        lax.all_gather(w_down, "ctx", axis=1, tiled=True),
        lax.all_gather(gain_query, "ctx", axis=0, tiled=True),
        lax.all_gather(gain_key, "ctx", axis=0, tiled=True),
        lax.all_gather(gain_attention, "ctx", axis=0, tiled=True),
        lax.all_gather(gain_feedforward, "ctx", axis=0, tiled=True),
    )
    wq_full, wk_full, wv_full, wo_full, wg_full, wu_full, wd_full = gathered[:7]
    g_query = gathered[7].astype(jnp.float32)
    g_key = gathered[8].astype(jnp.float32)
    g_attn = gathered[9].astype(jnp.float32)
    g_feed = gathered[10].astype(jnp.float32)
    seq_count, block_len, local_width = tokens.shape
    row_count = seq_count * block_len
    scale = HD ** (-0.5)
    tok_full = full_width(tokens)
    tok_rows = tok_full.reshape(row_count, -1)
    width = tok_rows.shape[1]
    queries = jnp.dot(tok_rows, wq_full, preferred_element_type=jnp.float32)
    keys_raw = jnp.dot(tok_rows, wk_full, preferred_element_type=jnp.float32)
    values_raw = jnp.dot(tok_rows, wv_full, preferred_element_type=jnp.float32)
    head_width = queries.shape[1]
    head_count = head_width // HD
    q_squares, k_squares = tp_total(
        (jnp.sum(queries * queries, axis=1), jnp.sum(keys_raw * keys_raw, axis=1))
    )
    q_inverse = lax.rsqrt(q_squares / width + EPS)[:, None]
    k_inverse = lax.rsqrt(k_squares / width + EPS)[:, None]
    q_normed = queries * q_inverse * g_query
    k_normed = keys_raw * k_inverse * g_key
    ctx_rank = lax.axis_index("ctx")
    ranks = jnp.arange(block_order.shape[1], dtype=jnp.int32)
    my_block = jnp.sum(jnp.where(ranks[None, :] == ctx_rank, block_order, 0), axis=1)
    q_pos = my_block[:, None] * block_len + jnp.arange(block_len, dtype=jnp.int32)[None, :]
    cosine, sine = rotary_tables(q_pos)
    q_rot = rotate(q_normed.reshape(seq_count, block_len, head_count, HD), cosine, sine).astype(
        jnp.bfloat16
    )
    k_rot = rotate(k_normed.reshape(seq_count, block_len, head_count, HD), cosine, sine).astype(
        jnp.bfloat16
    )
    k_flat = k_rot.reshape(seq_count, block_len, head_width)
    v_flat = values_raw.astype(jnp.bfloat16).reshape(seq_count, block_len, head_width)

    def stat_block(state, key_piece, k_pos):
        run_max, run_sum = state
        scores = (
            jnp.einsum("sqhd,skhd->shqk", q_rot, key_piece, preferred_element_type=jnp.float32)
            * scale
        )
        visible = k_pos[:, None, None, :] <= q_pos[:, None, :, None]
        scores = jnp.where(visible, scores, NEGATIVE)
        new_max = jnp.maximum(run_max, jnp.max(scores, axis=-1))
        weights = jnp.where(visible, jnp.exp(scores - new_max[..., None]), 0.0)
        run_sum = run_sum * jnp.exp(run_max - new_max) + jnp.sum(weights, axis=-1)
        return (new_max, run_sum)

    init = (
        jnp.full((seq_count, head_count, block_len), NEGATIVE, jnp.float32),
        jnp.zeros((seq_count, head_count, block_len), jnp.float32),
    )
    fold_key_all = lax.all_gather(k_flat, "ctx", axis=1, tiled=True)
    count = fold_key_all.shape[1]
    span = span_of()

    def fold_one_span(step_index, inner):
        offset = step_index * span
        key_piece = lax.dynamic_slice_in_dim(fold_key_all, offset, span, 1).reshape(
            seq_count, span, head_count, HD
        )
        k_pos = key_positions(block_order, offset, span, block_len)
        return stat_block(inner, key_piece, k_pos)

    run_max, run_sum = lax.fori_loop(0, count // span, fold_one_span, init)
    key_all, val_all = (
        lax.all_gather(k_flat, "ctx", axis=1, tiled=True),
        lax.all_gather(v_flat, "ctx", axis=1, tiled=True),
    )
    log_total = run_max + jnp.log(run_sum)
    total_len = key_all.shape[1]
    total_span = span_of()

    def value_span(step_index, acc):
        offset = step_index * total_span
        key_piece = lax.dynamic_slice_in_dim(key_all, offset, total_span, 1).reshape(
            seq_count, total_span, head_count, HD
        )
        val_piece = lax.dynamic_slice_in_dim(val_all, offset, total_span, 1).reshape(
            seq_count, total_span, head_count, HD
        )
        k_pos = key_positions(block_order, offset, total_span, block_len)
        scores = (
            jnp.einsum("sqhd,skhd->shqk", q_rot, key_piece, preferred_element_type=jnp.float32)
            * scale
        )
        visible = k_pos[:, None, None, :] <= q_pos[:, None, :, None]
        weights = jnp.where(visible, jnp.exp(scores - log_total[..., None]), 0.0).astype(
            jnp.bfloat16
        )
        return acc + jnp.einsum(
            "shqk,skhd->sqhd", weights, val_piece, preferred_element_type=jnp.float32
        )

    attended = lax.fori_loop(
        0,
        total_len // total_span,
        value_span,
        jnp.zeros((seq_count, block_len, head_count, HD), jnp.float32),
    )
    attn_bf = attended.reshape(row_count, head_width).astype(jnp.bfloat16)
    attn_proj = share(
        jnp.dot(attn_bf, wo_full, preferred_element_type=jnp.float32).reshape(
            seq_count, block_len, -1
        )
    )
    (a_squares,) = tp_total((jnp.sum(attn_proj * attn_proj, axis=2),))
    a_inverse = lax.rsqrt(a_squares / width + EPS)[..., None]
    hidden_state = tokens.astype(jnp.float32) + attn_proj * a_inverse * g_attn
    hidden_rows = full_width(hidden_state.astype(jnp.bfloat16)).reshape(row_count, -1)
    gate = jnp.dot(hidden_rows, wg_full, preferred_element_type=jnp.float32)
    up_vals = jnp.dot(hidden_rows, wu_full, preferred_element_type=jnp.float32)
    sigma = jax.nn.sigmoid(gate)
    activation = (gate * sigma * up_vals).astype(jnp.bfloat16)
    mixed = share(
        jnp.dot(activation, wd_full, preferred_element_type=jnp.float32).reshape(
            seq_count, block_len, -1
        )
    )
    (m_squares,) = tp_total((jnp.sum(mixed * mixed, axis=2),))
    m_inverse = lax.rsqrt(m_squares / width + EPS)[..., None]
    output = hidden_state + mixed * m_inverse * g_feed
    upstream = cotangent.astype(jnp.float32)
    (m_dots,) = tp_total((jnp.sum(g_feed * upstream * mixed, axis=2),))
    d_mixed = m_inverse * (g_feed * upstream) - mixed * m_inverse**3 * (m_dots / width)[..., None]
    d_gfeed = jnp.sum(upstream * mixed * m_inverse, axis=(0, 1))
    d_mixed_rows = full_width(d_mixed.astype(jnp.bfloat16)).reshape(row_count, -1)
    grad_down = jnp.dot(activation.T, d_mixed_rows, preferred_element_type=jnp.float32)
    d_act = jnp.dot(d_mixed_rows, wd_full.T, preferred_element_type=jnp.float32)
    d_up_bf = (d_act * gate * sigma).astype(jnp.bfloat16)
    d_gate_bf = (d_act * up_vals * sigma * (1.0 + gate * (1.0 - sigma))).astype(jnp.bfloat16)
    grad_gate = jnp.dot(hidden_rows.T, d_gate_bf, preferred_element_type=jnp.float32)
    grad_up = jnp.dot(hidden_rows.T, d_up_bf, preferred_element_type=jnp.float32)
    back_ff = jnp.dot(d_gate_bf, wg_full.T, preferred_element_type=jnp.float32) + jnp.dot(
        d_up_bf, wu_full.T, preferred_element_type=jnp.float32
    )
    d_hidden = upstream + share(back_ff.reshape(seq_count, block_len, -1))
    (a_dots,) = tp_total((jnp.sum(g_attn * d_hidden * attn_proj, axis=2),))
    d_attn = (
        a_inverse * (g_attn * d_hidden) - attn_proj * a_inverse**3 * (a_dots / width)[..., None]
    )
    d_gattn = jnp.sum(d_hidden * attn_proj * a_inverse, axis=(0, 1))
    d_attn_rows = full_width(d_attn.astype(jnp.bfloat16)).reshape(row_count, -1)
    grad_outproj = jnp.dot(attn_bf.T, d_attn_rows, preferred_element_type=jnp.float32)
    d_heads = jnp.dot(d_attn_rows, wo_full.T, preferred_element_type=jnp.float32).reshape(
        seq_count, block_len, head_count, HD
    )
    deltas = jnp.sum(d_heads * attended, axis=3).transpose(0, 2, 1)
    d_heads_bf = d_heads.astype(jnp.bfloat16)

    def grad_block(key_piece, val_piece, k_pos):
        scores = (
            jnp.einsum("sqhd,skhd->shqk", q_rot, key_piece, preferred_element_type=jnp.float32)
            * scale
        )
        visible = k_pos[:, None, None, :] <= q_pos[:, None, :, None]
        probs = jnp.where(visible, jnp.exp(scores - log_total[..., None]), 0.0)
        d_probs = jnp.einsum(
            "sqhd,skhd->shqk", d_heads_bf, val_piece, preferred_element_type=jnp.float32
        )
        d_scores = (probs * (d_probs - deltas[..., None])).astype(jnp.bfloat16)
        return (probs, d_scores)

    def query_span(step_index, acc):
        offset = step_index * total_span
        key_piece = lax.dynamic_slice_in_dim(key_all, offset, total_span, 1).reshape(
            seq_count, total_span, head_count, HD
        )
        val_piece = lax.dynamic_slice_in_dim(val_all, offset, total_span, 1).reshape(
            seq_count, total_span, head_count, HD
        )
        k_pos = key_positions(block_order, offset, total_span, block_len)
        probs, d_scores = grad_block(key_piece, val_piece, k_pos)
        return (
            acc
            + jnp.einsum("shqk,skhd->sqhd", d_scores, key_piece, preferred_element_type=jnp.float32)
            * scale
        )

    d_qrot = lax.fori_loop(
        0,
        total_len // total_span,
        query_span,
        jnp.zeros((seq_count, block_len, head_count, HD), jnp.float32),
    )
    count = block_len * lax.axis_size("ctx")
    key_span = span_of()

    def key_one_span(step_index, buffer):
        offset = step_index * key_span
        key_piece = lax.dynamic_slice_in_dim(key_all, offset, key_span, 1).reshape(
            seq_count, key_span, head_count, HD
        )
        val_piece = lax.dynamic_slice_in_dim(val_all, offset, key_span, 1).reshape(
            seq_count, key_span, head_count, HD
        )
        k_pos = key_positions(block_order, offset, key_span, block_len)
        probs, d_scores = grad_block(key_piece, val_piece, k_pos)
        d_keyp = (
            jnp.einsum("shqk,sqhd->skhd", d_scores, q_rot, preferred_element_type=jnp.float32)
            * scale
        )
        d_valp = jnp.einsum(
            "shqk,sqhd->skhd",
            probs.astype(jnp.bfloat16),
            d_heads_bf,
            preferred_element_type=jnp.float32,
        )
        both = jnp.concatenate(
            [
                d_keyp.reshape(seq_count, key_span, head_width),
                d_valp.reshape(seq_count, key_span, head_width),
            ],
            axis=2,
        )
        return lax.dynamic_update_slice_in_dim(buffer, both.transpose(1, 0, 2), offset, 0)

    key_sums = (
        lax.psum_scatter(
            lax.fori_loop(
                0,
                count // key_span,
                key_one_span,
                jnp.zeros((count, seq_count, 2 * head_width), jnp.float32),
            ).astype(jnp.bfloat16),
            "ctx",
            scatter_dimension=0,
            tiled=True,
        )
        .astype(jnp.float32)
        .transpose(1, 0, 2)
    )
    d_krot = key_sums[..., :head_width].reshape(seq_count, block_len, head_count, HD)
    d_values = key_sums[..., head_width:].reshape(row_count, head_width)
    dq_normed = unrotate(d_qrot, cosine, sine).reshape(row_count, head_width)
    dk_normed = unrotate(d_krot, cosine, sine).reshape(row_count, head_width)
    q_dots, k_dots = tp_total(
        (
            jnp.sum(g_query * dq_normed * queries, axis=1),
            jnp.sum(g_key * dk_normed * keys_raw, axis=1),
        )
    )
    d_queries = (
        q_inverse * (g_query * dq_normed) - queries * q_inverse**3 * (q_dots / width)[:, None]
    )
    d_keys = k_inverse * (g_key * dk_normed) - keys_raw * k_inverse**3 * (k_dots / width)[:, None]
    d_gquery = jnp.sum(dq_normed * queries * q_inverse, axis=0)
    d_gkey = jnp.sum(dk_normed * keys_raw * k_inverse, axis=0)
    dq_bf = d_queries.astype(jnp.bfloat16)
    dk_bf = d_keys.astype(jnp.bfloat16)
    dv_bf = d_values.astype(jnp.bfloat16)
    grad_q = jnp.dot(tok_rows.T, dq_bf, preferred_element_type=jnp.float32)
    grad_k = jnp.dot(tok_rows.T, dk_bf, preferred_element_type=jnp.float32)
    grad_v = jnp.dot(tok_rows.T, dv_bf, preferred_element_type=jnp.float32)
    back_attn = (
        jnp.dot(dq_bf, wq_full.T, preferred_element_type=jnp.float32)
        + jnp.dot(dk_bf, wk_full.T, preferred_element_type=jnp.float32)
        + jnp.dot(dv_bf, wv_full.T, preferred_element_type=jnp.float32)
    )
    grad_input = d_hidden + share(back_attn.reshape(seq_count, block_len, -1))
    summed = (
        lax.psum_scatter(
            grad_q.astype(jnp.bfloat16), "ctx", scatter_dimension=0, tiled=True
        ).astype(jnp.float32),
        lax.psum_scatter(
            grad_k.astype(jnp.bfloat16), "ctx", scatter_dimension=0, tiled=True
        ).astype(jnp.float32),
        lax.psum_scatter(
            grad_v.astype(jnp.bfloat16), "ctx", scatter_dimension=0, tiled=True
        ).astype(jnp.float32),
        lax.psum_scatter(
            grad_outproj.astype(jnp.bfloat16), "ctx", scatter_dimension=1, tiled=True
        ).astype(jnp.float32),
        lax.psum_scatter(
            grad_gate.astype(jnp.bfloat16), "ctx", scatter_dimension=0, tiled=True
        ).astype(jnp.float32),
        lax.psum_scatter(
            grad_up.astype(jnp.bfloat16), "ctx", scatter_dimension=0, tiled=True
        ).astype(jnp.float32),
        lax.psum_scatter(
            grad_down.astype(jnp.bfloat16), "ctx", scatter_dimension=1, tiled=True
        ).astype(jnp.float32),
        lax.psum_scatter(
            d_gquery.astype(jnp.bfloat16), "ctx", scatter_dimension=0, tiled=True
        ).astype(jnp.float32),
        lax.psum_scatter(
            d_gkey.astype(jnp.bfloat16), "ctx", scatter_dimension=0, tiled=True
        ).astype(jnp.float32),
        lax.psum_scatter(
            d_gattn.astype(jnp.bfloat16), "ctx", scatter_dimension=0, tiled=True
        ).astype(jnp.float32),
        lax.psum_scatter(
            d_gfeed.astype(jnp.bfloat16), "ctx", scatter_dimension=0, tiled=True
        ).astype(jnp.float32),
    )
    return (
        output,
        grad_input,
        summed[0],
        summed[1],
        summed[2],
        summed[3],
        summed[4],
        summed[5],
        summed[6],
        summed[7],
        summed[8],
        summed[9],
        summed[10],
    )


MESH = pl.DeviceIdType.MESH
NT = (((1,), (1,)), ((), ()))
TN = (((0,), (0,)), ((), ()))
F32 = jnp.float32
BF16 = jnp.bfloat16
COLS = (0, 1, 2, 4, 5)


def layer_kernel(dims, *refs):
    (chips, tps, seqs, blk, width, head_w, ff_w) = dims
    rows = seqs * blk
    both = 2 * rows
    share_rows = rows // tps
    feats = width // tps
    heads = head_w // HD
    slab = width // (2 * chips)
    halves = (head_w, head_w, head_w, head_w, ff_w, ff_w, ff_w)
    total = 2 * chips * blk
    scale = HD ** (-0.5)
    it = iter(refs)

    def take(n):
        return [next(it) for _ in range(n)]

    (tok_in, cot_in) = take(2)
    w_in = take(7)
    (blocks, *gains, table) = take(6)
    (out_ref, gin_ref, ggain_ref) = take(3)
    rx_g = take(7)
    summed = take(4)
    w = take(7)
    via = take(7)
    (tok, tok_t, hid, hid_t, dmix, dattn) = take(6)
    (lin, fac, act, act_t, dgate, dup) = take(6)
    (st_p, rx_p, st_z, rx_z, rx_f) = take(5)
    (q_raw, k_raw, qkv, qa, probs, att_f, att_st, att, att_t) = take(9)
    (dh, d_o, dqkv_st, dqkv) = take(4)
    (sq_own, sq_rx, inv_q, inv_k) = take(4)
    (cot, proj, hstate, dhid, stage) = take(5)
    (gbuf, gall, gfull, gqk, gg_row, gg_rx1, gg_mid, gg_rx2) = take(8)
    (ws, wr, gs, gr) = take(4)
    (zs, zr, ps, pr) = take(4)
    (rps, rpr, rzs, rzr) = take(4)
    (ms, mr) = take(2)
    (ss, sr) = take(2)
    (as_, ar) = take(2)
    (loc,) = take(1)
    (d_acc, cosf, sinf, pos_row, gtile) = take(5)
    (xs, xr) = take(2)

    ctx = lax.axis_index("ctx")
    z = lax.axis_index("tp")
    c = ctx // 2
    k = ctx % 2
    ok = 1 - k
    partner = c * 2 + ok
    near = (c + 1 - 2 * (c % 2), (c + 2) % chips)
    far = chips - 1 - c

    def zp(i):
        return (z + i) % tps

    def chip(i):
        return (c + i) % chips

    def ds(start, size):
        return pl.ds(pl.multiple_of(start, size), size)

    def remote(src, dst, ssem, rsem, to_ctx, to_z):
        return pltpu.make_async_remote_copy(
            src_ref=src,
            dst_ref=dst,
            send_sem=ssem,
            recv_sem=rsem,
            device_id=(to_ctx, to_z),
            device_id_type=MESH,
        )

    peers = [(chip(i) * 2 + (k + d) % 2, z) for i in range(chips) for d in range(2) if i or d]
    peers += [(ctx, zp(i)) for i in range(1, tps)]
    peers += [(partner, zp(i)) for i in range(1, tps)]
    barrier = pltpu.get_barrier_semaphore()
    for peer in peers:
        pl.semaphore_signal(barrier, inc=1, device_id=peer, device_id_type=MESH)

    def go(copy):
        copy.start()
        return copy

    def sent(ref, sem):
        remote(ref, ref, sem, sem, partner, z).wait_send()

    def came(ref, sem):
        remote(ref, ref, sem, sem, partner, z).wait_recv()

    def slab_of(m, owner):
        if m in COLS:
            return w[m].at[ds(owner * slab, slab), :]
        return w[m].at[:, ds(owner * slab, slab)]

    def slabs(m, count):
        return w[m].at[0 : count * slab, :] if m in COLS else w[m].at[:, 0 : count * slab]

    def half_of(m, core):
        if m in COLS:
            return w_in[m].at[:, ds(core * halves[m], halves[m])]
        return w_in[m].at[ds(core * halves[m], halves[m]), :]

    w_own = {}
    w_wait = {}

    def send_w(m, d):
        core = (k + d) % 2
        for n in range(2):
            go(remote(half_of(m, core), slab_of(m, ctx), ws.at[m, 0], wr.at[m, 2 * n + k], near[n] * 2 + core, z))
        if d:
            go(remote(half_of(m, ok), slab_of(m, ctx), ws.at[m, 0], wr.at[m, 4], partner, z))
        else:
            w_own[m] = pltpu.make_async_copy(half_of(m, k), slab_of(m, ctx), loc.at[m])
            w_own[m].start()

    def source(n):
        if n < 4:
            return near[n // 2] * 2 + n % 2
        return partner if n == 4 else far * 2 + n - 5

    def got_w(m, *which):
        for n in which:
            if (m, n) not in w_wait:
                w_wait[m, n] = True
                came(slabs(m, 1), wr.at[m, n])

    def pass_w(m):
        for n in range(2):
            got_w(m, 3 * n)
            mine = slab_of(m, source(3 * n))
            go(remote(mine, mine, ws.at[m, 1], wr.at[m, 5 + n], near[1 - n] * 2 + k, z))

    def free_w(m):
        sent(slabs(m, 2), ws.at[m, 1])

    def wait_w(m):
        w_own[m].wait()
        got_w(m, *range(7))

    def into(m, n, core):
        if m in COLS:
            return rx_g[m].at[n, :, ds(core * halves[m], halves[m])]
        return rx_g[m].at[n, ds(core * halves[m], halves[m]), :]

    g_own = {}

    def send_far(m):
        for n in range(2):
            go(remote(slab_of(m, far * 2 + n), via[m].at[n], gs.at[m], gr.at[m, n], near[n] * 2 + k, z))

    def send_near(m, n):
        go(remote(slab_of(m, near[n] * 2 + n), into(m, 1 + n, k), gs.at[m], gr.at[m, 2], near[n] * 2 + n, z))

    def send_home(m):
        go(remote(slab_of(m, partner), into(m, 0, k), gs.at[m], gr.at[m, 2], partner, z))
        copy = pltpu.make_async_copy(slab_of(m, ctx), into(m, 0, k), loc.at[8 + m])
        copy.start()
        g_own[m] = copy

    def send_g(m):
        send_far(m)
        send_near(m, 0)
        send_near(m, 1)
        send_home(m)

    def pass_g(m):
        for n in range(2):
            to = near[1 - n] * 2 + n
            came(via[m].at[n], gr.at[m, n])
            total = slab_of(m, to)[...].astype(F32) + via[m][n].astype(F32)
            slab_of(m, to)[...] = total.astype(BF16)
            go(remote(slab_of(m, to), into(m, 2 - n, k), gs.at[m], gr.at[m, 2], to, z))

    def wait_g(m):
        g_own[m].wait()
        came(slabs(m, 5), gr.at[m, 2])

    def add_up(m):
        wait_g(m)
        if m in COLS:
            n = slab
            parts = (hid.at[0:n, :], hid.at[n : 2 * n, :], dmix.at[0:n, :], dmix.at[n : 2 * n, :])
        else:
            n = 2 * halves[m]
            parts = (hid_t.at[0:n, 0:slab], hid_t.at[0:n, slab : 2 * slab], tok_t.at[0:n, 0:slab], tok_t.at[0:n, slab : 2 * slab])
        loads = [pltpu.make_async_copy(rx_g[m].at[i], parts[i], loc.at[i]) for i in range(3)]
        for copy in loads:
            copy.start()
        for copy in loads:
            copy.wait()

        def add_step(j, carry):
            here = (slice(None), ds(j * 256, 256)) if m in COLS else (ds(j * 256, 256), slice(None))
            value = parts[0][here].astype(F32) + parts[1][here].astype(F32) + parts[2][here].astype(F32)
            parts[3][here] = value.astype(BF16)
            return carry

        lax.fori_loop(0, 2 * halves[m] // 256, add_step, 0)
        copy = pltpu.make_async_copy(parts[3], summed[m - 3], loc.at[3])
        copy.start()
        copy.wait()

    lane = lax.broadcasted_iota(jnp.int32, (blk, HD), 1)
    gtile[...] = jnp.zeros((8, 128), F32)
    for r in range(4):
        value = gains[r][...].astype(F32)
        value = jnp.concatenate([value, value], axis=1)
        gtile[r : r + 1, :] = jnp.where(lane[0:1, :] // 64 == k, value, 0.0)
    own_tok = pltpu.make_async_copy(tok_in, tok.at[ds(k * rows, rows), ds(z * feats, feats)], loc.at[16])
    own_tok.start()
    own_cot = pltpu.make_async_copy(cot_in.at[ds(z * share_rows, share_rows), :], cot.at[:, ds(z * feats, feats)], loc.at[17])
    own_cot.start()
    pl.semaphore_wait(barrier, len(peers))
    own_gain = pltpu.make_async_copy(gtile, gbuf.at[ctx], loc.at[18])
    own_gain.start()

    for i in range(1, tps):
        go(remote(tok_in, tok.at[ds(k * rows, rows), ds(z * feats, feats)], zs.at[0], zr.at[0, i - 1], ctx, zp(i)))
    go(remote(tok_in, tok.at[ds(k * rows, rows), ds(z * feats, feats)], ps.at[0], pr.at[0], partner, z))
    slots = [(i, d) for i in range(chips) for d in range(2)]
    for i, d in slots:
        if i or d:
            go(remote(gtile, gbuf.at[ctx], ms.at[0], mr.at[0], chip(i) * 2 + (k + d) % 2, z))
    for i in range(1, tps):
        go(remote(cot_in.at[ds(zp(i) * share_rows, share_rows), :], cot.at[:, ds(z * feats, feats)], ms.at[1], mr.at[1], ctx, zp(i)))
    for m in (0, 1, 2, 3):
        send_w(m, 0)
        send_w(m, 1)

    own_gain.wait()
    came(gbuf.at[0 : 2 * chips - 1], mr.at[0])
    own_gain2 = pltpu.make_async_copy(gbuf, gall.at[z], loc.at[19])
    own_gain2.start()
    for i in range(1, tps):
        go(remote(gbuf, gall.at[z], ms.at[2], mr.at[2], ctx, zp(i)))
    for r in range(2):
        pieces = [gbuf[4 * k + 2 * m, r : r + 1, :] + gbuf[4 * k + 2 * m + 1, r : r + 1, :] for m in range(head_w // 128)]
        gqk[r : r + 1, :] = jnp.concatenate(pieces, axis=1)

    sign = jnp.where(lane < HD // 2, -1.0, 1.0)
    for core in range(2):
        for s in range(seqs):
            block = blocks[s, 2 * c + core]
            c_block, s_block = table[0, pl.ds(block, 1), :], table[1, pl.ds(block, 1), :]
            c_in, s_in = table[2], table[3]
            here = slice((core * seqs + s) * blk, (core * seqs + s + 1) * blk)
            cosf[here, :] = c_block * c_in - s_block * s_in
            sinf[here, :] = (s_block * c_in + c_block * s_in) * sign
    for j in range(2 * chips):
        start = blocks[c // heads, j] * blk
        here = slice(j * blk, (j + 1) * blk)
        pos_row[:, here] = start + lane[0:8, :]

    own_tok.wait()
    pass_w(0)
    for i in range(1, tps):
        pass_w(i)
        if i == tps - 1:
            send_w(4, 0)
        came(tok.at[0:rows, 0:feats], zr.at[0, i - 1])
        part = tok.at[ds(k * rows, rows), ds(((z - i) % tps) * feats, feats)]
        go(remote(part, part, ps.at[0], pr.at[0], partner, z))
    came(tok.at[0:rows, :], pr.at[0])

    def row_of(value):
        folded = value[:, :128]
        for h in range(1, heads):
            folded = folded + value[:, h * 128 : (h + 1) * 128]
        return jnp.sum(jnp.transpose(folded), axis=0, keepdims=True)

    def column_of(row):
        return jnp.transpose(jnp.broadcast_to(row, (128, both)))

    def totals(idx):
        n = 0
        for i in range(tps):
            for d in range(2):
                if i or d:
                    to = ctx if d == 0 else partner
                    go(remote(sq_own.at[idx], sq_rx.at[idx, n], ss.at[idx], sr.at[idx], to, zp(i)))
                    n += 1
        came(sq_rx.at[idx], sr.at[idx])
        total = sq_own[idx]
        for j in range(n):
            total = total + sq_rx[idx, j]
        return total

    for m in (0, 1, 2):
        wait_w(m)
        value = jnp.dot(tok[...], w[m][...], preferred_element_type=F32)
        if m == 0:
            q_raw[...] = value
            sq_own[0, 0:1, :] = row_of(value * value)
        elif m == 1:
            k_raw[...] = value
            sq_own[0, 1:2, :] = row_of(value * value)
        else:
            qkv[2] = value.astype(BF16).reshape(2, seqs, blk, head_w)
    sq_own[0, 2:8, :] = jnp.zeros((6, both), F32)
    squares = totals(0)
    inverse = lax.rsqrt(squares / width + EPS)
    inv_q[...] = column_of(inverse[0:1, :])
    inv_k[...] = column_of(inverse[1:2, :])
    for t, (raw, inv) in enumerate(((q_raw, inv_q), (k_raw, inv_k))):
        for h in range(heads):
            lanes = slice(h * HD, (h + 1) * HD)
            normed = raw[:, lanes] * inv[...] * gqk[t : t + 1, lanes]
            turned = normed * cosf[...] + pltpu.roll(normed, HD // 2, 1) * sinf[...]
            qkv[t, :, :, :, lanes] = turned.astype(BF16).reshape(2, seqs, blk, HD)

    def to_owner(idx, value, owned, stacked):
        size = owned.at[:, 0 : 2 * chips - 2] if stacked else owned.at[0 : 2 * chips - 2]
        for i in range(chips):
            to = chip(i)
            s, h = to // heads, to % heads
            if stacked:
                src = value.at[:, :, s, :, ds(h * HD, HD)]
                dst = owned.at[:, ds(2 * c, 2)]
            else:
                src = value.at[:, s, :, ds(h * HD, HD)]
                dst = owned.at[ds(2 * c, 2)]
            if i:
                go(remote(src, dst, as_.at[idx], ar.at[idx], to * 2 + k, z))
            else:
                own = pltpu.make_async_copy(src, dst, loc.at[20 + idx])
                own.start()
        return own, size, idx

    def from_owner(idx, owned, value, stacked):
        size = owned.at[:, 0 : 2 * chips - 2] if stacked else owned.at[0 : 2 * chips - 2]
        s, h = c // heads, c % heads
        for i in range(chips):
            to = chip(i)
            if stacked:
                src = owned.at[:, ds(2 * to, 2)]
                dst = value.at[:, :, s, :, ds(h * HD, HD)]
            else:
                src = owned.at[ds(2 * to, 2)]
                dst = value.at[:, s, :, ds(h * HD, HD)]
            if i:
                go(remote(src, dst, as_.at[idx], ar.at[idx], to * 2 + k, z))
            else:
                own = pltpu.make_async_copy(src, dst, loc.at[20 + idx])
                own.start()
        return own, size, idx

    def arrive(pair):
        own, size, idx = pair
        own.wait()
        came(size, ar.at[idx])
        sent(size, as_.at[idx])

    pair = to_owner(0, qkv, qa, True)
    send_w(4, 1)
    arrive(pair)
    step = 2 * blk

    def attend(i, carry):
        here = ds(i * step, step)
        q = qa[0, pl.ds(2 * i, 2)].reshape(step, HD)
        s = lax.dot_general(q, qa[1].reshape(total, HD), NT, preferred_element_type=F32) * scale
        at = lax.broadcasted_iota(jnp.int32, (step, 1), 0)
        first = blocks[c // heads, 2 * i] * blk
        second = (blocks[c // heads, 2 * i + 1] - 1) * blk
        visible = pos_row[0:1, :] <= at + jnp.where(at < blk, first, second)
        s = jnp.where(visible, s, NEGATIVE)
        top = jnp.max(s, axis=1, keepdims=True)
        e = jnp.where(visible, jnp.exp(s - top), 0.0)
        p = (e * (1.0 / jnp.sum(e, axis=1, keepdims=True))).astype(BF16)
        probs[here, :] = p
        o = jnp.dot(p, qa[2].reshape(total, HD), preferred_element_type=F32)
        att_f[here, :] = o
        att_st[pl.ds(2 * i, 2)] = o.astype(BF16).reshape(2, blk, HD)
        return carry

    lax.fori_loop(0, chips, attend, 0)
    back = from_owner(1, att_st, att, False)
    pass_w(4)
    send_w(5, 0)
    send_w(5, 1)
    send_w(6, 0)
    own_gain2.wait()
    came(gall.at[0 : tps - 1], mr.at[2])
    for r in range(2):
        pieces = []
        for zz in range(tps):
            for m in range(chips):
                pieces.append(gall[zz, 2 * m, 2 + r : 3 + r, :] + gall[zz, 2 * m + 1, 2 + r : 3 + r, :])
        gfull[r : r + 1, :] = jnp.concatenate(pieces, axis=1)
    for s in range(width // 256):
        tok_t[s * 256 : (s + 1) * 256, :] = jnp.transpose(tok[:, s * 256 : (s + 1) * 256])
    arrive(back)
    wait_w(3)

    cw = feats
    rs_live = {}

    def rp_copy(idx, i, off):
        return remote(st_p.at[:, ds(off, cw)], rx_p.at[idx % 2, :, ds(off, cw)], rps.at[idx], rpr.at[idx, i], partner, z)

    def rz_copy(idx, i, j, off):
        return remote(
            st_z.at[ds(zp(j) * share_rows, share_rows), ds(off, cw)],
            rx_z.at[idx % 2, j - 1, :, ds(off, cw)],
            rzs.at[idx],
            rzr.at[idx],
            ctx,
            zp(j),
        )

    def reduce_rows(idx, partial, offset, before=None, meanwhile=None):
        def one(i):
            off = offset(i)
            if before is not None:
                before(i)
            st_p[:, ds(off, cw)] = partial(ok, off).astype(BF16)
            rp_copy(idx, i, off).start()
            mine = partial(k, off)
            rp_copy(idx, i, off).wait_recv()
            st_z[:, ds(off, cw)] = (mine + rx_p[idx % 2, :, ds(off, cw)].astype(F32)).astype(BF16)
            for j in range(1, tps):
                rz_copy(idx, i, j, off).start()

        if before is None:
            lax.fori_loop(0, tps, lambda i, x: (one(i), x)[1], 0)
        else:
            for i in range(tps):
                one(i)
        if meanwhile is not None:
            meanwhile()
        came(rx_z.at[idx % 2], rzr.at[idx])
        sent(rx_z.at[idx % 2], rzs.at[idx])
        sent(st_p, rps.at[idx])
        mine = st_z[ds(z * share_rows, share_rows), :].astype(F32)
        for j in range(tps - 1):
            mine = mine + rx_z[idx % 2, j].astype(F32)
        return mine

    def straight(i):
        return i * cw

    def mean_of(value):
        return jnp.sum(value, axis=1, keepdims=True) / width

    def spread(idx, buf):
        mine = buf.at[ds(k * rows + z * share_rows, share_rows), :]
        for i in range(1, tps):
            go(remote(mine, mine, zs.at[idx], zr.at[idx, i - 1], ctx, zp(i)))
        go(remote(mine, mine, ps.at[idx], pr.at[idx], partner, z))

        def finish(meanwhile=None):
            for i in range(1, tps):
                came(buf.at[0:share_rows, :], zr.at[idx, i - 1])
                if i == 1 and meanwhile is not None:
                    meanwhile()
                part = buf.at[ds(k * rows + ((z - i) % tps) * share_rows, share_rows), :]
                go(remote(part, part, ps.at[idx], pr.at[idx], partner, z))
            came(buf.at[0:rows, :], pr.at[idx])
            sent(buf.at[0 : (tps - 1) * share_rows, :], zs.at[idx])
            sent(buf.at[0:rows, :], ps.at[idx])

        return finish

    my_rows = ds(k * rows + z * share_rows, share_rows)
    heads_rows = [None]

    def o_partial(core, off):
        left = att[pl.ds(core, 1)].reshape(rows, head_w)
        return jnp.dot(left, w[3][:, ds(off, cw)], preferred_element_type=F32)

    value = reduce_rows(0, o_partial, straight)
    proj[...] = value
    a_inverse = lax.rsqrt(mean_of(value * value) + EPS)
    state = tok[my_rows, :].astype(F32) + value * a_inverse * gfull[0:1, :]
    hstate[...] = state
    hid[my_rows, :] = state.astype(BF16)
    finish = spread(1, hid)
    own_cot.wait()
    came(cot.at[:, 0 : (tps - 1) * feats], mr.at[1])
    att_t[...] = jnp.transpose(att[...].reshape(both, head_w))

    def more_weights():
        pass_w(5)
        send_w(6, 1)

    finish(more_weights)

    fw = 256
    wait_w(4)

    def gate_step(j, carry):
        here = ds(j * fw, fw)
        lin[:, here] = jnp.dot(hid[...], w[4][:, here], preferred_element_type=F32)
        return carry

    lax.fori_loop(0, ff_w // fw, gate_step, 0)
    for s in range(width // 256):
        hid_t[s * 256 : (s + 1) * 256, :] = jnp.transpose(hid[:, s * 256 : (s + 1) * 256])
    wait_w(5)

    def up_step(j, carry):
        here = ds(j * fw, fw)
        up = jnp.dot(hid[...], w[5][:, here], preferred_element_type=F32)
        gate = lin[:, here]
        sigma = jax.nn.sigmoid(gate)
        swish = gate * sigma
        lin[:, here] = swish
        fac[:, here] = up * sigma * (1.0 + gate * (1.0 - sigma))
        value = (swish * up).astype(BF16)
        act[:, here] = value
        act_t[here, :] = jnp.transpose(value)
        return carry

    lax.fori_loop(0, ff_w // fw, up_step, 0)

    def down_partial(core, off):
        return jnp.dot(act[ds(core * rows, rows), :], w[6][:, ds(off, cw)], preferred_element_type=F32)

    def from_chip(i):
        return (c, near[0], near[1], far)[i] * cw

    def down_ready(i):
        if i == 0:
            w_own[6].wait()
        if i == 1:
            pass_w(6)
        got_w(6, *((4,), (0, 1), (2, 3), (5, 6))[i])

    value = reduce_rows(1, down_partial, from_chip, down_ready)
    m_inverse = lax.rsqrt(mean_of(value * value) + EPS)
    scaled = value * m_inverse
    upstream = cot[...].astype(F32)
    gained = upstream * gfull[1:2, :]
    back_mix = m_inverse * gained - scaled * (m_inverse * m_inverse) * mean_of(gained * value)
    dmix[my_rows, :] = back_mix.astype(BF16)
    order = (far, near[0], near[1], c)

    def mix_along(n, i):
        here = dmix.at[my_rows, ds(order[n] * cw, cw)]
        return remote(here, here, xs.at[n], xr.at[n], ctx, zp(i))

    def mix_across(n, i):
        owner = (z - i) % tps
        here = dmix.at[ds(k * rows + owner * share_rows, share_rows), ds(order[n] * cw, cw)]
        return remote(here, here, xs.at[chips], xr.at[chips + n], partner, z)

    def mix_start(n):
        for i in range(1, tps):
            mix_along(n, i).start()
        mix_across(n, 0).start()

    mix_start(0)
    gg_row[1:2, :] = jnp.sum(upstream * scaled, axis=0, keepdims=True)
    stage[...] = hstate[...] + scaled * gfull[1:2, :]

    free_w(6)
    for n in range(chips):
        sent(dmix.at[0:share_rows, 0 : (tps - 1) * cw], xs.at[n])
        if n < chips - 1:
            mix_start(n + 1)
        came(dmix.at[0:share_rows, 0 : (tps - 1) * cw], xr.at[n])
        for i in range(1, tps):
            mix_across(n, i).start()
        came(dmix.at[0:rows, 0:cw], xr.at[chips + n])
        off = order[n] * cw

        def dact_step(j, carry):
            here = ds(j * fw, fw)
            d_act = lax.dot_general(dmix[:, ds(off, cw)], w[6][here, ds(off, cw)], NT, preferred_element_type=F32)
            part = (ds((j // 2) * both, both), ds((j % 2) * fw, fw))
            if n:
                d_act = d_act + d_acc[part]
            if n < chips - 1:
                d_acc[part] = d_act
            else:
                dup[:, here] = (d_act * lin[:, here]).astype(BF16)
                dgate[:, here] = (d_act * fac[:, here]).astype(BF16)
            return carry

        lax.fori_loop(0, ff_w // fw, dact_step, 0)
        grad = jnp.dot(act_t[...], dmix[:, ds(off, cw)], preferred_element_type=F32)
        w[6][:, ds(off, cw)] = grad.astype(BF16)
        if n == 0:
            send_far(6)
        elif n < chips - 1:
            send_near(6, n - 1)
        else:
            send_home(6)

    sent(dmix.at[0:rows, :], xs.at[chips])
    for i in range(1, tps):
        go(remote(stage.at[:, ds(zp(i) * feats, feats)], out_ref.at[ds(z * share_rows, share_rows), :], ms.at[3], mr.at[3], ctx, zp(i)))
    own_out = pltpu.make_async_copy(stage.at[:, ds(z * feats, feats)], out_ref.at[ds(z * share_rows, share_rows), :], loc.at[24])
    own_out.start()

    def ff_partial(core, off):
        here = ds(core * rows, rows)
        return lax.dot_general(dgate[here, :], w[4][ds(off, cw), :], NT, preferred_element_type=F32) + lax.dot_general(
            dup[here, :], w[5][ds(off, cw), :], NT, preferred_element_type=F32
        )

    def ggate_step(j, carry):
        here = ds(j * fw, fw)
        w[4][:, here] = jnp.dot(hid_t[...], dgate[:, here], preferred_element_type=F32).astype(BF16)
        return carry

    def gup_step(j, carry):
        here = ds(j * fw, fw)
        w[5][:, here] = jnp.dot(hid_t[...], dup[:, here], preferred_element_type=F32).astype(BF16)
        return carry

    def gate_grad():
        free_w(4)
        lax.fori_loop(0, ff_w // fw, ggate_step, 0)
        send_g(4)
        free_w(5)
        lax.fori_loop(0, ff_w // fw, gup_step, 0)
        send_far(5)

    pass_g(6)
    value = reduce_rows(2, ff_partial, straight, meanwhile=gate_grad) + cot[...].astype(F32)
    dhid[...] = value
    projected = proj[...]
    a_inverse = lax.rsqrt(mean_of(projected * projected) + EPS)
    scaled = projected * a_inverse
    gained = value * gfull[0:1, :]
    gg_row[0:1, :] = jnp.sum(value * scaled, axis=0, keepdims=True)
    gg_row[2:8, :] = jnp.zeros((6, width), F32)
    back_att = a_inverse * gained - scaled * (a_inverse * a_inverse) * mean_of(gained * projected)
    dattn[my_rows, :] = back_att.astype(BF16)
    finish = spread(3, dattn)
    for i in range(1, tps):
        go(remote(gg_row.at[:, ds(zp(i) * feats, feats)], gg_rx1.at[i - 1], ms.at[4], mr.at[4], ctx, zp(i)))

    finish(lambda: pass_g(4))

    value = lax.dot_general(dattn[...], w[3][...], NT, preferred_element_type=F32)
    dh[...] = value.astype(BF16).reshape(2, seqs, blk, head_w)
    pair = to_owner(2, dh, d_o, False)
    send_near(5, 0)
    send_near(5, 1)
    send_home(5)

    def go_step(j, carry):
        here = ds(j * fw, fw)
        w[3][:, here] = jnp.dot(att_t[...], dattn[:, here], preferred_element_type=F32).astype(BF16)
        return carry

    free_w(3)
    lax.fori_loop(0, width // fw, go_step, 0)
    arrive(pair)
    dk_acc, dv_acc = d_acc.at[:, 0:HD], d_acc.at[:, HD : 2 * HD]
    dk_acc[...] = jnp.zeros((total, HD), F32)
    dv_acc[...] = jnp.zeros((total, HD), F32)

    def unattend(i, carry):
        here = ds(i * step, step)
        q = qa[0, pl.ds(2 * i, 2)].reshape(step, HD)
        d_out = d_o[pl.ds(2 * i, 2)].reshape(step, HD)
        d_p = lax.dot_general(d_out, qa[2].reshape(total, HD), NT, preferred_element_type=F32)
        delta = jnp.sum(d_out.astype(F32) * att_f[here, :], axis=1, keepdims=True)
        p = probs[here, :]
        d_s = (p.astype(F32) * (d_p - delta)).astype(BF16)
        d_q = jnp.dot(d_s, qa[1].reshape(total, HD), preferred_element_type=F32) * scale
        dqkv_st[0, pl.ds(2 * i, 2)] = d_q.astype(BF16).reshape(2, blk, HD)
        dk_acc[...] += lax.dot_general(d_s, q, TN, preferred_element_type=F32)
        dv_acc[...] += lax.dot_general(p, d_out, TN, preferred_element_type=F32)
        return carry

    lax.fori_loop(0, chips, unattend, 0)
    dqkv_st[1] = (dk_acc[...] * scale).astype(BF16).reshape(2 * chips, blk, HD)
    dqkv_st[2] = dv_acc[...].astype(BF16).reshape(2 * chips, blk, HD)
    pair = from_owner(3, dqkv_st, dqkv, True)

    pass_g(5)
    send_g(3)
    arrive(pair)

    gg_mid[...] = jnp.zeros((8, feats), F32)
    for t, (raw, inv) in enumerate(((q_raw, inv_q), (k_raw, inv_k))):
        folded = None
        for h in range(heads):
            lanes = slice(h * HD, (h + 1) * HD)
            turned = dqkv[t, :, :, :, lanes].reshape(both, HD).astype(F32)
            back_rot = turned * cosf[...] - pltpu.roll(turned, HD // 2, 1) * sinf[...]
            plain = raw[:, lanes]
            scaled = plain * inv[...]
            gg_mid[2 + t : 3 + t, pl.ds(pl.multiple_of(k * head_w + h * HD, HD), HD)] = jnp.sum(back_rot * scaled, axis=0, keepdims=True)
            gained = back_rot * gqk[t : t + 1, lanes]
            dqkv[t, :, :, :, lanes] = gained.astype(BF16).reshape(2, seqs, blk, HD)
            term = gained * plain
            folded = term if folded is None else folded + term
        sq_own[1, t : t + 1, :] = jnp.sum(jnp.transpose(folded), axis=0, keepdims=True)
    sq_own[1, 2:8, :] = jnp.zeros((6, both), F32)
    dots = totals(1) / width
    for t, (raw, inv) in enumerate(((q_raw, inv_q), (k_raw, inv_k))):
        spread_dot = column_of(dots[t : t + 1, :])
        for h in range(heads):
            lanes = slice(h * HD, (h + 1) * HD)
            gained = dqkv[t, :, :, :, lanes].reshape(both, HD).astype(F32)
            r = inv[...]
            grad = r * gained - raw[:, lanes] * (r * r * r) * spread_dot
            dqkv[t, :, :, :, lanes] = grad.astype(BF16).reshape(2, seqs, blk, HD)

    def rf_copy(i, off):
        return remote(st_z.at[:, ds(off, cw)], rx_f.at[i], rzs.at[3], rzr.at[3], ctx, zp(i + 1))

    def in_partial(core, off):
        here = ds(off, cw)
        acc = None
        for t in range(3):
            left = dqkv[t, pl.ds(core, 1)].reshape(rows, head_w)
            term = lax.dot_general(left, w[t][here, :], NT, preferred_element_type=F32)
            acc = term if acc is None else acc + term
        return acc

    own_rows = ds(z * share_rows, share_rows)
    for i in range(tps):
        off = zp(i + 1) * cw
        st_p[:, ds(off, cw)] = in_partial(ok, off).astype(BF16)
        rp_copy(3, i, off).start()
        mine = in_partial(k, off)
        rp_copy(3, i, off).wait_recv()
        st_z[:, ds(off, cw)] = (mine + rx_p[1, :, ds(off, cw)].astype(F32)).astype(BF16)
        st_z[own_rows, ds(off, cw)] = (st_z[own_rows, ds(off, cw)].astype(F32) + dhid[:, ds(off, cw)]).astype(BF16)
        if i < tps - 1:
            rf_copy(i, off).start()

    pass_g(3)
    for m in range(3):

        def gqkv_step(j, carry):
            here = ds(j * 512, 512)
            right = dqkv[m].reshape(both, head_w)
            w[m][here, :] = jnp.dot(tok_t[here, :], right, preferred_element_type=F32).astype(BF16)
            return carry

        free_w(m)
        lax.fori_loop(0, width // 512, gqkv_step, 0)
        send_g(m)
    middle = gg_row[:, ds(z * feats, feats)]
    came(gg_rx1, mr.at[4])
    for i in range(tps - 1):
        middle = middle + gg_rx1[i]
    gg_mid[...] = gg_mid[...] + middle
    n = 0
    for i, d in slots:
        if i or d:
            core = (k + d) % 2
            go(remote(gg_mid.at[:, ds(chip(i) * 128, 128)], gg_rx2.at[n], ms.at[5], mr.at[5], chip(i) * 2 + core, z))
            n += 1

    add_up(6)
    add_up(4)
    for m in range(3):
        pass_g(m)
    add_up(3)
    add_up(5)
    came(rx_f, rzr.at[3])
    sent(rx_f, rzs.at[3])
    sent(st_p, rps.at[3])
    final = st_z[:, ds(z * feats, cw)].astype(F32)
    for i in range(tps - 1):
        final = final + rx_f[i].astype(F32)
    gin_ref[...] = final
    gain_sum = gg_mid[:, ds(c * 128, 128)]
    came(gg_rx2, mr.at[5])
    for i in range(2 * chips - 1):
        gain_sum = gain_sum + gg_rx2[i]
    ggain_ref[...] = jnp.where(k == 1, pltpu.roll(gain_sum, 64, 1), gain_sum)
    own_out.wait()
    came(stage.at[:, 0 : (tps - 1) * feats], mr.at[3])
    for m in range(3):
        wait_g(m)
    sent(tok.at[0:rows, 0 : (tps - 1) * feats], zs.at[0])
    sent(tok.at[0:rows, :], ps.at[0])
    sent(gbuf.at[0 : 2 * chips - 1], ms.at[0])
    sent(cot.at[:, 0 : (tps - 1) * feats], ms.at[1])
    sent(gall.at[0 : tps - 1], ms.at[2])
    sent(stage.at[:, 0 : (tps - 1) * feats], ms.at[3])
    sent(gg_rx1, ms.at[4])
    sent(gg_rx2, ms.at[5])
    for idx in range(2):
        sent(sq_rx.at[idx], ss.at[idx])
    for m in range(7):
        sent(slabs(m, 5), ws.at[m, 0])
        sent(slabs(m, 7), gs.at[m])


def fused(
    tokens,
    w_query,
    w_key,
    w_value,
    w_output,
    w_gate,
    w_up,
    w_down,
    gain_query,
    gain_key,
    gain_attention,
    gain_feedforward,
    block_order,
    cotangent,
):
    seqs, blk, feats = tokens.shape
    tps = lax.axis_size("tp")
    chips = lax.axis_size("ctx") // 2
    width = feats * tps
    rows = seqs * blk
    both = 2 * rows
    share_rows = rows // tps
    total = 2 * chips * blk
    head_w = w_query.shape[1] // 2
    ff_w = w_gate.shape[1] // 2
    heads = head_w // HD
    slab = width // (2 * chips)
    frequency = THETA ** (-2.0 * np.arange(HD // 2) / HD)
    frequency = np.concatenate([frequency, frequency])
    starts = np.zeros((blk, 1))
    starts[: 2 * chips, 0] = np.arange(2 * chips) * blk
    inside = np.arange(blk)[:, None] * 1.0
    table = np.stack([f(at * frequency) for at in (starts, inside) for f in (np.cos, np.sin)]).astype(np.float32)
    gains = [gain.reshape(1, -1) for gain in (gain_query, gain_key, gain_attention, gain_feedforward)]
    weights = (w_query, w_key, w_value, w_output, w_gate, w_up, w_down)
    dims = (chips, tps, seqs, blk, width, head_w, ff_w)
    halves = (head_w, head_w, head_w, head_w, ff_w, ff_w, ff_w)
    hbm = pl.BlockSpec(memory_space=pl.ANY)
    vmem = pl.BlockSpec(memory_space=pltpu.VMEM)

    def v(shape, dtype=BF16):
        return pltpu.VMEM(shape, dtype)

    w_shapes = [v((width, h)) if m in COLS else v((h, width)) for m, h in enumerate(halves)]
    dma = pltpu.SemaphoreType.DMA
    v_shapes = [v((2, slab, h)) if m in COLS else v((2, h, slab)) for m, h in enumerate(halves)]
    scratch = w_shapes + v_shapes + [
        v((both, width)),
        v((width, both)),
        v((both, width)),
        v((width, both)),
        v((both, width)),
        v((both, width)),
        v((both, ff_w), F32),
        v((both, ff_w), F32),
        v((both, ff_w)),
        v((ff_w, both)),
        v((both, ff_w)),
        v((both, ff_w)),
        v((rows, width)),
        v((2, rows, width)),
        v((rows, width)),
        v((2, tps - 1, share_rows, width)),
        v((tps - 1, rows, feats)),
        v((both, head_w), F32),
        v((both, head_w), F32),
        v((3, 2, seqs, blk, head_w)),
        v((3, 2 * chips, blk, HD)),
        v((total, total)),
        v((total, HD), F32),
        v((2 * chips, blk, HD)),
        v((2, seqs, blk, head_w)),
        v((head_w, both)),
        v((2, seqs, blk, head_w)),
        v((2 * chips, blk, HD)),
        v((3, 2 * chips, blk, HD)),
        v((3, 2, seqs, blk, head_w)),
        v((2, 8, both), F32),
        v((2, 2 * tps - 1, 8, both), F32),
        v((both, 128), F32),
        v((both, 128), F32),
        v((share_rows, width)),
        v((share_rows, width), F32),
        v((share_rows, width), F32),
        v((share_rows, width), F32),
        v((share_rows, width), F32),
        v((2 * chips, 8, 128), F32),
        v((tps, 2 * chips, 8, 128), F32),
        v((8, width), F32),
        v((8, head_w), F32),
        v((8, width), F32),
        v((tps - 1, 8, feats), F32),
        v((8, feats), F32),
        v((2 * chips - 1, 8, 128), F32),
        dma((7, 2)),
        dma((7, 7)),
        dma((7,)),
        dma((7, 3)),
        dma((4,)),
        dma((4, tps - 1)),
        dma((4,)),
        dma((4,)),
        dma((4,)),
        dma((4, tps)),
        dma((4,)),
        dma((4,)),
        dma((6,)),
        dma((6,)),
        dma((2,)),
        dma((2,)),
        dma((4,)),
        dma((4,)),
        dma((25,)),
        v((2 * both, ff_w // 2), F32),
        v((both, HD), F32),
        v((both, HD), F32),
        v((8, total), jnp.int32),
        v((8, 128), F32),
        dma((chips + 1,)),
        dma((2 * chips,)),
    ]
    results = pl.pallas_call(
        functools.partial(layer_kernel, dims),
        out_shape=[
            jax.ShapeDtypeStruct((rows, feats), F32),
            jax.ShapeDtypeStruct((rows, feats), F32),
            jax.ShapeDtypeStruct((8, 128), F32),
        ]
        + [jax.ShapeDtypeStruct((3,) + weight.shape, BF16) for weight in weights]
        + [jax.ShapeDtypeStruct(weight.shape, BF16) for weight in weights[3:]],
        in_specs=[hbm] * 9 + [pl.BlockSpec(memory_space=pltpu.SMEM)] + [vmem] * 5,
        out_specs=[hbm, vmem, vmem] + [hbm] * 11,
        scratch_shapes=scratch,
        compiler_params=pltpu.CompilerParams(
            collective_id=0, has_side_effects=True, vmem_limit_bytes=67043328
        ),
        name="layer",
    )(tokens.reshape(rows, feats), cotangent.reshape(rows, feats), *weights, block_order, *gains, table)
    steps = 2
    shapes = [value.shape for value in results[:2]] + [weight.shape for weight in weights]

    def rows_of(shape):
        return pl.BlockSpec((shape[0] // steps, shape[1]), lambda i: (i, 0))

    three = pl.BlockSpec((3, slab // steps, 2 * head_w), lambda i: (0, i, 0))
    whole = pl.BlockSpec((8, 128), lambda i: (0, 0))
    gain = pl.BlockSpec((1, 64), lambda i: (0, 0))
    wide = pl.pallas_call(
        widen_kernel,
        grid=(steps,),
        out_shape=[jax.ShapeDtypeStruct(shape, F32) for shape in shapes] + [jax.ShapeDtypeStruct((1, 64), F32)] * 4,
        in_specs=[rows_of(shapes[0])] * 2 + [three] * 3 + [rows_of(shape) for shape in shapes[5:]] + [whole],
        out_specs=[rows_of(shape) for shape in shapes] + [gain] * 4,
        name="widen",
    )(*results[:2], *results[3:6], *results[10:], results[2])
    output = wide[0].reshape(tokens.shape)
    grad_input = wide[1].reshape(tokens.shape)
    lanes = [value.reshape(64) for value in wide[9:]]
    return (output, grad_input, *wide[2:9], lanes[2], lanes[3], lanes[0], lanes[1])


def widen_kernel(*refs):
    given, made = refs[:10], refs[10:]
    for i in range(2):
        made[i][...] = given[i][...]
    for i in range(2, 5):
        made[i][...] = given[i][0].astype(F32) + given[i][1].astype(F32) + given[i][2].astype(F32)
    for i in range(5, 9):
        made[i][...] = given[i][...].astype(F32)
    for i in range(4):
        made[9 + i][...] = given[9][i : i + 1, 0:64]


def fits(mesh):
    return mesh.shape["ctx"] == 8 and mesh.shape["tp"] == 4


def solution(mesh):
    placed = (
        P(None, "ctx", "tp"),
        P("ctx", "tp"),
        P("ctx", "tp"),
        P("ctx", "tp"),
        P("tp", "ctx"),
        P("ctx", "tp"),
        P("ctx", "tp"),
        P("tp", "ctx"),
        P(("tp", "ctx")),
        P(("tp", "ctx")),
        P(("tp", "ctx")),
        P(("tp", "ctx")),
        P(),
        P(None, "ctx", "tp"),
    )
    return jax.shard_map(
        fused if fits(mesh) else shards,
        mesh=mesh,
        in_specs=placed,
        out_specs=(
            P(None, "ctx", "tp"),
            P(None, "ctx", "tp"),
            P("ctx", "tp"),
            P("ctx", "tp"),
            P("ctx", "tp"),
            P("tp", "ctx"),
            P("ctx", "tp"),
            P("ctx", "tp"),
            P("tp", "ctx"),
            P(("tp", "ctx")),
            P(("tp", "ctx")),
            P(("tp", "ctx")),
            P(("tp", "ctx")),
        ),
        check_vma=False,
    )
```
